8 devices in a mesh: dp: 1 (over z), pool: 2 (over y), ep: 4 (over x, core).
Axes of the slice: x: 2, y: 2, z: 1, core: 2. Of those that a mesh axis runs over, the one named last changes fastest.
Arguments:
- hidden_in: bfloat16 [512, 896], P(('dp', 'ep'))
- k_cache: bfloat16 [2, 512, 512, 2, 128], P(None, ('dp', 'ep'), 'pool')
- v_cache: bfloat16 [2, 512, 512, 2, 128], P(None, ('dp', 'ep'), 'pool')
- cache_len: int32 [512], P(('dp', 'ep'))
- w_q: bfloat16 [2, 896, 2048], replicated
- w_k: bfloat16 [2, 896, 256], replicated
- w_v: bfloat16 [2, 896, 256], replicated
- w_o: bfloat16 [2, 2048, 896], replicated
- w_router: float32 [2, 896, 256], replicated
- expert_ids: int32 [2, 512, 8], P(None, ('dp', 'ep'))
- w_one: bfloat16 [2, 256, 896, 256], P(None, 'ep', None, 'pool')
- w_three: bfloat16 [2, 256, 896, 256], P(None, 'ep', None, 'pool')
- w_two: bfloat16 [2, 256, 256, 896], P(None, 'ep', 'pool')
Outputs:
- output: bfloat16 [512, 896], P(('dp', 'ep'))
All inputs are finite; a program needn't handle non-finite values.
Results may differ from the reference program's by a relative error of at most 0.02.
Values are sent between devices in bfloat16 or wider.
A program may use at most 1 GiB of HBM per device.

```python
import jax
import jax.numpy as jnp
from jax import lax

D_MODEL = 896
N_HEADS = 16
KV_HEADS = 2
HEAD_DIM = 128
N_EXPERTS = 256
TOP_K = 8
FF_DIM = 256
NUM_LAYERS = 2
EP_GROUP = 4
BATCH_TOK = 512
SEQ_LEN = 512

GROUP_SIZE = N_HEADS // KV_HEADS
LOCAL_EXP = N_EXPERTS // EP_GROUP
TOK_SHARD = BATCH_TOK // EP_GROUP


def draw_ids(rkey):
    k_shift, k_first, k_second = jax.random.split(rkey, 3)
    shift_dev = jax.random.randint(k_shift, (NUM_LAYERS, EP_GROUP, 1, 1), 0, EP_GROUP)
    pair_idx = jnp.arange(TOK_SHARD)[:, None] * TOP_K + jnp.arange(TOP_K)[None, :]
    dest_dev = (pair_idx[None, None] + shift_dev) % EP_GROUP
    first_draw = jax.random.randint(k_first, (NUM_LAYERS, EP_GROUP, TOK_SHARD, 1), 0, LOCAL_EXP)
    second_draw = jax.random.randint(k_second, (NUM_LAYERS, EP_GROUP, TOK_SHARD, 1), 0, LOCAL_EXP)
    start_exp = (first_draw * second_draw) // LOCAL_EXP
    local_id = (start_exp + jnp.arange(TOP_K)[None, None, None, :] // EP_GROUP) % LOCAL_EXP
    chosen = dest_dev * LOCAL_EXP + local_id
    return chosen.reshape(NUM_LAYERS, BATCH_TOK, TOP_K).astype(jnp.int32)


def draw_lens(lkey):
    lens_drawn = jax.random.randint(lkey, (BATCH_TOK,), 1, SEQ_LEN + 1)
    return lens_drawn.at[0].set(SEQ_LEN).astype(jnp.int32)


def setup_inputs(seed: int = 0, part: int = 0) -> dict:
    base_key = jax.random.key(seed)
    part_key = jax.random.fold_in(base_key, part)
    share_keys = jax.random.split(base_key, 8)
    part_keys = jax.random.split(part_key, 5)
    attn_in = N_HEADS * HEAD_DIM
    kv_in = KV_HEADS * HEAD_DIM
    cache_shape = (NUM_LAYERS, BATCH_TOK, SEQ_LEN, KV_HEADS, HEAD_DIM)
    hidden_in = jax.random.normal(part_keys[0], (BATCH_TOK, D_MODEL), jnp.float32).astype(jnp.bfloat16)
    k_cache = jax.random.normal(part_keys[1], cache_shape, jnp.float32).astype(jnp.bfloat16)
    v_cache = jax.random.normal(part_keys[2], cache_shape, jnp.float32).astype(jnp.bfloat16)
    cache_len = draw_lens(part_keys[3])
    expert_ids = draw_ids(part_keys[4])
    w_q = (jax.random.normal(share_keys[0], (NUM_LAYERS, D_MODEL, attn_in), jnp.float32) * (2.0 * D_MODEL ** -0.5)).astype(jnp.bfloat16)
    w_k = (jax.random.normal(share_keys[1], (NUM_LAYERS, D_MODEL, kv_in), jnp.float32) * D_MODEL ** -0.5).astype(jnp.bfloat16)
    w_v = (jax.random.normal(share_keys[2], (NUM_LAYERS, D_MODEL, kv_in), jnp.float32) * D_MODEL ** -0.5).astype(jnp.bfloat16)
    w_o = (jax.random.normal(share_keys[3], (NUM_LAYERS, attn_in, D_MODEL), jnp.float32) * (2.0 * attn_in ** -0.5)).astype(jnp.bfloat16)
    w_router = jax.random.normal(share_keys[4], (NUM_LAYERS, D_MODEL, N_EXPERTS), jnp.float32) * (1.5 * D_MODEL ** -0.5)
    w_one = (jax.random.normal(share_keys[5], (NUM_LAYERS, N_EXPERTS, D_MODEL, FF_DIM), jnp.float32) * D_MODEL ** -0.5).astype(jnp.bfloat16)
    w_three = (jax.random.normal(share_keys[6], (NUM_LAYERS, N_EXPERTS, D_MODEL, FF_DIM), jnp.float32) * D_MODEL ** -0.5).astype(jnp.bfloat16)
    w_two = (jax.random.normal(share_keys[7], (NUM_LAYERS, N_EXPERTS, FF_DIM, D_MODEL), jnp.float32) * (2.0 * FF_DIM ** -0.5)).astype(jnp.bfloat16)
    return dict(hidden_in=hidden_in, k_cache=k_cache, v_cache=v_cache, cache_len=cache_len, w_q=w_q, w_k=w_k, w_v=w_v, w_o=w_o, w_router=w_router, expert_ids=expert_ids, w_one=w_one, w_three=w_three, w_two=w_two)


def rms_norm(in_vals):
    in_vals = in_vals.astype(jnp.float32)
    return in_vals * lax.rsqrt(jnp.mean(in_vals * in_vals, axis=-1, keepdims=True) + 1e-6)


def attend_token(packed):
    q_tok, k_new, v_new, k_rows, v_rows, valid_len = packed
    att_scale = HEAD_DIM ** -0.5
    q_grp = q_tok.reshape(KV_HEADS, GROUP_SIZE, HEAD_DIM).astype(jnp.float32)
    score_vals = jnp.einsum('gqd,sgd->gqs', q_grp, k_rows.astype(jnp.float32)) * att_scale
    pos_mask = jnp.arange(SEQ_LEN) < valid_len
    score_vals = jnp.where(pos_mask[None, None, :], score_vals, -1e30)
    new_score = jnp.einsum('gqd,gd->gq', q_grp, k_new.astype(jnp.float32)) * att_scale
    top_score = jnp.maximum(jnp.max(score_vals, axis=-1), new_score)
    prob_vals = jnp.exp(score_vals - top_score[..., None])
    new_prob = jnp.exp(new_score - top_score)
    denom_sum = jnp.sum(prob_vals, axis=-1) + new_prob
    numer_sum = jnp.einsum('gqs,sgd->gqd', prob_vals.astype(jnp.bfloat16).astype(jnp.float32), v_rows.astype(jnp.float32))
    numer_sum = numer_sum + new_prob[..., None] * v_new.astype(jnp.float32)[:, None, :]
    return (numer_sum / denom_sum[..., None]).reshape(N_HEADS * HEAD_DIM)


def moe_experts(u_rows, ids_layer, w_one, w_three, w_two):
    flat_ids = ids_layer.reshape(-1)
    sort_order = jnp.argsort(flat_ids, stable=True)
    tok_rows = u_rows[sort_order // TOP_K].astype(jnp.float32)
    group_sizes = jnp.bincount(flat_ids, length=N_EXPERTS).astype(jnp.int32)
    h_one = lax.ragged_dot(tok_rows, w_one.astype(jnp.float32), group_sizes)
    h_three = lax.ragged_dot(tok_rows, w_three.astype(jnp.float32), group_sizes)
    act_rows = (jax.nn.silu(h_one) * h_three).astype(jnp.bfloat16).astype(jnp.float32)
    out_rows = lax.ragged_dot(act_rows, w_two.astype(jnp.float32), group_sizes).astype(jnp.bfloat16)
    back_order = jnp.argsort(sort_order)
    return out_rows[back_order].reshape(BATCH_TOK, TOP_K, D_MODEL)


def reference(hidden_in, k_cache, v_cache, cache_len, w_q, w_k, w_v, w_o, w_router, expert_ids, w_one, w_three, w_two):
    def layer_step(hidden, layer_in):
        kc_l, vc_l, wq_l, wk_l, wv_l, wo_l, wr_l, ids_l, w1_l, w3_l, w2_l = layer_in
        normed = rms_norm(hidden).astype(jnp.bfloat16)
        q_rows = jnp.dot(normed, wq_l, preferred_element_type=jnp.float32).astype(jnp.bfloat16)
        k_new = jnp.dot(normed, wk_l, preferred_element_type=jnp.float32).astype(jnp.bfloat16).reshape(BATCH_TOK, KV_HEADS, HEAD_DIM)
        v_new = jnp.dot(normed, wv_l, preferred_element_type=jnp.float32).astype(jnp.bfloat16).reshape(BATCH_TOK, KV_HEADS, HEAD_DIM)
        attn_out = lax.map(attend_token, (q_rows, k_new, v_new, kc_l, vc_l, cache_len)).astype(jnp.bfloat16)
        resid_rows = (hidden.astype(jnp.float32) + jnp.dot(attn_out, wo_l, preferred_element_type=jnp.float32)).astype(jnp.bfloat16)
        u_rows = rms_norm(resid_rows).astype(jnp.bfloat16)
        logits = jnp.dot(u_rows.astype(jnp.float32), wr_l)
        gate_vals = jax.nn.softmax(jnp.take_along_axis(logits, ids_l, axis=1), axis=-1)
        pair_rows = moe_experts(u_rows, ids_l, w1_l, w3_l, w2_l)
        mixed_sum = jnp.sum(gate_vals[..., None] * pair_rows.astype(jnp.float32), axis=1)
        return (resid_rows.astype(jnp.float32) + mixed_sum).astype(jnp.bfloat16), None
    hidden_out, unused_ys = lax.scan(layer_step, hidden_in, (k_cache, v_cache, w_q, w_k, w_v, w_o, w_router, expert_ids, w_one, w_three, w_two))
    return hidden_out
```

```python
import functools

import jax
import jax.numpy as jnp
from jax import lax
from jax.experimental import pallas as pl
from jax.experimental.pallas import tpu as pltpu
from jax.sharding import PartitionSpec as P

MESH = pl.DeviceIdType.MESH
F32, BF16, I32 = jnp.float32, jnp.bfloat16, jnp.int32
NORM_EPS = 1e-6
T, D, HD, H = 128, 896, 128, 16
HALF = T // 2
KV = 2
POS = 256
ROWS = POS * KV
CH = 8
NCH = T // CH
NB = 8
ALL = 4 * T
NE = 64
PAIRS = 1024
FF = 128
NW = 24
MC = 32
CM = 384
NX = 8
XR = PAIRS // NX
VMEM_LIMIT = 60 * 1024 * 1024


def rms(v):
    v = v.astype(F32)
    return v * lax.rsqrt(jnp.mean(v * v, axis=-1, keepdims=True) + NORM_EPS)


def mm(a, b):
    return jnp.dot(a, b, preferred_element_type=F32)


def iota(shape, dim):
    return lax.broadcasted_iota(I32, shape, dim)


def peers():
    g, p, e = lax.axis_index("dp"), lax.axis_index("pool"), lax.axis_index("ep")
    core = lax.rem(e, 2)
    e_x = lax.rem(e + 2, 4)
    e_d = e + 1 - 2 * core
    e_z = lax.rem(e_d + 2, 4)
    return p, e, e_x, e_d, e_z, (g, 1 - p, e), (g, p, e_x), (g, p, e_d), (g, p, e_z)


def entry_barrier(targets):
    bar = pltpu.get_barrier_semaphore()
    for dev in targets:
        pl.semaphore_signal(bar, inc=1, device_id=dev, device_id_type=MESH)
    pl.semaphore_wait(bar, len(targets))


def remote(src, dst, send_sem, recv_sem, dev):
    return pltpu.make_async_remote_copy(src_ref=src, dst_ref=dst, send_sem=send_sem, recv_sem=recv_sem,
                                        device_id=dev, device_id_type=MESH)


def attn_kernel(layer, first, *refs):
    if first:
        (x_ref, len_ref, idt_ref, k_ref, v_ref, wq_ref, wk_ref, wv_ref, wo_ref, a_ref, ida_ref, *scr) = refs
    else:
        (x_ref, len_ref, k_ref, v_ref, wq_ref, wk_ref, wv_ref, wo_ref, a_ref, *scr) = refs
    (kbuf, vbuf, wq_v, wk_v, wv_v, wo_v, q2d, kn2d, vn2d, num, nrec, stat, ssend, srec,
     kv_sem, w_sem, ns_sem, nr_sem, ss_sem, sr_sem, gs_sem, gr_sem, is_sem, ir_sem) = scr
    p, e, e_x, e_d, e_z, dev_y, dev_x, dev_d, dev_z = peers()

    def tok_of(c):
        first_half = (1 - p) * HALF + c * CH
        second_half = p * HALF + (c - NCH // 2) * CH
        return pl.multiple_of(jnp.where(c < NCH // 2, first_half, second_half), CH)

    def kv_copies(c):
        slot = lax.rem(c, NB)
        src = pl.ds(tok_of(c), CH)
        return (pltpu.make_async_copy(k_ref.at[layer, src], kbuf.at[slot], kv_sem.at[0, slot]),
                pltpu.make_async_copy(v_ref.at[layer, src], vbuf.at[slot], kv_sem.at[1, slot]))

    weights = [pltpu.make_async_copy(r.at[layer], b, w_sem.at[i])
               for i, (r, b) in enumerate(((wq_ref, wq_v), (wk_ref, wk_v), (wv_ref, wv_v), (wo_ref, wo_v)))]
    for cp in weights[:3]:
        cp.start()
    for c in range(NB):
        for cp in kv_copies(jnp.int32(c)):
            cp.start()
    weights[3].start()

    entry_barrier((dev_y, dev_x, dev_d, dev_z))

    id_copies = []
    if first:
        mine = (slice(None), slice(None), pl.ds(pl.multiple_of(e * T, T), T))
        ida_ref[mine] = idt_ref[...]
        for i, dev in enumerate((dev_x, dev_d, dev_z)):
            id_copies.append(remote(idt_ref, ida_ref.at[mine], is_sem.at[i], ir_sem.at[i], dev))
            id_copies[-1].start()

    normed = rms(x_ref[...]).astype(BF16)
    for cp in weights[:3]:
        cp.wait()
    for hp in range(H // 2):
        pair = mm(normed, wq_v[:, hp * 256:(hp + 1) * 256]).astype(BF16).astype(F32)
        for i in range(2):
            q2d[pl.ds(hp * 2 + i, T, stride=H), :] = pair[:, i * HD:(i + 1) * HD]
    for w, dst in ((wk_v, kn2d), (wv_v, vn2d)):
        pair = mm(normed, w[...]).astype(BF16).astype(F32)
        for i in range(KV):
            dst[pl.ds(i, T, stride=KV), :] = pair[:, i * HD:(i + 1) * HD]

    scale = HD ** -0.5
    col = iota((H, ROWS), 1)
    group_ok = (col & 1) == (iota((H, ROWS), 0) // (H // KV))
    col_pos = jnp.where(group_ok, col >> 1, 1 << 30)
    lane = iota((H, T), 1)

    def heads_of(ref, tok):
        two = ref[pl.ds(tok * KV, KV), :]
        return jnp.concatenate([jnp.broadcast_to(two[i:i + 1], (H // KV, HD)) for i in range(KV)], axis=0)

    def num_copy(c):
        rows = pl.ds(pl.multiple_of(c * (CH * H), CH * H), CH * H)
        return remote(num.at[rows], nrec.at[rows], ns_sem.at[c], nr_sem.at[c], dev_y)

    stat_copy = remote(ssend, srec, ss_sem, sr_sem, dev_y)

    def chunk(c, carry):
        slot = lax.rem(c, NB)
        for cp in kv_copies(c):
            cp.wait()
        tok0 = tok_of(c)
        m_all, l_all, n_all = stat[0], stat[1], stat[2]
        for j0 in range(0, CH, 4):
            group = range(j0, j0 + 4)
            qs, ss = {}, {}
            for j in group:
                qs[j] = q2d[pl.ds(pl.multiple_of((tok0 + j) * H, H), H), :]
                ss[j] = lax.dot_general(qs[j].astype(BF16), kbuf[slot, j], (((1,), (1,)), ((), ())),
                                        preferred_element_type=F32) * scale
            ps = {}
            for j in group:
                limit = len_ref[tok0 + j] - p * POS
                s = jnp.where(col_pos < limit, ss[j], -1e30)
                s_new = jnp.sum(qs[j] * heads_of(kn2d, tok0 + j), axis=1, keepdims=True) * scale
                m = jnp.maximum(jnp.max(s, axis=1, keepdims=True), s_new)
                pr = jnp.exp(s - m)
                ps[j] = pr.astype(BF16)
                here = lane == c * CH + j
                m_all = jnp.where(here, m, m_all)
                l_all = jnp.where(here, jnp.sum(pr, axis=1, keepdims=True), l_all)
                n_all = jnp.where(here, s_new, n_all)
            for j in group:
                num[pl.ds(pl.multiple_of((c * CH + j) * H, H), H), :] = mm(ps[j], vbuf[slot, j])
        stat[0], stat[1], stat[2] = m_all, l_all, n_all

        @pl.when(c + NB < NCH)
        def _():
            for cp in kv_copies(c + NB):
                cp.start()

        @pl.when(c == NCH // 2 - 1)
        def _():
            ssend[0], ssend[1] = m_all, l_all

        @pl.when((c >= 1) & (c <= NCH // 2))
        def _():
            num_copy(c - 1).start()

        @pl.when(c == NCH // 2)
        def _():
            stat_copy.start()

        return carry

    stat[...] = jnp.zeros_like(stat)
    lax.fori_loop(0, NCH, chunk, 0)

    weights[3].wait()
    stat_copy.wait()
    m_own, l_own, s_new = stat[0], stat[1], stat[2]
    m_far = pltpu.roll(srec[0], HALF, axis=1)
    l_far = pltpu.roll(srec[1], HALF, axis=1)
    m = jnp.maximum(m_own, m_far)
    w_own, w_far, w_new = jnp.exp(m_own - m), jnp.exp(m_far - m), jnp.exp(s_new - m)
    denom = l_own * w_own + l_far * w_far + w_new
    c_own, c_far, c_new = w_own / denom, w_far / denom, w_new / denom

    def combine(c, carry):
        num_copy(c).wait()
        for j in range(CH):
            i = c * CH + j
            pick = lane == HALF + i
            own, far, new = [jnp.sum(jnp.where(pick, v, 0.0), axis=1, keepdims=True) for v in (c_own, c_far, c_new)]
            there = pl.ds(pl.multiple_of(i * H, H), H)
            here = pl.ds(pl.multiple_of((HALF + i) * H, H), H)
            num[here, :] = num[here, :] * own + nrec[there, :] * far + heads_of(vn2d, p * HALF + i) * new
        return carry

    lax.fori_loop(0, NCH // 2, combine, 0)

    proj = jnp.zeros((HALF, D), F32)
    for hp in range(H // 2):
        pair = jnp.concatenate([num[pl.ds(HALF * H + hp * 2 + i, HALF, stride=H), :].astype(BF16) for i in range(2)], axis=1)
        proj = proj + mm(pair, wo_v[hp * 256:(hp + 1) * 256, :])
    mine = pl.ds(pl.multiple_of(p * HALF, HALF), HALF)

    def rows(pp, ee):
        return pl.ds(pl.multiple_of(ee * T + pp * HALF, HALF), HALF)

    a_ref[rows(p, e), :] = (x_ref[mine, :].astype(F32) + proj).astype(BF16)

    def gather(i, pp, ee, dev):
        block = a_ref.at[rows(pp, ee)]
        cp = remote(block, block, gs_sem.at[i], gr_sem.at[i], dev)
        cp.start()
        return cp

    copies = [gather(0, p, e, dev_y), gather(1, p, e, dev_x), gather(2, p, e, dev_d)]
    copies[0].wait_recv()
    copies += [gather(3, 1 - p, e, dev_x), gather(4, 1 - p, e, dev_d)]
    copies[1].wait_recv()
    copies += [gather(5, p, e_x, dev_d)]
    copies[3].wait_recv()
    copies += [gather(6, 1 - p, e_x, dev_d)]
    for i in (2, 4, 5, 6):
        copies[i].wait_recv()
    for cp in copies:
        cp.wait_send()
    for cp in id_copies:
        cp.wait()


def attention(layer, x, cache_len, id_t, k, v, wq, wk, wv, wo, cid):
    first = id_t is not None
    vm, sm, hb = (pl.BlockSpec(memory_space=m) for m in (pltpu.VMEM, pltpu.SMEM, pl.ANY))
    dma = pltpu.SemaphoreType.DMA
    outs = [jax.ShapeDtypeStruct((ALL, D), BF16)]
    if first:
        outs.append(jax.ShapeDtypeStruct((id_t.shape[0], 8, ALL), I32))
    out = pl.pallas_call(
        functools.partial(attn_kernel, layer, first),
        name=f"attn_{layer}",
        out_shape=outs,
        in_specs=[vm, sm] + ([vm] if first else []) + [hb] * 6,
        out_specs=[vm] * len(outs),
        scratch_shapes=[
            pltpu.VMEM((NB, CH, ROWS, HD), BF16), pltpu.VMEM((NB, CH, ROWS, HD), BF16),
            pltpu.VMEM((D, H * HD), BF16), pltpu.VMEM((D, KV * HD), BF16), pltpu.VMEM((D, KV * HD), BF16),
            pltpu.VMEM((H * HD, D), BF16),
            pltpu.VMEM((T * H, HD), F32), pltpu.VMEM((T * KV, HD), F32), pltpu.VMEM((T * KV, HD), F32),
            pltpu.VMEM((T * H, HD), F32), pltpu.VMEM((HALF * H, HD), F32),
            pltpu.VMEM((3, H, T), F32), pltpu.VMEM((2, H, T), F32), pltpu.VMEM((2, H, T), F32),
            dma((2, NB)), dma((4,)), dma((NCH // 2,)), dma((NCH // 2,)), dma(()), dma(()),
            dma((7,)), dma((7,)), dma((3,)), dma((3,)),
        ],
        compiler_params=pltpu.CompilerParams(collective_id=cid, has_side_effects=True, vmem_limit_bytes=VMEM_LIMIT),
    )(*([x, cache_len] + ([id_t] if first else []) + [k, v, wq, wk, wv, wo]))
    return out if first else (out[0], None)


def expert_kernel(layer, a_ref, idt_ref, w1_ref, w3_ref, w2_ref, ym_ref, yt_ref,
                  w1b, w3b, w2b, u, xs, ym, yt, tail, pos, meta, smeta, w_sem, m_sem, o_sem):
    e = lax.axis_index("ep")

    def w_copies(i):
        slot = lax.rem(i, NW)
        return [pltpu.make_async_copy(r.at[layer, i], b.at[slot], w_sem.at[n, slot])
                for n, (r, b) in enumerate(((w1_ref, w1b), (w3_ref, w3b), (w2_ref, w2b)))]

    def start(i, carry):
        for cp in w_copies(i):
            cp.start()
        return carry

    lax.fori_loop(0, NW, start, 0)

    u[...] = rms(a_ref[...]).astype(BF16)
    sub = iota((128, ALL), 0)
    local = [idt_ref[layer, k:k + 1, :] - e * NE for k in range(8)]
    local = [jnp.where((v >= 0) & (v < NE), v, -1) for v in local]
    mask = jnp.zeros((128, ALL), F32)
    for v in local:
        mask = jnp.where(v == sub, 1.0, mask)
    mask_b = mask.astype(BF16)
    before = (iota((ALL, ALL), 0) < iota((ALL, ALL), 1)).astype(BF16)
    rank = mm(mask_b, before)
    n_col = jnp.broadcast_to(jnp.sum(mask, axis=1, keepdims=True), (128, 128)).astype(I32)
    n_row = lax.dot_general(jnp.ones((8, ALL), BF16), mask_b, (((1,), (1,)), ((), ())),
                            preferred_element_type=F32).astype(I32)
    lower = (iota((128, 128), 1) < iota((128, 128), 0)).astype(BF16)
    upper = (iota((128, 128), 0) < iota((128, 128), 1)).astype(BF16)
    as_b = lambda v: v.astype(F32).astype(BF16)
    off_col = mm(lower, as_b((n_col + 15) >> 4)) * 16.0
    off_row = mm(as_b((n_row + 15) >> 4), upper)
    offc_row = mm(as_b(n_row >> 4), upper) * 16.0 + mm(as_b(n_row & 15), upper)
    meta[0] = n_row
    meta[1] = off_row.astype(I32)
    meta[2] = offc_row.astype(I32)
    m_copy = pltpu.make_async_copy(meta, smeta, m_sem)
    m_copy.start()
    where_to = off_col[:, 0:1] + rank + 1.0
    for k in range(8):
        pos[k:k + 1, :] = (jnp.sum(jnp.where(local[k] == sub, where_to, 0.0), axis=0, keepdims=True) - 1.0).astype(I32)
    m_copy.wait()

    def dispatch(i, carry):
        row = iota((256, ALL), 0) + i * 256
        hit = jnp.zeros((256, ALL), F32)
        for k in range(8):
            hit = jnp.where(pos[k:k + 1, :] == row, 1.0, hit)
        xs[pl.ds(pl.multiple_of(i * 256, 256), 256), :] = mm(hit.astype(BF16), u[...]).astype(BF16)
        return carry

    lax.fori_loop(0, (smeta[1, 0, NE] + 15) >> 4, dispatch, 0)

    def expert(i, carry):
        slot = lax.rem(i, NW)
        for cp in w_copies(i):
            cp.wait()
        n, off, offc = smeta[0, 0, i], smeta[1, 0, i], smeta[2, 0, i]

        def rows_step(j, c2):
            rows = xs[pl.ds(pl.multiple_of(off * 16 + j * MC, 16), MC), :]
            act = (jax.nn.silu(mm(rows, w1b[slot])) * mm(rows, w3b[slot])).astype(BF16)
            y = mm(act, w2b[slot])
            to = pl.ds(offc + j * MC, MC)
            for t in range(6):
                ym[t // 3, t % 3, to, :] = y[:, t * 128:(t + 1) * 128]
            yt[to, :] = y[:, 2 * CM:]
            return c2

        lax.fori_loop(0, (n + MC - 1) // MC, rows_step, 0)

        @pl.when(i + NW < NE)
        def _():
            start(i + NW, 0)

        return carry

    lax.fori_loop(0, NE, expert, 0)
    out = pltpu.make_async_copy(ym.at[:, :, pl.ds(0, PAIRS)], ym_ref, o_sem.at[0])
    out.start()
    top, bot = yt[:PAIRS // 2, :], yt[PAIRS // 2:PAIRS, :]
    left = iota((PAIRS // 2, 128), 1) < 64
    tail[0] = jnp.where(left, top, pltpu.roll(bot, 64, axis=1))
    tail[1] = jnp.where(left, pltpu.roll(top, 64, axis=1), bot)
    out2 = pltpu.make_async_copy(tail, yt_ref, o_sem.at[1])
    out2.start()
    out.wait()
    out2.wait()


def experts(layer, a_all, id_t, w1, w3, w2):
    vm, hb = (pl.BlockSpec(memory_space=m) for m in (pltpu.VMEM, pl.ANY))
    dma = pltpu.SemaphoreType.DMA
    return pl.pallas_call(
        functools.partial(expert_kernel, layer),
        name=f"experts_{layer}",
        out_shape=[jax.ShapeDtypeStruct((2, 3, PAIRS, 128), F32), jax.ShapeDtypeStruct((2, PAIRS // 2, 128), F32)],
        in_specs=[vm, vm, hb, hb, hb],
        out_specs=[hb, hb],
        scratch_shapes=[
            pltpu.VMEM((NW, D, FF), BF16), pltpu.VMEM((NW, D, FF), BF16), pltpu.VMEM((NW, FF, D), BF16),
            pltpu.VMEM((ALL, D), BF16), pltpu.VMEM((2304, D), BF16),
            pltpu.VMEM((2, 3, PAIRS + MC, 128), F32), pltpu.VMEM((PAIRS + MC, 128), F32),
            pltpu.VMEM((2, PAIRS // 2, 128), F32),
            pltpu.VMEM((8, ALL), I32), pltpu.VMEM((3, 8, 128), I32), pltpu.SMEM((3, 8, 128), I32),
            dma((3, NW)), dma(()), dma((2,)),
        ],
        compiler_params=pltpu.CompilerParams(vmem_limit_bytes=VMEM_LIMIT),
    )(a_all, id_t, w1, w3, w2)


def merge_kernel(layer, a_ref, id_ref, ym_ref, yt_ref, wr_ref, x_ref,
                 my_m, my_t, rec_m, rec_t, wr, gate, acc_m, acc_t, back_m, back_t, send_m, send_t, far_m, far_t,
                 l_sem, xs_sem, xr_sem, bs_sem, br_sem, fs_sem, fr_sem):
    p, e, e_x, e_d, e_z, dev_y, dev_x, dev_d, dev_z = peers()
    loads = [pltpu.make_async_copy(src, dst, l_sem.at[i])
             for i, (src, dst) in enumerate(((wr_ref.at[layer], wr), (ym_ref.at[p], my_m), (yt_ref.at[p], my_t)))]
    for cp in loads:
        cp.start()
    entry_barrier((dev_y, dev_x, dev_d, dev_z))

    def y_copy(c):
        block = pl.ds(c * XR, XR)
        return remote(ym_ref.at[1 - p, :, block], rec_m.at[:, block], xs_sem.at[c], xr_sem.at[c], dev_y)

    t_copy = remote(yt_ref.at[1 - p], rec_t, xs_sem.at[NX], xr_sem.at[NX], dev_y)
    y_copies = [y_copy(c) for c in range(NX)]
    for cp in y_copies:
        cp.start()
    t_copy.start()

    loads[0].wait()
    u = rms(a_ref[...]).astype(BF16)
    logits = jnp.zeros((ALL, 256), F32)
    rest = wr[...]
    for _ in range(3):
        part = rest.astype(BF16)
        rest = rest - part.astype(F32)
        logits = logits + mm(u, part)
    col = iota((ALL, 256), 1)
    ids = [id_ref[layer, :, k:k + 1] for k in range(8)]
    g = [jnp.sum(jnp.where(v == col, logits, 0.0), axis=1, keepdims=True) for v in ids]
    top = functools.reduce(jnp.maximum, g)
    g = [jnp.exp(v - top) for v in g]
    total = functools.reduce(jnp.add, g)
    g = [v / total for v in g]

    lane = iota((ALL, 128), 1)
    local = [jnp.where((v >= e * NE) & (v < (e + 1) * NE), v - e * NE, -1) for v in ids]
    mask = jnp.zeros((ALL, 128), F32)
    for v in local:
        mask = jnp.where(v == lane, 1.0, mask)
    mask_b = mask.astype(BF16)
    before = (iota((ALL, ALL), 1) < iota((ALL, ALL), 0)).astype(BF16)
    rank = mm(before, mask_b)
    n_row = mm(jnp.ones((8, ALL), BF16), mask_b).astype(I32)
    upper = (iota((128, 128), 0) < iota((128, 128), 1)).astype(BF16)
    as_b = lambda v: v.astype(F32).astype(BF16)
    offc = mm(as_b(n_row >> 4), upper) * 16.0 + mm(as_b(n_row & 15), upper)
    where_to = offc[0:1, :] + rank + 1.0
    pos = [(jnp.sum(jnp.where(v == lane, where_to, 0.0), axis=1, keepdims=True) - 1.0).astype(I32) for v in local]

    for c in range(PAIRS // 128):
        w = jnp.zeros((ALL, 128), F32)
        for k in range(8):
            w = jnp.where(pos[k] == lane + c * 128, g[k], w)
        for i in range(3):
            part = w.astype(BF16)
            w = w - part.astype(F32)
            gate[i, :, c * 128:(c + 1) * 128] = part

    def mix(block, y):
        return sum(mm(gate[i, :, block], y) for i in range(3))

    loads[1].wait()
    loads[2].wait()
    for c in range(NX):
        block = slice(c * XR, (c + 1) * XR)
        y_copies[c].wait_recv()
        part = mix(block, jnp.concatenate([(my_m[t, block, :] + rec_m[t, block, :]).astype(BF16) for t in range(3)], axis=1))
        acc_m[...] = part if c == 0 else acc_m[...] + part
    t_copy.wait_recv()
    y_tail = (my_t[...] + rec_t[...]).astype(BF16)
    half0, half1 = mix(slice(0, PAIRS // 2), y_tail), mix(slice(PAIRS // 2, PAIRS), y_tail)
    keep0 = jnp.broadcast_to(p == 0, half0.shape)
    acc_t[...] = jnp.where(keep0, half0, pltpu.roll(half0, 64, axis=1)) + jnp.where(keep0, pltpu.roll(half1, 64, axis=1), half1)

    def block_of(ee):
        return pl.ds(pl.multiple_of(ee * T, T), T)

    backs = []
    for i, (ee, dev) in enumerate(((e_x, dev_x), (e_z, dev_z), (e_d, dev_d))):
        backs.append(remote(acc_m.at[block_of(ee)], back_m.at[i], bs_sem.at[2 * i], br_sem.at[2 * i], dev))
        backs.append(remote(acc_t.at[block_of(ee)], back_t.at[i], bs_sem.at[2 * i + 1], br_sem.at[2 * i + 1], dev))
    for cp in backs:
        cp.start()
    sum_m, sum_t = acc_m[block_of(e), :], acc_t[block_of(e), :]
    a_m = a_ref[block_of(e), pl.ds(pl.multiple_of(p * CM, CM), CM)].astype(F32)
    a_t = a_ref[block_of(e), 2 * CM:].astype(F32)
    for i in (2, 0, 1):
        backs[2 * i].wait_recv()
        backs[2 * i + 1].wait_recv()
        sum_m = sum_m + back_m[i]
        sum_t = sum_t + back_t[i]
    send_m[...] = (a_m + sum_m).astype(BF16)
    send_t[...] = (a_t + sum_t).astype(BF16)
    outs = [remote(send_m, far_m, fs_sem.at[0], fr_sem.at[0], dev_y),
            remote(send_t, far_t, fs_sem.at[1], fr_sem.at[1], dev_y)]
    for cp in outs:
        cp.start()
    x_ref[:, pl.ds(pl.multiple_of(p * CM, CM), CM)] = send_m[...]
    for cp in outs:
        cp.wait()
    x_ref[:, pl.ds(pl.multiple_of((1 - p) * CM, CM), CM)] = far_m[...]
    keep_own = (iota((T, 128), 1) // 64) == p
    x_ref[:, 2 * CM:] = jnp.where(keep_own, send_t[...].astype(F32), far_t[...].astype(F32)).astype(BF16)
    for cp in y_copies + [t_copy] + backs:
        cp.wait_send()


def merge(layer, a_all, ids, ym, yt, wr, cid):
    vm, hb = (pl.BlockSpec(memory_space=m) for m in (pltpu.VMEM, pl.ANY))
    dma = pltpu.SemaphoreType.DMA
    return pl.pallas_call(
        functools.partial(merge_kernel, layer),
        name=f"merge_{layer}",
        out_shape=jax.ShapeDtypeStruct((T, D), BF16),
        in_specs=[vm, vm, hb, hb, hb],
        out_specs=vm,
        scratch_shapes=[
            pltpu.VMEM((3, PAIRS, 128), F32), pltpu.VMEM((PAIRS // 2, 128), F32),
            pltpu.VMEM((3, PAIRS, 128), F32), pltpu.VMEM((PAIRS // 2, 128), F32),
            pltpu.VMEM((D, 256), F32), pltpu.VMEM((3, ALL, PAIRS), BF16),
            pltpu.VMEM((ALL, CM), F32), pltpu.VMEM((ALL, 128), F32),
            pltpu.VMEM((3, T, CM), F32), pltpu.VMEM((3, T, 128), F32),
            pltpu.VMEM((T, CM), BF16), pltpu.VMEM((T, 128), BF16),
            pltpu.VMEM((T, CM), BF16), pltpu.VMEM((T, 128), BF16),
            dma((3,)), dma((NX + 1,)), dma((NX + 1,)), dma((6,)), dma((6,)), dma((2,)), dma((2,)),
        ],
        compiler_params=pltpu.CompilerParams(collective_id=cid, has_side_effects=True, vmem_limit_bytes=VMEM_LIMIT),
    )(a_all, ids, ym, yt, wr)


def solution(mesh):
    tok_spec = P(('dp', 'ep'), None)
    cache_spec = P(None, ('dp', 'ep'), 'pool', None, None)
    up_spec = P(None, 'ep', None, 'pool')
    down_spec = P(None, 'ep', 'pool', None)
    in_specs = (tok_spec, cache_spec, cache_spec, P(('dp', 'ep')), P(), P(), P(), P(), P(), P(None, ('dp', 'ep'), None),
                up_spec, up_spec, down_spec)

    def body(hidden, k_cache, v_cache, cache_len, w_q, w_k, w_v, w_o, w_router, expert_ids, w_one, w_three, w_two):
        layers = w_q.shape[0]
        k = k_cache.reshape(layers, T, ROWS, HD)
        v = v_cache.reshape(layers, T, ROWS, HD)
        id_t = jnp.swapaxes(expert_ids, 1, 2)
        ids_t = ids = None
        for layer in range(layers):
            a_all, gathered = attention(layer, hidden, cache_len, id_t if layer == 0 else None, k, v, w_q, w_k, w_v, w_o, 2 * layer)
            if layer == 0:
                ids_t, ids = gathered, jnp.swapaxes(gathered, 1, 2)
            ym, yt = experts(layer, a_all, ids_t, w_one, w_three, w_two)
            hidden = merge(layer, a_all, ids, ym, yt, w_router, 2 * layer + 1)
        return hidden

    return jax.shard_map(body, mesh=mesh, in_specs=in_specs, out_specs=tok_spec, check_vma=False)
```

```python
import functools

import jax
import jax.numpy as jnp
from jax import lax
from jax.experimental import pallas as pl
from jax.experimental.pallas import tpu as pltpu
from jax.sharding import PartitionSpec as P

MESH = pl.DeviceIdType.MESH
F32, BF16, I32 = jnp.float32, jnp.bfloat16, jnp.int32
NORM_EPS = 1e-6
T, D, HD, H = 128, 896, 128, 16
HALF = T // 2
KV = 2
POS = 256
ROWS = POS * KV
CH = 8
NCH = T // CH
NB = 8
ALL = 4 * T
NE = 64
PAIRS = 1024
FF = 128
NW = 32
MC = 32
CM = 384
PARTS = 2
NR = PAIRS // PARTS
PR = 3 * NR + NR // 2
PAD = MC
VMEM_LIMIT = 60 * 1024 * 1024


def rms(v):
    v = v.astype(F32)
    return v * lax.rsqrt(jnp.mean(v * v, axis=-1, keepdims=True) + NORM_EPS)


def mm(a, b):
    return jnp.dot(a, b, preferred_element_type=F32)


def iota(shape, dim):
    return lax.broadcasted_iota(I32, shape, dim)


def peers():
    g, p, e = lax.axis_index("dp"), lax.axis_index("pool"), lax.axis_index("ep")
    core = lax.rem(e, 2)
    e_x = lax.rem(e + 2, 4)
    e_d = e + 1 - 2 * core
    e_z = lax.rem(e_d + 2, 4)
    return p, e, e_x, e_d, e_z, (g, 1 - p, e), (g, p, e_x), (g, p, e_d), (g, p, e_z)


def entry_barrier(targets):
    bar = pltpu.get_barrier_semaphore()
    for dev in targets:
        pl.semaphore_signal(bar, inc=1, device_id=dev, device_id_type=MESH)
    pl.semaphore_wait(bar, len(targets))


def remote(src, dst, send_sem, recv_sem, dev):
    return pltpu.make_async_remote_copy(src_ref=src, dst_ref=dst, send_sem=send_sem, recv_sem=recv_sem,
                                        device_id=dev, device_id_type=MESH)


def route(ids, e, meta, pos):
    sub = iota((128, ALL), 0)
    local = [ids[k:k + 1, :] - e * NE for k in range(8)]
    local = [jnp.where((v >= 0) & (v < NE), v, -1) for v in local]
    mask = jnp.zeros((128, ALL), F32)
    for v in local:
        mask = jnp.where(v == sub, 1.0, mask)
    mask_b = mask.astype(BF16)
    before = (iota((ALL, ALL), 0) < iota((ALL, ALL), 1)).astype(BF16)
    rank = mm(mask_b, before)
    n_col = jnp.broadcast_to(jnp.sum(mask, axis=1, keepdims=True), (128, 128)).astype(I32)
    n_row = lax.dot_general(jnp.ones((8, ALL), BF16), mask_b, (((1,), (1,)), ((), ())),
                            preferred_element_type=F32).astype(I32)
    lower = (iota((128, 128), 1) < iota((128, 128), 0)).astype(BF16)
    upper = (iota((128, 128), 0) < iota((128, 128), 1)).astype(BF16)
    as_b = lambda v: v.astype(F32).astype(BF16)
    off_col = mm(lower, as_b((n_col + 15) >> 4)) * 16.0
    offc_col = mm(lower, as_b(n_col >> 4)) * 16.0 + mm(lower, as_b(n_col & 15))
    off_row = mm(as_b((n_row + 15) >> 4), upper).astype(I32)
    offc_row = (mm(as_b(n_row >> 4), upper) * 16.0 + mm(as_b(n_row & 15), upper)).astype(I32)
    real = iota((8, 128), 1) < NE
    table = [n_row, off_row, offc_row]
    for r in range(PARTS):
        lo = jnp.sum(jnp.where(real & (offc_row + n_row <= r * NR), 1.0, 0.0), axis=1, keepdims=True)
        hi = jnp.sum(jnp.where(real & (offc_row < (r + 1) * NR), 1.0, 0.0), axis=1, keepdims=True)
        table.append(jnp.where(iota((8, 128), 1) == 0, lo, hi).astype(I32))
    row = iota((8, 128), 0)
    packed = jnp.zeros((8, 128), I32)
    for i, v in enumerate(table):
        packed = jnp.where(row == i, v, packed)
    meta[...] = packed
    for base, off in ((0, off_col), (8, offc_col)):
        where_to = off[:, 0:1] + rank + 1.0
        for k in range(8):
            found = jnp.sum(jnp.where(local[k] == sub, where_to, 0.0), axis=0, keepdims=True)
            pos[base + k:base + k + 1, :] = (found - 1.0).astype(I32)


def attn_kernel(layer, first, *refs):
    if first:
        (x_ref, len_ref, idt_ref, k_ref, v_ref, wq_ref, wk_ref, wv_ref, wo_ref, a_ref, ida_ref, meta_ref, pos_ref, *scr) = refs
    else:
        (x_ref, len_ref, k_ref, v_ref, wq_ref, wk_ref, wv_ref, wo_ref, a_ref, *scr) = refs
    (kbuf, vbuf, wq_v, wk_v, wv_v, wo_v, q2d, kn2d, vn2d, num, nrec, stat, ssend, srec,
     kv_sem, w_sem, ns_sem, nr_sem, ss_sem, sr_sem, gs_sem, gr_sem, is_sem, ir_sem) = scr
    p, e, e_x, e_d, e_z, dev_y, dev_x, dev_d, dev_z = peers()

    def tok_of(c):
        first_half = (1 - p) * HALF + c * CH
        second_half = p * HALF + (c - NCH // 2) * CH
        return pl.multiple_of(jnp.where(c < NCH // 2, first_half, second_half), CH)

    def kv_copies(c):
        slot = c & (NB - 1)
        src = pl.ds(tok_of(c), CH)
        return (pltpu.make_async_copy(k_ref.at[layer, src], kbuf.at[slot], kv_sem.at[0, slot]),
                pltpu.make_async_copy(v_ref.at[layer, src], vbuf.at[slot], kv_sem.at[1, slot]))

    weights = [pltpu.make_async_copy(r.at[layer], b, w_sem.at[i])
               for i, (r, b) in enumerate(((wq_ref, wq_v), (wk_ref, wk_v), (wv_ref, wv_v), (wo_ref, wo_v)))]
    for cp in weights[:3]:
        cp.start()
    for c in range(2):
        for cp in kv_copies(jnp.int32(c)):
            cp.start()

    entry_barrier((dev_y, dev_x, dev_d, dev_z))

    id_copies = []
    if first:
        mine = (slice(None), slice(None), pl.ds(pl.multiple_of(e * T, T), T))
        ida_ref[mine] = idt_ref[...]
        for i, dev in enumerate((dev_x, dev_d, dev_z)):
            id_copies.append(remote(idt_ref, ida_ref.at[mine], is_sem.at[i], ir_sem.at[i], dev))
            id_copies[-1].start()

    normed = rms(x_ref[...]).astype(BF16)
    for cp in weights[:3]:
        cp.wait()
    for c in range(2, NB):
        for cp in kv_copies(jnp.int32(c)):
            cp.start()
    weights[3].start()
    for hp in range(H // 2):
        pair = mm(normed, wq_v[:, hp * 256:(hp + 1) * 256]).astype(BF16).astype(F32)
        for i in range(2):
            q2d[pl.ds(hp * 2 + i, T, stride=H), :] = pair[:, i * HD:(i + 1) * HD]
    for w, dst in ((wk_v, kn2d), (wv_v, vn2d)):
        pair = mm(normed, w[...]).astype(BF16).astype(F32)
        for i in range(KV):
            dst[pl.ds(i, T, stride=KV), :] = pair[:, i * HD:(i + 1) * HD]

    scale = HD ** -0.5
    col = iota((H, ROWS), 1)
    group_ok = (col & 1) == (iota((H, ROWS), 0) // (H // KV))
    col_pos = jnp.where(group_ok, col >> 1, 1 << 30)
    lane = iota((H, T), 1)

    def heads_of(ref, tok):
        two = ref[pl.ds(tok * KV, KV), :]
        return jnp.concatenate([jnp.broadcast_to(two[i:i + 1], (H // KV, HD)) for i in range(KV)], axis=0)

    def num_copy(c):
        rows = pl.ds(pl.multiple_of(c * (CH * H), CH * H), CH * H)
        return remote(num.at[rows], nrec.at[rows], ns_sem.at[c], nr_sem.at[c], dev_y)

    stat_copy = remote(ssend, srec, ss_sem, sr_sem, dev_y)

    def chunk(c, carry):
        slot = c & (NB - 1)
        for cp in kv_copies(c):
            cp.wait()
        tok0 = tok_of(c)
        m_all, l_all, n_all = stat[0], stat[1], stat[2]
        for j0 in range(0, CH, 4):
            group = range(j0, j0 + 4)
            qs, ss = {}, {}
            for j in group:
                qs[j] = q2d[pl.ds(pl.multiple_of((tok0 + j) * H, H), H), :]
                ss[j] = lax.dot_general(qs[j].astype(BF16), kbuf[slot, j], (((1,), (1,)), ((), ())),
                                        preferred_element_type=F32) * scale
            ps = {}
            for j in group:
                limit = len_ref[tok0 + j] - p * POS
                s = jnp.where(col_pos < limit, ss[j], -1e30)
                s_new = jnp.sum(qs[j] * heads_of(kn2d, tok0 + j), axis=1, keepdims=True) * scale
                m = jnp.maximum(jnp.max(s, axis=1, keepdims=True), s_new)
                pr = jnp.exp(s - m)
                ps[j] = pr.astype(BF16)
                here = lane == c * CH + j
                m_all = jnp.where(here, m, m_all)
                l_all = jnp.where(here, jnp.sum(pr, axis=1, keepdims=True), l_all)
                n_all = jnp.where(here, s_new, n_all)
            for j in group:
                num[pl.ds(pl.multiple_of((c * CH + j) * H, H), H), :] = mm(ps[j], vbuf[slot, j])
        stat[0], stat[1], stat[2] = m_all, l_all, n_all

        @pl.when(c + NB < NCH)
        def _():
            for cp in kv_copies(c + NB):
                cp.start()

        @pl.when(c == NCH // 2 - 1)
        def _():
            ssend[0], ssend[1] = m_all, l_all

        @pl.when((c >= 1) & (c <= NCH // 2))
        def _():
            num_copy(c - 1).start()

        @pl.when(c == NCH // 2)
        def _():
            stat_copy.start()

        return carry

    stat[...] = jnp.zeros_like(stat)
    lax.fori_loop(0, NCH, chunk, 0)

    weights[3].wait()
    stat_copy.wait()
    m_own, l_own, s_new = stat[0], stat[1], stat[2]
    m_far = pltpu.roll(srec[0], HALF, axis=1)
    l_far = pltpu.roll(srec[1], HALF, axis=1)
    m = jnp.maximum(m_own, m_far)
    w_own, w_far, w_new = jnp.exp(m_own - m), jnp.exp(m_far - m), jnp.exp(s_new - m)
    denom = l_own * w_own + l_far * w_far + w_new
    c_own, c_far, c_new = w_own / denom, w_far / denom, w_new / denom

    def combine(c, carry):
        num_copy(c).wait()
        for j in range(CH):
            i = c * CH + j
            pick = lane == HALF + i
            own, far, new = [jnp.sum(jnp.where(pick, v, 0.0), axis=1, keepdims=True) for v in (c_own, c_far, c_new)]
            there = pl.ds(pl.multiple_of(i * H, H), H)
            here = pl.ds(pl.multiple_of((HALF + i) * H, H), H)
            num[here, :] = num[here, :] * own + nrec[there, :] * far + heads_of(vn2d, p * HALF + i) * new
        return carry

    lax.fori_loop(0, NCH // 2, combine, 0)

    proj = jnp.zeros((HALF, D), F32)
    for hp in range(H // 2):
        pair = jnp.concatenate([num[pl.ds(HALF * H + hp * 2 + i, HALF, stride=H), :].astype(BF16) for i in range(2)], axis=1)
        proj = proj + mm(pair, wo_v[hp * 256:(hp + 1) * 256, :])
    mine = pl.ds(pl.multiple_of(p * HALF, HALF), HALF)

    def rows(pp, ee):
        return pl.ds(pl.multiple_of(ee * T + pp * HALF, HALF), HALF)

    a_ref[rows(p, e), :] = (x_ref[mine, :].astype(F32) + proj).astype(BF16)

    def gather(i, pp, ee, dev):
        block = a_ref.at[rows(pp, ee)]
        cp = remote(block, block, gs_sem.at[i], gr_sem.at[i], dev)
        cp.start()
        return cp

    copies = [gather(0, p, e, dev_y), gather(1, p, e, dev_x), gather(2, p, e, dev_d)]
    if first:
        for cp in id_copies:
            cp.wait()
        for n in range(ida_ref.shape[0]):
            route(ida_ref.at[n], e, meta_ref.at[n], pos_ref.at[n])
    copies[0].wait_recv()
    copies += [gather(3, 1 - p, e, dev_x), gather(4, 1 - p, e, dev_d)]
    copies[1].wait_recv()
    copies += [gather(5, p, e_x, dev_d)]
    copies[3].wait_recv()
    copies += [gather(6, 1 - p, e_x, dev_d)]
    for i in (2, 4, 5, 6):
        copies[i].wait_recv()
    for cp in copies:
        cp.wait_send()


def attention(layer, x, cache_len, id_t, k, v, wq, wk, wv, wo, cid):
    first = id_t is not None
    vm, sm, hb = (pl.BlockSpec(memory_space=m) for m in (pltpu.VMEM, pltpu.SMEM, pl.ANY))
    dma = pltpu.SemaphoreType.DMA
    outs = [jax.ShapeDtypeStruct((ALL, D), BF16)]
    if first:
        layers = id_t.shape[0]
        outs += [jax.ShapeDtypeStruct((layers, 8, ALL), I32), jax.ShapeDtypeStruct((layers, 8, 128), I32),
                 jax.ShapeDtypeStruct((layers, 16, ALL), I32)]
    out = pl.pallas_call(
        functools.partial(attn_kernel, layer, first),
        name=f"attn_{layer}",
        out_shape=outs,
        in_specs=[vm, sm] + ([vm] if first else []) + [hb] * 6,
        out_specs=[vm] * len(outs),
        scratch_shapes=[
            pltpu.VMEM((NB, CH, ROWS, HD), BF16), pltpu.VMEM((NB, CH, ROWS, HD), BF16),
            pltpu.VMEM((D, H * HD), BF16), pltpu.VMEM((D, KV * HD), BF16), pltpu.VMEM((D, KV * HD), BF16),
            pltpu.VMEM((H * HD, D), BF16),
            pltpu.VMEM((T * H, HD), F32), pltpu.VMEM((T * KV, HD), F32), pltpu.VMEM((T * KV, HD), F32),
            pltpu.VMEM((T * H, HD), F32), pltpu.VMEM((HALF * H, HD), F32),
            pltpu.VMEM((3, H, T), F32), pltpu.VMEM((2, H, T), F32), pltpu.VMEM((2, H, T), F32),
            dma((2, NB)), dma((4,)), dma((NCH // 2,)), dma((NCH // 2,)), dma(()), dma(()),
            dma((7,)), dma((7,)), dma((3,)), dma((3,)),
        ],
        compiler_params=pltpu.CompilerParams(collective_id=cid, has_side_effects=True, vmem_limit_bytes=VMEM_LIMIT),
    )(*([x, cache_len] + ([id_t] if first else []) + [k, v, wq, wk, wv, wo]))
    return out


def expert_kernel(layer, part, a_ref, meta, pos_ref, w1_ref, w3_ref, w2_ref, mine_ref, theirs_ref,
                  w1b, w3b, w2b, u, xs, ym, yt, tail, w_sem, o_sem):
    p = lax.axis_index("pool")
    r0 = part * NR
    lo, hi = meta[layer, 3 + part, 0], meta[layer, 3 + part, 1]

    def w_copies(i):
        slot = i & (NW - 1)
        return [pltpu.make_async_copy(r.at[layer, i], b.at[slot], w_sem.at[n, slot])
                for n, (r, b) in enumerate(((w1_ref, w1b), (w3_ref, w3b), (w2_ref, w2b)))]

    def start(i, carry):
        for cp in w_copies(i):
            cp.start()
        return carry

    lax.fori_loop(lo, jnp.minimum(lo + NW, hi), start, 0)

    u[...] = rms(a_ref[...]).astype(BF16)

    def dispatch(i, carry):
        row = iota((256, ALL), 0) + i * 256
        hit = jnp.zeros((256, ALL), F32)
        for k in range(8):
            hit = jnp.where(pos_ref[layer, k:k + 1, :] == row, 1.0, hit)
        xs[pl.ds(pl.multiple_of(i * 256, 256), 256), :] = mm(hit.astype(BF16), u[...]).astype(BF16)
        return carry

    lax.fori_loop(meta[layer, 1, lo] >> 4, (meta[layer, 1, hi] + 15) >> 4, dispatch, 0)

    def expert(i, carry):
        slot = i & (NW - 1)
        for cp in w_copies(i):
            cp.wait()
        n, off, offc = meta[layer, 0, i], meta[layer, 1, i], meta[layer, 2, i]

        def rows_step(j, c2):
            rows = xs[pl.ds(pl.multiple_of(off * 16 + j * MC, 16), MC), :]
            act = (jax.nn.silu(mm(rows, w1b[slot])) * mm(rows, w3b[slot])).astype(BF16)
            y = mm(act, w2b[slot])
            to = pl.ds(offc + j * MC + (PAD - r0), MC)
            for t in range(6):
                ym[t // 3, t % 3, to, :] = y[:, t * 128:(t + 1) * 128]
            yt[to, :] = y[:, 2 * CM:]
            return c2

        first = jnp.maximum(r0 - offc, 0) >> 5
        last = (jnp.minimum(n, r0 + NR - offc) + MC - 1) >> 5
        lax.fori_loop(first, last, rows_step, 0)

        @pl.when(i + NW < hi)
        def _():
            start(i + NW, 0)

        return carry

    lax.fori_loop(lo, hi, expert, 0)
    copies = []
    for n, (q, ref) in enumerate(((1 - p, theirs_ref), (p, mine_ref))):
        for t in range(3):
            copies.append(pltpu.make_async_copy(ym.at[q, t, pl.ds(PAD, NR)], ref.at[pl.ds(t * NR, NR)], o_sem.at[n, t]))
            copies[-1].start()
    top, bot = yt[PAD:PAD + NR // 2, :], yt[PAD + NR // 2:PAD + NR, :]
    left = iota((NR // 2, 128), 1) < 64
    tail[0] = jnp.where(left, top, pltpu.roll(bot, 64, axis=1))
    tail[1] = jnp.where(left, pltpu.roll(top, 64, axis=1), bot)
    for n, (q, ref) in enumerate(((1 - p, theirs_ref), (p, mine_ref))):
        copies.append(pltpu.make_async_copy(tail.at[q], ref.at[pl.ds(3 * NR, NR // 2)], o_sem.at[n, 3]))
        copies[-1].start()
    for cp in copies:
        cp.wait()


def experts(layer, part, a_all, meta, pos, w1, w3, w2):
    vm, sm, hb = (pl.BlockSpec(memory_space=m) for m in (pltpu.VMEM, pltpu.SMEM, pl.ANY))
    dma = pltpu.SemaphoreType.DMA
    return pl.pallas_call(
        functools.partial(expert_kernel, layer, part),
        name=f"experts_{layer}_{part}",
        out_shape=[jax.ShapeDtypeStruct((PR, 128), F32)] * 2,
        in_specs=[vm, sm, vm, hb, hb, hb],
        out_specs=[hb, hb],
        scratch_shapes=[
            pltpu.VMEM((NW, D, FF), BF16), pltpu.VMEM((NW, D, FF), BF16), pltpu.VMEM((NW, FF, D), BF16),
            pltpu.VMEM((ALL, D), BF16), pltpu.VMEM((2304, D), BF16),
            pltpu.VMEM((2, 3, NR + 2 * PAD, 128), F32), pltpu.VMEM((NR + 2 * PAD, 128), F32),
            pltpu.VMEM((2, NR // 2, 128), F32),
            dma((3, NW)), dma((2, 4)),
        ],
        compiler_params=pltpu.CompilerParams(vmem_limit_bytes=VMEM_LIMIT),
        cost_estimate=pl.CostEstimate(flops=4_000_000_000, bytes_accessed=44_000_000 // PARTS, transcendentals=PAIRS * FF // PARTS),
    )(a_all, meta, pos, w1, w3, w2)


def merge_kernel(layer, a_ref, id_ref, pos_ref, mine0_ref, far0_ref, mine1_ref, theirs1_ref, wr_ref, x_ref,
                 y_own, y_far, wr, gate, base, acc, back, xsend, xfar,
                 l_sem, ys_sem, yr_sem, bs_sem, br_sem, fs_sem, fr_sem):
    p, e, e_x, e_d, e_z, dev_y, dev_x, dev_d, dev_z = peers()
    loads = [pltpu.make_async_copy(src, dst, l_sem.at[i])
             for i, (src, dst) in enumerate(((wr_ref.at[layer], wr), (mine0_ref, y_own.at[0]), (far0_ref, y_far.at[0]),
                                             (mine1_ref, y_own.at[1])))]
    for cp in loads:
        cp.start()
    entry_barrier((dev_y, dev_x, dev_d, dev_z))
    spans = [(t * NR, NR) for t in range(3)] + [(3 * NR, NR // 2)]
    y_copies = [remote(theirs1_ref.at[pl.ds(b, n)], y_far.at[1, pl.ds(b, n)], ys_sem.at[t], yr_sem.at[t], dev_y)
                for t, (b, n) in enumerate(spans)]
    for cp in y_copies:
        cp.start()

    loads[0].wait()
    u = rms(a_ref[...]).astype(BF16)
    logits = jnp.zeros((ALL, 256), F32)
    rest = wr[...]
    for _ in range(3):
        part = rest.astype(BF16)
        rest = rest - part.astype(F32)
        logits = logits + mm(u, part)
    col = iota((ALL, 256), 1)
    g = [jnp.sum(jnp.where(id_ref[layer, :, k:k + 1] == col, logits, 0.0), axis=1, keepdims=True) for k in range(8)]
    top = functools.reduce(jnp.maximum, g)
    g = [jnp.exp(v - top) for v in g]
    total = functools.reduce(jnp.add, g)
    g = [v / total for v in g]
    pos = [pos_ref[layer, :, 8 + k:9 + k] for k in range(8)]
    lane = iota((ALL, 128), 1)
    for c in range(PAIRS // 128):
        w = jnp.zeros((ALL, 128), F32)
        for k in range(8):
            w = jnp.where(pos[k] == lane + c * 128, g[k], w)
        for i in range(3):
            part = w.astype(BF16)
            w = w - part.astype(F32)
            gate[i, :, c * 128:(c + 1) * 128] = part

    def mix(h, t):
        b, n = spans[t]
        y = (y_own[h, b:b + n, :] + y_far[h, b:b + n, :]).astype(BF16)
        first = h * NR
        if t < 3:
            return sum(mm(gate[i, :, first:first + NR], y) for i in range(3))
        lo, hi = [sum(mm(gate[i, :, first + q * n:first + (q + 1) * n], y) for i in range(3)) for q in range(2)]
        keep = jnp.broadcast_to(p == 0, lo.shape)
        return jnp.where(keep, lo, pltpu.roll(lo, 64, axis=1)) + jnp.where(keep, pltpu.roll(hi, 64, axis=1), hi)

    loads[1].wait()
    loads[2].wait()
    for t in range(4):
        base[t] = mix(0, t)
    loads[3].wait()

    def block_of(ee):
        return pl.ds(pl.multiple_of(ee * T, T), T)

    def give(t):
        cps = [remote(acc.at[t, block_of(ee)], back.at[t, i], bs_sem.at[t, i], br_sem.at[t, i], dev)
               for i, (ee, dev) in enumerate(((e_x, dev_x), (e_z, dev_z), (e_d, dev_d)))]
        for cp in cps:
            cp.start()
        return cps

    def cols(q, t):
        return pl.ds(pl.multiple_of(q * CM + t * 128, 128), 128) if t < 3 else slice(2 * CM, D)

    def finish(t, cps):
        for cp in cps:
            cp.wait_recv()
        total = acc[t, block_of(e), :] + back[t, 0] + back[t, 1] + back[t, 2]
        xsend[t] = (a_ref[block_of(e), cols(p, t)].astype(F32) + total).astype(BF16)
        cp = remote(xsend.at[t], xfar.at[t], fs_sem.at[t], fr_sem.at[t], dev_y)
        cp.start()
        return cp

    given, sent = [], []
    for t in range(4):
        y_copies[t].wait_recv()
        acc[t] = base[t] + mix(1, t)
        given.append(give(t))
        if t >= 1:
            sent.append(finish(t - 1, given[t - 1]))
    sent.append(finish(3, given[3]))
    for t in range(3):
        x_ref[:, cols(p, t)] = xsend[t]
        sent[t].wait()
        x_ref[:, cols(1 - p, t)] = xfar[t]
    sent[3].wait()
    keep_own = (iota((T, 128), 1) // 64) == p
    x_ref[:, 2 * CM:] = jnp.where(keep_own, xsend[3].astype(F32), xfar[3].astype(F32)).astype(BF16)
    for cp in y_copies + [c for cps in given for c in cps]:
        cp.wait_send()


def merge(layer, a_all, ids, pos, mine0, far0, mine1, theirs1, wr, cid):
    vm, hb = (pl.BlockSpec(memory_space=m) for m in (pltpu.VMEM, pl.ANY))
    dma = pltpu.SemaphoreType.DMA
    return pl.pallas_call(
        functools.partial(merge_kernel, layer),
        name=f"merge_{layer}",
        out_shape=jax.ShapeDtypeStruct((T, D), BF16),
        in_specs=[vm, vm, vm, hb, hb, hb, hb, hb],
        out_specs=vm,
        scratch_shapes=[
            pltpu.VMEM((2, PR, 128), F32), pltpu.VMEM((2, PR, 128), F32),
            pltpu.VMEM((D, 256), F32), pltpu.VMEM((3, ALL, PAIRS), BF16),
            pltpu.VMEM((4, ALL, 128), F32), pltpu.VMEM((4, ALL, 128), F32), pltpu.VMEM((4, 3, T, 128), F32),
            pltpu.VMEM((4, T, 128), BF16), pltpu.VMEM((4, T, 128), BF16),
            dma((4,)), dma((4,)), dma((4,)), dma((4, 3)), dma((4, 3)), dma((4,)), dma((4,)),
        ],
        compiler_params=pltpu.CompilerParams(collective_id=cid, has_side_effects=True, vmem_limit_bytes=VMEM_LIMIT),
    )(a_all, ids, pos, mine0, far0, mine1, theirs1, wr)


def solution(mesh):
    tok_spec = P(('dp', 'ep'), None)
    cache_spec = P(None, ('dp', 'ep'), 'pool', None, None)
    up_spec = P(None, 'ep', None, 'pool')
    down_spec = P(None, 'ep', 'pool', None)
    in_specs = (tok_spec, cache_spec, cache_spec, P(('dp', 'ep')), P(), P(), P(), P(), P(), P(None, ('dp', 'ep'), None),
                up_spec, up_spec, down_spec)

    def body(hidden, k_cache, v_cache, cache_len, w_q, w_k, w_v, w_o, w_router, expert_ids, w_one, w_three, w_two):
        layers = w_q.shape[0]
        k = k_cache.reshape(layers, T, ROWS, HD)
        v = v_cache.reshape(layers, T, ROWS, HD)
        id_t = jnp.swapaxes(expert_ids, 1, 2)
        for layer in range(layers):
            a_all, *extra = attention(layer, hidden, cache_len, id_t if layer == 0 else None, k, v, w_q, w_k, w_v, w_o, 2 * layer)
            if layer == 0:
                ids_t, meta, pos_t = extra
                ids, pos = jnp.swapaxes(ids_t, 1, 2), jnp.swapaxes(pos_t, 1, 2)
            mine0, theirs0 = experts(layer, 0, a_all, meta, pos_t, w_one, w_three, w_two)
            far0 = lax.ppermute(theirs0, 'pool', [(0, 1), (1, 0)])
            mine1, theirs1 = experts(layer, 1, a_all, meta, pos_t, w_one, w_three, w_two)
            hidden = merge(layer, a_all, ids, pos, mine0, far0, mine1, theirs1, w_router, 2 * layer + 1)
        return hidden

    return jax.shard_map(body, mesh=mesh, in_specs=in_specs, out_specs=tok_spec, check_vma=False)
```

```python
import functools

import jax
import jax.numpy as jnp
from jax import lax
from jax.experimental import pallas as pl
from jax.experimental.pallas import tpu as pltpu
from jax.sharding import PartitionSpec as P

MESH = pl.DeviceIdType.MESH
F32, BF16, I32 = jnp.float32, jnp.bfloat16, jnp.int32
NORM_EPS = 1e-6
T, D, HD, H = 128, 896, 128, 16
HALF = T // 2
KV = 2
POS = 256
ROWS = POS * KV
CH = 8
NCH = T // CH
NB = 8
ALL = 4 * T
NE = 64
PAIRS = 1024
FF = 128
NW = 32
MC = 32
CM = 384
PARTS = 2
NR = PAIRS // PARTS
PR = 3 * NR + NR // 2
PAD = MC
MIB = 1024 * 1024


def rms(v):
    v = v.astype(F32)
    return v * lax.rsqrt(jnp.mean(v * v, axis=-1, keepdims=True) + NORM_EPS)


def mm(a, b):
    return jnp.dot(a, b, preferred_element_type=F32)


def iota(shape, dim):
    return lax.broadcasted_iota(I32, shape, dim)


def peers():
    g, p, e = lax.axis_index("dp"), lax.axis_index("pool"), lax.axis_index("ep")
    core = lax.rem(e, 2)
    e_x = lax.rem(e + 2, 4)
    e_d = e + 1 - 2 * core
    e_z = lax.rem(e_d + 2, 4)
    return p, e, e_x, e_d, e_z, (g, 1 - p, e), (g, p, e_x), (g, p, e_d), (g, p, e_z), (g, 1 - p, e_x)


def entry_barrier(targets):
    bar = pltpu.get_barrier_semaphore()
    for dev in targets:
        pl.semaphore_signal(bar, inc=1, device_id=dev, device_id_type=MESH)
    pl.semaphore_wait(bar, len(targets))


def remote(src, dst, send_sem, recv_sem, dev):
    return pltpu.make_async_remote_copy(src_ref=src, dst_ref=dst, send_sem=send_sem, recv_sem=recv_sem,
                                        device_id=dev, device_id_type=MESH)


def route(ids, e, meta, pos):
    sub = iota((128, ALL), 0)
    local = [ids[k:k + 1, :] - e * NE for k in range(8)]
    local = [jnp.where((v >= 0) & (v < NE), v, -1) for v in local]
    mask = jnp.zeros((128, ALL), F32)
    for v in local:
        mask = jnp.where(v == sub, 1.0, mask)
    mask_b = mask.astype(BF16)
    before = (iota((ALL, ALL), 0) < iota((ALL, ALL), 1)).astype(BF16)
    rank = mm(mask_b, before)
    n_col = jnp.broadcast_to(jnp.sum(mask, axis=1, keepdims=True), (128, 128)).astype(I32)
    n_row = lax.dot_general(jnp.ones((8, ALL), BF16), mask_b, (((1,), (1,)), ((), ())),
                            preferred_element_type=F32).astype(I32)
    lower = (iota((128, 128), 1) < iota((128, 128), 0)).astype(BF16)
    upper = (iota((128, 128), 0) < iota((128, 128), 1)).astype(BF16)
    as_b = lambda v: v.astype(F32).astype(BF16)
    off_col = mm(lower, as_b((n_col + 15) >> 4)) * 16.0
    offc_col = mm(lower, as_b(n_col >> 4)) * 16.0 + mm(lower, as_b(n_col & 15))
    off_row = mm(as_b((n_row + 15) >> 4), upper).astype(I32)
    offc_row = (mm(as_b(n_row >> 4), upper) * 16.0 + mm(as_b(n_row & 15), upper)).astype(I32)
    real = iota((8, 128), 1) < NE
    table = [n_row, off_row, offc_row]
    for r in range(PARTS):
        lo = jnp.sum(jnp.where(real & (offc_row + n_row <= r * NR), 1.0, 0.0), axis=1, keepdims=True)
        hi = jnp.sum(jnp.where(real & (offc_row < (r + 1) * NR), 1.0, 0.0), axis=1, keepdims=True)
        table.append(jnp.where(iota((8, 128), 1) == 0, lo, hi).astype(I32))
    row = iota((8, 128), 0)
    packed = jnp.zeros((8, 128), I32)
    for i, v in enumerate(table):
        packed = jnp.where(row == i, v, packed)
    meta[...] = packed
    for base, off in ((0, off_col), (8, offc_col)):
        where_to = off[:, 0:1] + rank + 1.0
        for k in range(8):
            found = jnp.sum(jnp.where(local[k] == sub, where_to, 0.0), axis=0, keepdims=True)
            pos[base + k:base + k + 1, :] = (found - 1.0).astype(I32)


def attn_kernel(layer, first, *refs):
    if first:
        (x_ref, len_ref, idt_ref, k_ref, v_ref, wq_ref, wk_ref, wv_ref, wo_ref, a_ref, ida_ref, meta_ref, pos_ref, *scr) = refs
    else:
        (x_ref, len_ref, k_ref, v_ref, wq_ref, wk_ref, wv_ref, wo_ref, a_ref, *scr) = refs
    (kbuf, vbuf, wq_v, wk_v, wv_v, wo_v, q2d, kn2d, vn2d, num, nrec, stat, ssend, srec,
     kv_sem, w_sem, ns_sem, nr_sem, ss_sem, sr_sem, gs_sem, gr_sem, is_sem, ir_sem) = scr
    p, e, e_x, e_d, e_z, dev_y, dev_x, dev_d, dev_z, dev_yx = peers()

    def tok_of(c):
        first_half = (1 - p) * HALF + c * CH
        second_half = p * HALF + (c - NCH // 2) * CH
        return pl.multiple_of(jnp.where(c < NCH // 2, first_half, second_half), CH)

    def kv_copies(c):
        slot = c & (NB - 1)
        src = pl.ds(tok_of(c), CH)
        return (pltpu.make_async_copy(k_ref.at[layer, src], kbuf.at[slot], kv_sem.at[0, slot]),
                pltpu.make_async_copy(v_ref.at[layer, src], vbuf.at[slot], kv_sem.at[1, slot]))

    weights = [pltpu.make_async_copy(r.at[layer], b, w_sem.at[i])
               for i, (r, b) in enumerate(((wq_ref, wq_v), (wk_ref, wk_v), (wv_ref, wv_v), (wo_ref, wo_v)))]
    for cp in weights[:3]:
        cp.start()
    for c in range(2):
        for cp in kv_copies(jnp.int32(c)):
            cp.start()

    entry_barrier((dev_y, dev_x, dev_d, dev_z, dev_yx))

    id_copies = []
    if first:
        mine = (slice(None), slice(None), pl.ds(pl.multiple_of(e * T, T), T))
        ida_ref[mine] = idt_ref[...]
        for i, dev in enumerate((dev_x, dev_d, dev_z)):
            id_copies.append(remote(idt_ref, ida_ref.at[mine], is_sem.at[i], ir_sem.at[i], dev))
            id_copies[-1].start()

    normed = rms(x_ref[...]).astype(BF16)
    for cp in weights[:3]:
        cp.wait()
    for c in range(2, NB):
        for cp in kv_copies(jnp.int32(c)):
            cp.start()
    weights[3].start()
    for hp in range(H // 2):
        pair = mm(normed, wq_v[:, hp * 256:(hp + 1) * 256]).astype(BF16).astype(F32)
        for i in range(2):
            q2d[pl.ds(hp * 2 + i, T, stride=H), :] = pair[:, i * HD:(i + 1) * HD]
    for w, dst in ((wk_v, kn2d), (wv_v, vn2d)):
        pair = mm(normed, w[...]).astype(BF16).astype(F32)
        for i in range(KV):
            dst[pl.ds(i, T, stride=KV), :] = pair[:, i * HD:(i + 1) * HD]

    scale = HD ** -0.5
    col = iota((H, ROWS), 1)
    group_ok = (col & 1) == (iota((H, ROWS), 0) // (H // KV))
    col_pos = jnp.where(group_ok, col >> 1, 1 << 30)
    lane = iota((H, T), 1)

    def heads_of(ref, tok):
        two = ref[pl.ds(tok * KV, KV), :]
        return jnp.concatenate([jnp.broadcast_to(two[i:i + 1], (H // KV, HD)) for i in range(KV)], axis=0)

    def num_copy(c):
        rows = pl.ds(pl.multiple_of(c * (CH * H), CH * H), CH * H)
        return remote(num.at[rows], nrec.at[rows], ns_sem.at[c], nr_sem.at[c], dev_y)

    stat_copy = remote(ssend, srec, ss_sem, sr_sem, dev_y)

    def chunk(c, carry):
        slot = c & (NB - 1)
        for cp in kv_copies(c):
            cp.wait()
        tok0 = tok_of(c)
        m_all, l_all, n_all = stat[0], stat[1], stat[2]
        for j0 in range(0, CH, 4):
            group = range(j0, j0 + 4)
            qs, ss = {}, {}
            for j in group:
                qs[j] = q2d[pl.ds(pl.multiple_of((tok0 + j) * H, H), H), :]
                ss[j] = lax.dot_general(qs[j].astype(BF16), kbuf[slot, j], (((1,), (1,)), ((), ())),
                                        preferred_element_type=F32) * scale
            ps = {}
            for j in group:
                limit = len_ref[tok0 + j] - p * POS
                s = jnp.where(col_pos < limit, ss[j], -1e30)
                s_new = jnp.sum(qs[j] * heads_of(kn2d, tok0 + j), axis=1, keepdims=True) * scale
                m = jnp.maximum(jnp.max(s, axis=1, keepdims=True), s_new)
                pr = jnp.exp(s - m)
                ps[j] = pr.astype(BF16)
                here = lane == c * CH + j
                m_all = jnp.where(here, m, m_all)
                l_all = jnp.where(here, jnp.sum(pr, axis=1, keepdims=True), l_all)
                n_all = jnp.where(here, s_new, n_all)
            for j in group:
                num[pl.ds(pl.multiple_of((c * CH + j) * H, H), H), :] = mm(ps[j], vbuf[slot, j])
        stat[0], stat[1], stat[2] = m_all, l_all, n_all

        @pl.when(c + NB < NCH)
        def _():
            for cp in kv_copies(c + NB):
                cp.start()

        @pl.when(c == NCH // 2 - 1)
        def _():
            ssend[0], ssend[1] = m_all, l_all

        @pl.when((c >= 1) & (c <= NCH // 2))
        def _():
            num_copy(c - 1).start()

        @pl.when(c == NCH // 2)
        def _():
            stat_copy.start()

        return carry

    stat[...] = jnp.zeros_like(stat)
    lax.fori_loop(0, NCH, chunk, 0)

    weights[3].wait()
    stat_copy.wait()
    m_own, l_own, s_new = stat[0], stat[1], stat[2]
    m_far = pltpu.roll(srec[0], HALF, axis=1)
    l_far = pltpu.roll(srec[1], HALF, axis=1)
    m = jnp.maximum(m_own, m_far)
    w_own, w_far, w_new = jnp.exp(m_own - m), jnp.exp(m_far - m), jnp.exp(s_new - m)
    denom = l_own * w_own + l_far * w_far + w_new
    c_own, c_far, c_new = w_own / denom, w_far / denom, w_new / denom

    def combine(c, carry):
        num_copy(c).wait()
        for j in range(CH):
            i = c * CH + j
            pick = lane == HALF + i
            own, far, new = [jnp.sum(jnp.where(pick, v, 0.0), axis=1, keepdims=True) for v in (c_own, c_far, c_new)]
            there = pl.ds(pl.multiple_of(i * H, H), H)
            here = pl.ds(pl.multiple_of((HALF + i) * H, H), H)
            num[here, :] = num[here, :] * own + nrec[there, :] * far + heads_of(vn2d, p * HALF + i) * new
        return carry

    lax.fori_loop(0, NCH // 2, combine, 0)

    proj = jnp.zeros((HALF, D), F32)
    for hp in range(H // 2):
        pair = jnp.concatenate([num[pl.ds(HALF * H + hp * 2 + i, HALF, stride=H), :].astype(BF16) for i in range(2)], axis=1)
        proj = proj + mm(pair, wo_v[hp * 256:(hp + 1) * 256, :])
    mine = pl.ds(pl.multiple_of(p * HALF, HALF), HALF)

    def rows(pp, ee):
        return pl.ds(pl.multiple_of(ee * T + pp * HALF, HALF), HALF)

    a_ref[rows(p, e), :] = (x_ref[mine, :].astype(F32) + proj).astype(BF16)

    def gather(i, pp, ee, dev):
        block = a_ref.at[rows(pp, ee)]
        cp = remote(block, block, gs_sem.at[i], gr_sem.at[i], dev)
        cp.start()
        return cp

    copies = [gather(0, p, e, dev_yx), gather(1, p, e, dev_x), gather(2, p, e, dev_y), gather(3, p, e, dev_d)]
    if first:
        for cp in id_copies:
            cp.wait()
        for n in range(ida_ref.shape[0]):
            route(ida_ref.at[n], e, meta_ref.at[n], pos_ref.at[n])
    for i, pp, ee in ((2, 1 - p, e), (1, p, e_x), (0, 1 - p, e_x)):
        copies[i].wait_recv()
        copies.append(gather(len(copies), pp, ee, dev_d))
    for i in range(3, 7):
        copies[i].wait_recv()
    for cp in copies:
        cp.wait_send()


def attention(layer, x, cache_len, id_t, k, v, wq, wk, wv, wo, cid):
    first = id_t is not None
    vm, sm, hb = (pl.BlockSpec(memory_space=m) for m in (pltpu.VMEM, pltpu.SMEM, pltpu.HBM))
    dma = pltpu.SemaphoreType.DMA
    outs = [jax.ShapeDtypeStruct((ALL, D), BF16)]
    if first:
        layers = id_t.shape[0]
        outs += [jax.ShapeDtypeStruct((layers, 8, ALL), I32), jax.ShapeDtypeStruct((layers, 8, 128), I32),
                 jax.ShapeDtypeStruct((layers, 16, ALL), I32)]
    out = pl.pallas_call(
        functools.partial(attn_kernel, layer, first),
        name=f"attn_{layer}",
        out_shape=outs,
        in_specs=[vm, sm] + ([vm] if first else []) + [hb] * 6,
        out_specs=[vm] * len(outs),
        scratch_shapes=[
            pltpu.VMEM((NB, CH, ROWS, HD), BF16), pltpu.VMEM((NB, CH, ROWS, HD), BF16),
            pltpu.VMEM((D, H * HD), BF16), pltpu.VMEM((D, KV * HD), BF16), pltpu.VMEM((D, KV * HD), BF16),
            pltpu.VMEM((H * HD, D), BF16),
            pltpu.VMEM((T * H, HD), F32), pltpu.VMEM((T * KV, HD), F32), pltpu.VMEM((T * KV, HD), F32),
            pltpu.VMEM((T * H, HD), F32), pltpu.VMEM((HALF * H, HD), F32),
            pltpu.VMEM((3, H, T), F32), pltpu.VMEM((2, H, T), F32), pltpu.VMEM((2, H, T), F32),
            dma((2, NB)), dma((4,)), dma((NCH // 2,)), dma((NCH // 2,)), dma(()), dma(()),
            dma((7,)), dma((7,)), dma((3,)), dma((3,)),
        ],
        compiler_params=pltpu.CompilerParams(collective_id=cid, has_side_effects=True, vmem_limit_bytes=61 * MIB),
    )(*([x, cache_len] + ([id_t] if first else []) + [k, v, wq, wk, wv, wo]))
    return out


def expert_kernel(layer, part, a_ref, meta, pos_ref, w1_ref, w3_ref, w2_ref, mine_ref, theirs_ref,
                  w1b, w3b, w2b, u, xs, ym, yt, tail, w_sem, o_sem):
    p = lax.axis_index("pool")
    r0 = part * NR
    lo, hi = meta[layer, 3 + part, 0], meta[layer, 3 + part, 1]
    odd = (hi - lo) & 1
    lo, hi = jnp.where((odd == 1) & (hi == NE), lo - 1, lo), jnp.where((odd == 1) & (hi < NE), hi + 1, hi)

    def w_copies(i):
        slot = i & (NW - 1)
        return [pltpu.make_async_copy(r.at[layer, i], b.at[slot], w_sem.at[n, slot])
                for n, (r, b) in enumerate(((w1_ref, w1b), (w3_ref, w3b), (w2_ref, w2b)))]

    def start(i, carry):
        for cp in w_copies(i):
            cp.start()
        return carry

    lax.fori_loop(lo, jnp.minimum(lo + NW, hi), start, 0)

    u[...] = rms(a_ref[...]).astype(BF16)

    def dispatch(i, carry):
        row = iota((256, ALL), 0) + i * 256
        hit = jnp.zeros((256, ALL), F32)
        for k in range(8):
            hit = jnp.where(pos_ref[layer, k:k + 1, :] == row, 1.0, hit)
        xs[pl.ds(pl.multiple_of(i * 256, 256), 256), :] = mm(hit.astype(BF16), u[...]).astype(BF16)
        return carry

    lax.fori_loop(meta[layer, 1, lo] >> 4, (meta[layer, 1, hi] + 15) >> 4, dispatch, 0)

    def rows_at(i, j):
        slot = i & (NW - 1)
        rows = xs[pl.ds(pl.multiple_of(meta[layer, 1, i] * 16 + j * MC, 16), MC), :]
        act = (jax.nn.silu(mm(rows, w1b[slot])) * mm(rows, w3b[slot])).astype(BF16)
        return mm(act, w2b[slot]), pl.ds(jnp.minimum(meta[layer, 2, i] + j * MC - r0, NR) + PAD, MC)

    def targets(to):
        return [ym.at[t // 3, t % 3, to] for t in range(6)] + [yt.at[to]]

    def first_step(i):
        return jnp.maximum(r0 - meta[layer, 2, i], 0) >> 5

    def more_steps(i):
        n, offc, first = meta[layer, 0, i], meta[layer, 2, i], first_step(i)

        def step(j, carry):
            y, to = rows_at(i, j)
            keep = iota((MC, 128), 0) < n - j * MC
            for t, ref in enumerate(targets(to)):
                ref[...] = jnp.where(keep, y[:, t * 128:(t + 1) * 128], ref[...])
            return carry

        lax.fori_loop(first + 1, (jnp.minimum(n, r0 + NR - offc) + MC - 1) >> 5, step, 0)

    def expert_pair(h, carry):
        pair = [lo + 2 * h, lo + 2 * h + 1]
        for i in pair:
            for cp in w_copies(i):
                cp.wait()
        done = [rows_at(i, first_step(i)) for i in pair]
        for y, to in done:
            for t, ref in enumerate(targets(to)):
                ref[...] = y[:, t * 128:(t + 1) * 128]
        for i in pair:
            more_steps(i)
        for i in pair:
            @pl.when(i + NW < hi)
            def _():
                start(i + NW, 0)
        return carry

    lax.fori_loop(0, (hi - lo) >> 1, expert_pair, 0)
    copies = []
    for n, (q, ref) in enumerate(((1 - p, theirs_ref), (p, mine_ref))):
        for t in range(3):
            copies.append(pltpu.make_async_copy(ym.at[q, t, pl.ds(PAD, NR)], ref.at[pl.ds(t * NR, NR)], o_sem.at[n, t]))
            copies[-1].start()
    top, bot = yt[PAD:PAD + NR // 2, :], yt[PAD + NR // 2:PAD + NR, :]
    left = iota((NR // 2, 128), 1) < 64
    tail[0] = jnp.where(left, top, pltpu.roll(bot, 64, axis=1))
    tail[1] = jnp.where(left, pltpu.roll(top, 64, axis=1), bot)
    for n, (q, ref) in enumerate(((1 - p, theirs_ref), (p, mine_ref))):
        copies.append(pltpu.make_async_copy(tail.at[q], ref.at[pl.ds(3 * NR, NR // 2)], o_sem.at[n, 3]))
        copies[-1].start()
    for cp in copies:
        cp.wait()


def experts(layer, part, a_all, meta, pos, w1, w3, w2):
    vm, sm, hb, anywhere = (pl.BlockSpec(memory_space=m) for m in (pltpu.VMEM, pltpu.SMEM, pltpu.HBM, pl.ANY))
    dma = pltpu.SemaphoreType.DMA
    return pl.pallas_call(
        functools.partial(expert_kernel, layer, part),
        name=f"experts_{layer}_{part}",
        out_shape=[jax.ShapeDtypeStruct((PR, 128), F32)] * 2,
        in_specs=[vm, sm, vm, hb, hb, hb],
        out_specs=[anywhere, anywhere],
        scratch_shapes=[
            pltpu.VMEM((NW, D, FF), BF16), pltpu.VMEM((NW, D, FF), BF16), pltpu.VMEM((NW, FF, D), BF16),
            pltpu.VMEM((ALL, D), BF16), pltpu.VMEM((2304, D), BF16),
            pltpu.VMEM((2, 3, NR + 2 * PAD, 128), F32), pltpu.VMEM((NR + 2 * PAD, 128), F32),
            pltpu.VMEM((2, NR // 2, 128), F32),
            dma((3, NW)), dma((2, 4)),
        ],
        compiler_params=pltpu.CompilerParams(vmem_limit_bytes=38 * MIB),
        cost_estimate=pl.CostEstimate(flops=4_000_000_000, bytes_accessed=44_000_000 // PARTS, transcendentals=PAIRS * FF // PARTS),
    )(a_all, meta, pos, w1, w3, w2)


def merge_kernel(layer, a_ref, id_ref, pos_ref, mine0_ref, far0_ref, mine1_ref, theirs1_ref, wr_ref, x_ref,
                 y_own, y_far, wr, gate, base, acc, back, xsend, xfar,
                 l_sem, ys_sem, yr_sem, bs_sem, br_sem, fs_sem, fr_sem):
    p, e, e_x, e_d, e_z, dev_y, dev_x, dev_d, dev_z, dev_yx = peers()
    loads = [pltpu.make_async_copy(src, dst, l_sem.at[i])
             for i, (src, dst) in enumerate(((wr_ref.at[layer], wr), (mine0_ref, y_own.at[0]), (far0_ref, y_far.at[0]),
                                             (mine1_ref, y_own.at[1])))]
    for cp in loads:
        cp.start()
    entry_barrier((dev_y, dev_x, dev_d, dev_z))
    spans = [(t * NR, NR) for t in range(3)] + [(3 * NR, NR // 2)]
    y_copies = [remote(theirs1_ref.at[pl.ds(b, n)], y_far.at[1, pl.ds(b, n)], ys_sem.at[t], yr_sem.at[t], dev_y)
                for t, (b, n) in enumerate(spans)]
    for cp in y_copies:
        cp.start()

    loads[0].wait()
    u = rms(a_ref[...]).astype(BF16)
    logits = jnp.zeros((ALL, 256), F32)
    rest = wr[...]
    for _ in range(3):
        part = rest.astype(BF16)
        rest = rest - part.astype(F32)
        logits = logits + mm(u, part)
    col = iota((ALL, 256), 1)
    g = [jnp.sum(jnp.where(id_ref[layer, :, k:k + 1] == col, logits, 0.0), axis=1, keepdims=True) for k in range(8)]
    top = functools.reduce(jnp.maximum, g)
    g = [jnp.exp(v - top) for v in g]
    total = functools.reduce(jnp.add, g)
    g = [v / total for v in g]
    pos = [pos_ref[layer, :, 8 + k:9 + k] for k in range(8)]
    lane = iota((ALL, 128), 1)
    for c in range(PAIRS // 128):
        w = jnp.zeros((ALL, 128), F32)
        for k in range(8):
            w = jnp.where(pos[k] == lane + c * 128, g[k], w)
        for i in range(3):
            part = w.astype(BF16)
            w = w - part.astype(F32)
            gate[i, :, c * 128:(c + 1) * 128] = part

    def mix(h, t):
        b, n = spans[t]
        y = (y_own[h, b:b + n, :] + y_far[h, b:b + n, :]).astype(BF16)
        first = h * NR
        if t < 3:
            return sum(mm(gate[i, :, first:first + NR], y) for i in range(3))
        lo, hi = [sum(mm(gate[i, :, first + q * n:first + (q + 1) * n], y) for i in range(3)) for q in range(2)]
        keep = jnp.broadcast_to(p == 0, lo.shape)
        return jnp.where(keep, lo, pltpu.roll(lo, 64, axis=1)) + jnp.where(keep, pltpu.roll(hi, 64, axis=1), hi)

    loads[1].wait()
    loads[2].wait()
    for t in range(4):
        base[t] = mix(0, t)
    loads[3].wait()

    def block_of(ee):
        return pl.ds(pl.multiple_of(ee * T, T), T)

    def give(t):
        cps = [remote(acc.at[t, block_of(ee)], back.at[t, i], bs_sem.at[t, i], br_sem.at[t, i], dev)
               for i, (ee, dev) in enumerate(((e_x, dev_x), (e_z, dev_z), (e_d, dev_d)))]
        for cp in cps:
            cp.start()
        return cps

    def cols(q, t):
        return pl.ds(pl.multiple_of(q * CM + t * 128, 128), 128) if t < 3 else slice(2 * CM, D)

    def finish(t, cps):
        for cp in cps:
            cp.wait_recv()
        total = acc[t, block_of(e), :] + back[t, 0] + back[t, 1] + back[t, 2]
        xsend[t] = (a_ref[block_of(e), cols(p, t)].astype(F32) + total).astype(BF16)
        cp = remote(xsend.at[t], xfar.at[t], fs_sem.at[t], fr_sem.at[t], dev_y)
        cp.start()
        return cp

    given, sent = [], []
    for t in range(4):
        y_copies[t].wait_recv()
        acc[t] = base[t] + mix(1, t)
        given.append(give(t))
        if t >= 1:
            sent.append(finish(t - 1, given[t - 1]))
    sent.append(finish(3, given[3]))
    for t in range(3):
        x_ref[:, cols(p, t)] = xsend[t]
        sent[t].wait()
        x_ref[:, cols(1 - p, t)] = xfar[t]
    sent[3].wait()
    keep_own = (iota((T, 128), 1) // 64) == p
    x_ref[:, 2 * CM:] = jnp.where(keep_own, xsend[3].astype(F32), xfar[3].astype(F32)).astype(BF16)
    for cp in y_copies + [c for cps in given for c in cps]:
        cp.wait_send()


def merge(layer, a_all, ids, pos, mine0, far0, mine1, theirs1, wr, cid):
    vm, hb, anywhere = (pl.BlockSpec(memory_space=m) for m in (pltpu.VMEM, pltpu.HBM, pl.ANY))
    dma = pltpu.SemaphoreType.DMA
    return pl.pallas_call(
        functools.partial(merge_kernel, layer),
        name=f"merge_{layer}",
        out_shape=jax.ShapeDtypeStruct((T, D), BF16),
        in_specs=[vm, vm, vm, anywhere, anywhere, anywhere, anywhere, hb],
        out_specs=vm,
        scratch_shapes=[
            pltpu.VMEM((2, PR, 128), F32), pltpu.VMEM((2, PR, 128), F32),
            pltpu.VMEM((D, 256), F32), pltpu.VMEM((3, ALL, PAIRS), BF16),
            pltpu.VMEM((4, ALL, 128), F32), pltpu.VMEM((4, ALL, 128), F32), pltpu.VMEM((4, 3, T, 128), F32),
            pltpu.VMEM((4, T, 128), BF16), pltpu.VMEM((4, T, 128), BF16),
            dma((4,)), dma((4,)), dma((4,)), dma((4, 3)), dma((4, 3)), dma((4,)), dma((4,)),
        ],
        compiler_params=pltpu.CompilerParams(collective_id=cid, has_side_effects=True, vmem_limit_bytes=24 * MIB),
    )(a_all, ids, pos, mine0, far0, mine1, theirs1, wr)


def solution(mesh):
    tok_spec = P(('dp', 'ep'), None)
    cache_spec = P(None, ('dp', 'ep'), 'pool', None, None)
    up_spec = P(None, 'ep', None, 'pool')
    down_spec = P(None, 'ep', 'pool', None)
    in_specs = (tok_spec, cache_spec, cache_spec, P(('dp', 'ep')), P(), P(), P(), P(), P(), P(None, ('dp', 'ep'), None),
                up_spec, up_spec, down_spec)

    def body(hidden, k_cache, v_cache, cache_len, w_q, w_k, w_v, w_o, w_router, expert_ids, w_one, w_three, w_two):
        layers = w_q.shape[0]
        k = k_cache.reshape(layers, T, ROWS, HD)
        v = v_cache.reshape(layers, T, ROWS, HD)
        id_t = jnp.swapaxes(expert_ids, 1, 2)
        for layer in range(layers):
            a_all, *extra = attention(layer, hidden, cache_len, id_t if layer == 0 else None, k, v, w_q, w_k, w_v, w_o, 2 * layer)
            if layer == 0:
                ids_t, meta, pos_t = extra
                ids, pos = jnp.swapaxes(ids_t, 1, 2), jnp.swapaxes(pos_t, 1, 2)
            mine0, theirs0 = experts(layer, 0, a_all, meta, pos_t, w_one, w_three, w_two)
            far0 = lax.ppermute(theirs0, 'pool', [(0, 1), (1, 0)])
            mine1, theirs1 = experts(layer, 1, a_all, meta, pos_t, w_one, w_three, w_two)
            hidden = merge(layer, a_all, ids, pos, mine0, far0, mine1, theirs1, w_router, 2 * layer + 1)
        return hidden

    return jax.shard_map(body, mesh=mesh, in_specs=in_specs, out_specs=tok_spec, check_vma=False)
```

```python
import functools

import jax
import jax.numpy as jnp
from jax import lax
from jax.experimental import pallas as pl
from jax.experimental.pallas import tpu as pltpu
from jax.sharding import PartitionSpec as P

MESH = pl.DeviceIdType.MESH
F32, BF16, I32 = jnp.float32, jnp.bfloat16, jnp.int32
NORM_EPS = 1e-6
T, D, HD, H = 128, 896, 128, 16
HALF = T // 2
KV = 2
POS = 256
ROWS = POS * KV
CH = 8
NCH = T // CH
NB = 8
ALL = 4 * T
NE = 64
PAIRS = 1024
FF = 128
NW = 32
MC = 32
CM = 384
PARTS = 2
NR = PAIRS // PARTS
PR = 3 * NR + NR // 2
PAD = MC
MIB = 1024 * 1024


def rms(v):
    v = v.astype(F32)
    return v * lax.rsqrt(jnp.mean(v * v, axis=-1, keepdims=True) + NORM_EPS)


def mm(a, b):
    return jnp.dot(a, b, preferred_element_type=F32)


def iota(shape, dim):
    return lax.broadcasted_iota(I32, shape, dim)


def peers():
    g, p, e = lax.axis_index("dp"), lax.axis_index("pool"), lax.axis_index("ep")
    core = lax.rem(e, 2)
    e_x = lax.rem(e + 2, 4)
    e_d = e + 1 - 2 * core
    e_z = lax.rem(e_d + 2, 4)
    return p, e, e_x, e_d, e_z, (g, 1 - p, e), (g, p, e_x), (g, p, e_d), (g, p, e_z), (g, 1 - p, e_x)


def entry_barrier(targets):
    bar = pltpu.get_barrier_semaphore()
    for dev in targets:
        pl.semaphore_signal(bar, inc=1, device_id=dev, device_id_type=MESH)
    pl.semaphore_wait(bar, len(targets))


def remote(src, dst, send_sem, recv_sem, dev):
    return pltpu.make_async_remote_copy(src_ref=src, dst_ref=dst, send_sem=send_sem, recv_sem=recv_sem,
                                        device_id=dev, device_id_type=MESH)


def route(ids, e, meta, pos):
    sub = iota((128, ALL), 0)
    local = [ids[k:k + 1, :] - e * NE for k in range(8)]
    local = [jnp.where((v >= 0) & (v < NE), v, -1) for v in local]
    mask = jnp.zeros((128, ALL), F32)
    for v in local:
        mask = jnp.where(v == sub, 1.0, mask)
    mask_b = mask.astype(BF16)
    before = (iota((ALL, ALL), 0) < iota((ALL, ALL), 1)).astype(BF16)
    rank = mm(mask_b, before)
    n_col = jnp.broadcast_to(jnp.sum(mask, axis=1, keepdims=True), (128, 128)).astype(I32)
    n_row = lax.dot_general(jnp.ones((8, ALL), BF16), mask_b, (((1,), (1,)), ((), ())),
                            preferred_element_type=F32).astype(I32)
    lower = (iota((128, 128), 1) < iota((128, 128), 0)).astype(BF16)
    upper = (iota((128, 128), 0) < iota((128, 128), 1)).astype(BF16)
    as_b = lambda v: v.astype(F32).astype(BF16)
    off_col = mm(lower, as_b((n_col + 15) >> 4)) * 16.0
    offc_col = mm(lower, as_b(n_col >> 4)) * 16.0 + mm(lower, as_b(n_col & 15))
    off_row = mm(as_b((n_row + 15) >> 4), upper).astype(I32)
    offc_row = (mm(as_b(n_row >> 4), upper) * 16.0 + mm(as_b(n_row & 15), upper)).astype(I32)
    real = iota((8, 128), 1) < NE
    table = [n_row, off_row, offc_row]
    for r in range(PARTS):
        lo = jnp.sum(jnp.where(real & (offc_row + n_row <= r * NR), 1.0, 0.0), axis=1, keepdims=True)
        hi = jnp.sum(jnp.where(real & (offc_row < (r + 1) * NR), 1.0, 0.0), axis=1, keepdims=True)
        table.append(jnp.where(iota((8, 128), 1) == 0, lo, hi).astype(I32))
    row = iota((8, 128), 0)
    packed = jnp.zeros((8, 128), I32)
    for i, v in enumerate(table):
        packed = jnp.where(row == i, v, packed)
    meta[...] = packed
    for base, off in ((0, off_col), (8, offc_col)):
        where_to = off[:, 0:1] + rank + 1.0
        for k in range(8):
            found = jnp.sum(jnp.where(local[k] == sub, where_to, 0.0), axis=0, keepdims=True)
            pos[base + k:base + k + 1, :] = (found - 1.0).astype(I32)


def attn_steps(layer, nb, devs, len_ref, hbm, scr):
    k_ref, v_ref, wq_ref, wk_ref, wv_ref, wo_ref = hbm
    (kbuf, vbuf, wq_v, wk_v, wv_v, wo_v, q2d, kn2d, vn2d, num, nrec, stat, ssend, srec,
     kv_sem, w_sem, ns_sem, nr_sem, ss_sem, sr_sem, gs_sem, gr_sem) = scr
    p, e, e_x, e_d, e_z, dev_y, dev_x, dev_d, dev_z, dev_yx = devs

    def tok_of(c):
        first_half = (1 - p) * HALF + c * CH
        second_half = p * HALF + (c - NCH // 2) * CH
        return pl.multiple_of(jnp.where(c < NCH // 2, first_half, second_half), CH)

    def kv_copies(c):
        slot = c & (nb - 1)
        src = pl.ds(tok_of(c), CH)
        return (pltpu.make_async_copy(k_ref.at[layer, src], kbuf.at[slot], kv_sem.at[0, slot]),
                pltpu.make_async_copy(v_ref.at[layer, src], vbuf.at[slot], kv_sem.at[1, slot]))

    weights = [pltpu.make_async_copy(r.at[layer], b, w_sem.at[i])
               for i, (r, b) in enumerate(((wq_ref, wq_v), (wk_ref, wk_v), (wv_ref, wv_v), (wo_ref, wo_v)))]
    def start_kv(first, last):
        for c in range(first, last):
            for cp in kv_copies(jnp.int32(c)):
                cp.start()

    def start(chunks):
        for cp in weights[:3]:
            cp.start()
        start_kv(0, chunks)

    def run(x_ref, a_ref, started, between):
        normed = rms(x_ref[...]).astype(BF16)
        for cp in weights[:3]:
            cp.wait()
        start_kv(started, nb)
        weights[3].start()
        for hp in range(H // 2):
            pair = mm(normed, wq_v[:, hp * 256:(hp + 1) * 256]).astype(BF16).astype(F32)
            for i in range(2):
                q2d[pl.ds(hp * 2 + i, T, stride=H), :] = pair[:, i * HD:(i + 1) * HD]
        for w, dst in ((wk_v, kn2d), (wv_v, vn2d)):
            pair = mm(normed, w[...]).astype(BF16).astype(F32)
            for i in range(KV):
                dst[pl.ds(i, T, stride=KV), :] = pair[:, i * HD:(i + 1) * HD]

        scale = HD ** -0.5
        col = iota((H, ROWS), 1)
        group_ok = (col & 1) == (iota((H, ROWS), 0) // (H // KV))
        col_pos = jnp.where(group_ok, col >> 1, 1 << 30)
        lane = iota((H, T), 1)

        def heads_of(ref, tok):
            two = ref[pl.ds(tok * KV, KV), :]
            return jnp.concatenate([jnp.broadcast_to(two[i:i + 1], (H // KV, HD)) for i in range(KV)], axis=0)

        def num_copy(c):
            rows = pl.ds(pl.multiple_of(c * (CH * H), CH * H), CH * H)
            return remote(num.at[rows], nrec.at[rows], ns_sem.at[c], nr_sem.at[c], dev_y)

        stat_copy = remote(ssend, srec, ss_sem, sr_sem, dev_y)

        def chunk(c, carry):
            slot = c & (nb - 1)
            for cp in kv_copies(c):
                cp.wait()
            tok0 = tok_of(c)
            m_all, l_all, n_all = stat[0], stat[1], stat[2]
            for j0 in range(0, CH, 4):
                group = range(j0, j0 + 4)
                qs, ss = {}, {}
                for j in group:
                    qs[j] = q2d[pl.ds(pl.multiple_of((tok0 + j) * H, H), H), :]
                    ss[j] = lax.dot_general(qs[j].astype(BF16), kbuf[slot, j], (((1,), (1,)), ((), ())),
                                            preferred_element_type=F32) * scale
                ps = {}
                for j in group:
                    limit = len_ref[tok0 + j] - p * POS
                    s = jnp.where(col_pos < limit, ss[j], -1e30)
                    s_new = jnp.sum(qs[j] * heads_of(kn2d, tok0 + j), axis=1, keepdims=True) * scale
                    m = jnp.maximum(jnp.max(s, axis=1, keepdims=True), s_new)
                    pr = jnp.exp(s - m)
                    ps[j] = pr.astype(BF16)
                    here = lane == c * CH + j
                    m_all = jnp.where(here, m, m_all)
                    l_all = jnp.where(here, jnp.sum(pr, axis=1, keepdims=True), l_all)
                    n_all = jnp.where(here, s_new, n_all)
                for j in group:
                    num[pl.ds(pl.multiple_of((c * CH + j) * H, H), H), :] = mm(ps[j], vbuf[slot, j])
            stat[0], stat[1], stat[2] = m_all, l_all, n_all

            @pl.when(c + nb < NCH)
            def _():
                for cp in kv_copies(c + nb):
                    cp.start()

            @pl.when(c == NCH // 2 - 1)
            def _():
                ssend[0], ssend[1] = m_all, l_all

            @pl.when((c >= 1) & (c <= NCH // 2))
            def _():
                num_copy(c - 1).start()

            @pl.when(c == NCH // 2)
            def _():
                stat_copy.start()

            return carry

        stat[...] = jnp.zeros_like(stat)
        lax.fori_loop(0, NCH, chunk, 0)

        weights[3].wait()
        stat_copy.wait()
        m_own, l_own, s_new = stat[0], stat[1], stat[2]
        m_far = pltpu.roll(srec[0], HALF, axis=1)
        l_far = pltpu.roll(srec[1], HALF, axis=1)
        m = jnp.maximum(m_own, m_far)
        w_own, w_far, w_new = jnp.exp(m_own - m), jnp.exp(m_far - m), jnp.exp(s_new - m)
        denom = l_own * w_own + l_far * w_far + w_new
        c_own, c_far, c_new = w_own / denom, w_far / denom, w_new / denom

        def combine(c, carry):
            num_copy(c).wait()
            for j in range(CH):
                i = c * CH + j
                pick = lane == HALF + i
                own, far, new = [jnp.sum(jnp.where(pick, v, 0.0), axis=1, keepdims=True) for v in (c_own, c_far, c_new)]
                there = pl.ds(pl.multiple_of(i * H, H), H)
                here = pl.ds(pl.multiple_of((HALF + i) * H, H), H)
                num[here, :] = num[here, :] * own + nrec[there, :] * far + heads_of(vn2d, p * HALF + i) * new
            return carry

        lax.fori_loop(0, NCH // 2, combine, 0)

        proj = jnp.zeros((HALF, D), F32)
        for hp in range(H // 2):
            pair = jnp.concatenate([num[pl.ds(HALF * H + hp * 2 + i, HALF, stride=H), :].astype(BF16) for i in range(2)], axis=1)
            proj = proj + mm(pair, wo_v[hp * 256:(hp + 1) * 256, :])
        mine = pl.ds(pl.multiple_of(p * HALF, HALF), HALF)

        def rows(pp, ee):
            return pl.ds(pl.multiple_of(ee * T + pp * HALF, HALF), HALF)

        a_ref[rows(p, e), :] = (x_ref[mine, :].astype(F32) + proj).astype(BF16)

        def gather(i, pp, ee, dev):
            block = a_ref.at[rows(pp, ee)]
            cp = remote(block, block, gs_sem.at[i], gr_sem.at[i], dev)
            cp.start()
            return cp

        copies = [gather(0, p, e, dev_yx), gather(1, p, e, dev_x), gather(2, p, e, dev_y), gather(3, p, e, dev_d)]
        between()
        for i, pp, ee in ((2, 1 - p, e), (1, p, e_x), (0, 1 - p, e_x)):
            copies[i].wait_recv()
            copies.append(gather(len(copies), pp, ee, dev_d))
        for i in range(3, 7):
            copies[i].wait_recv()
        for cp in copies:
            cp.wait_send()

    return start, run


def attn_kernel(x_ref, len_ref, idt_ref, *refs):
    hbm, (a_ref, ida_ref, meta_ref, pos_ref), scr = refs[:6], refs[6:10], refs[10:]
    is_sem, ir_sem = scr[-2:]
    devs = peers()
    p, e, e_x, e_d, e_z, dev_y, dev_x, dev_d, dev_z, dev_yx = devs
    start, run = attn_steps(0, NB, devs, len_ref, hbm, scr[:-2])
    start(2)
    entry_barrier((dev_y, dev_x, dev_d, dev_z, dev_yx))
    mine = (slice(None), slice(None), pl.ds(pl.multiple_of(e * T, T), T))
    ida_ref[mine] = idt_ref[...]
    id_copies = []
    for i, dev in enumerate((dev_x, dev_d, dev_z)):
        id_copies.append(remote(idt_ref, ida_ref.at[mine], is_sem.at[i], ir_sem.at[i], dev))
        id_copies[-1].start()

    def make_tables():
        for cp in id_copies:
            cp.wait()
        for n in range(ida_ref.shape[0]):
            route(ida_ref.at[n], e, meta_ref.at[n], pos_ref.at[n])

    run(x_ref, a_ref, 2, make_tables)


def attn_scratch(nb):
    dma = pltpu.SemaphoreType.DMA
    return [
        pltpu.VMEM((nb, CH, ROWS, HD), BF16), pltpu.VMEM((nb, CH, ROWS, HD), BF16),
        pltpu.VMEM((D, H * HD), BF16), pltpu.VMEM((D, KV * HD), BF16), pltpu.VMEM((D, KV * HD), BF16),
        pltpu.VMEM((H * HD, D), BF16),
        pltpu.VMEM((T * H, HD), F32), pltpu.VMEM((T * KV, HD), F32), pltpu.VMEM((T * KV, HD), F32),
        pltpu.VMEM((T * H, HD), F32), pltpu.VMEM((HALF * H, HD), F32),
        pltpu.VMEM((3, H, T), F32), pltpu.VMEM((2, H, T), F32), pltpu.VMEM((2, H, T), F32),
        dma((2, nb)), dma((4,)), dma((NCH // 2,)), dma((NCH // 2,)), dma(()), dma(()), dma((7,)), dma((7,)),
    ]


def attention(x, cache_len, id_t, hbm):
    vm, sm, hb = (pl.BlockSpec(memory_space=m) for m in (pltpu.VMEM, pltpu.SMEM, pltpu.HBM))
    dma = pltpu.SemaphoreType.DMA
    layers = id_t.shape[0]
    return pl.pallas_call(
        attn_kernel,
        name="attn_0",
        out_shape=[jax.ShapeDtypeStruct((ALL, D), BF16), jax.ShapeDtypeStruct((layers, 8, ALL), I32),
                   jax.ShapeDtypeStruct((layers, 8, 128), I32), jax.ShapeDtypeStruct((layers, 16, ALL), I32)],
        in_specs=[vm, sm, vm] + [hb] * 6,
        out_specs=[vm] * 4,
        scratch_shapes=attn_scratch(NB) + [dma((3,)), dma((3,))],
        compiler_params=pltpu.CompilerParams(collective_id=0, has_side_effects=True, vmem_limit_bytes=61 * MIB),
    )(x, cache_len, id_t, *hbm)


def expert_kernel(layer, part, a_ref, meta, pos_ref, w1_ref, w3_ref, w2_ref, mine_ref, theirs_ref,
                  w1b, w3b, w2b, u, xs, ym, yt, tail, w_sem, o_sem):
    p = lax.axis_index("pool")
    r0 = part * NR
    lo, hi = meta[layer, 3 + part, 0], meta[layer, 3 + part, 1]
    odd = (hi - lo) & 1
    lo, hi = jnp.where((odd == 1) & (hi == NE), lo - 1, lo), jnp.where((odd == 1) & (hi < NE), hi + 1, hi)

    def w_copies(i):
        slot = i & (NW - 1)
        return [pltpu.make_async_copy(r.at[layer, i], b.at[slot], w_sem.at[n, slot])
                for n, (r, b) in enumerate(((w1_ref, w1b), (w3_ref, w3b), (w2_ref, w2b)))]

    def start(i, carry):
        for cp in w_copies(i):
            cp.start()
        return carry

    lax.fori_loop(lo, jnp.minimum(lo + NW, hi), start, 0)

    u[...] = rms(a_ref[...]).astype(BF16)

    def dispatch(i, carry):
        row = iota((256, ALL), 0) + i * 256
        hit = jnp.zeros((256, ALL), F32)
        for k in range(8):
            hit = jnp.where(pos_ref[layer, k:k + 1, :] == row, 1.0, hit)
        xs[pl.ds(pl.multiple_of(i * 256, 256), 256), :] = mm(hit.astype(BF16), u[...]).astype(BF16)
        return carry

    lax.fori_loop(meta[layer, 1, lo] >> 4, (meta[layer, 1, hi] + 15) >> 4, dispatch, 0)

    def rows_at(i, j):
        slot = i & (NW - 1)
        rows = xs[pl.ds(pl.multiple_of(meta[layer, 1, i] * 16 + j * MC, 16), MC), :]
        act = (jax.nn.silu(mm(rows, w1b[slot])) * mm(rows, w3b[slot])).astype(BF16)
        return mm(act, w2b[slot]), pl.ds(jnp.minimum(meta[layer, 2, i] + j * MC - r0, NR) + PAD, MC)

    def targets(to):
        return [ym.at[t // 3, t % 3, to] for t in range(6)] + [yt.at[to]]

    def first_step(i):
        return jnp.maximum(r0 - meta[layer, 2, i], 0) >> 5

    def more_steps(i):
        n, offc, first = meta[layer, 0, i], meta[layer, 2, i], first_step(i)

        def step(j, carry):
            y, to = rows_at(i, j)
            keep = iota((MC, 128), 0) < n - j * MC
            for t, ref in enumerate(targets(to)):
                ref[...] = jnp.where(keep, y[:, t * 128:(t + 1) * 128], ref[...])
            return carry

        lax.fori_loop(first + 1, (jnp.minimum(n, r0 + NR - offc) + MC - 1) >> 5, step, 0)

    def expert_pair(h, carry):
        pair = [lo + 2 * h, lo + 2 * h + 1]
        for i in pair:
            for cp in w_copies(i):
                cp.wait()
        done = [rows_at(i, first_step(i)) for i in pair]
        for y, to in done:
            for t, ref in enumerate(targets(to)):
                ref[...] = y[:, t * 128:(t + 1) * 128]
        for i in pair:
            more_steps(i)
        for i in pair:
            @pl.when(i + NW < hi)
            def _():
                start(i + NW, 0)
        return carry

    lax.fori_loop(0, (hi - lo) >> 1, expert_pair, 0)
    copies = []
    for n, (q, ref) in enumerate(((1 - p, theirs_ref), (p, mine_ref))):
        for t in range(3):
            copies.append(pltpu.make_async_copy(ym.at[q, t, pl.ds(PAD, NR)], ref.at[pl.ds(t * NR, NR)], o_sem.at[n, t]))
            copies[-1].start()
    top, bot = yt[PAD:PAD + NR // 2, :], yt[PAD + NR // 2:PAD + NR, :]
    left = iota((NR // 2, 128), 1) < 64
    tail[0] = jnp.where(left, top, pltpu.roll(bot, 64, axis=1))
    tail[1] = jnp.where(left, pltpu.roll(top, 64, axis=1), bot)
    for n, (q, ref) in enumerate(((1 - p, theirs_ref), (p, mine_ref))):
        copies.append(pltpu.make_async_copy(tail.at[q], ref.at[pl.ds(3 * NR, NR // 2)], o_sem.at[n, 3]))
        copies[-1].start()
    for cp in copies:
        cp.wait()


def experts(layer, part, a_all, meta, pos, w1, w3, w2):
    vm, sm, hb, anywhere = (pl.BlockSpec(memory_space=m) for m in (pltpu.VMEM, pltpu.SMEM, pltpu.HBM, pl.ANY))
    dma = pltpu.SemaphoreType.DMA
    return pl.pallas_call(
        functools.partial(expert_kernel, layer, part),
        name=f"experts_{layer}_{part}",
        out_shape=[jax.ShapeDtypeStruct((PR, 128), F32)] * 2,
        in_specs=[vm, sm, vm, hb, hb, hb],
        out_specs=[anywhere, anywhere],
        scratch_shapes=[
            pltpu.VMEM((NW, D, FF), BF16), pltpu.VMEM((NW, D, FF), BF16), pltpu.VMEM((NW, FF, D), BF16),
            pltpu.VMEM((ALL, D), BF16), pltpu.VMEM((2304, D), BF16),
            pltpu.VMEM((2, 3, NR + 2 * PAD, 128), F32), pltpu.VMEM((NR + 2 * PAD, 128), F32),
            pltpu.VMEM((2, NR // 2, 128), F32),
            dma((3, NW)), dma((2, 4)),
        ],
        compiler_params=pltpu.CompilerParams(vmem_limit_bytes=38 * MIB),
        cost_estimate=pl.CostEstimate(flops=4_000_000_000, bytes_accessed=44_000_000 // PARTS, transcendentals=PAIRS * FF // PARTS),
    )(a_all, meta, pos, w1, w3, w2)


def merge_steps(layer, devs, ins, x_ref, scr, beside):
    a_ref, id_ref, pos_ref, mine0_ref, far0_ref, mine1_ref, theirs1_ref, wr_ref = ins
    (y_own, y_far, wr, gate, base, acc, back, xsend, xfar,
     l_sem, ys_sem, yr_sem, bs_sem, br_sem, fs_sem, fr_sem) = scr
    p, e, e_x, e_d, e_z, dev_y, dev_x, dev_d, dev_z, dev_yx = devs
    loads = [pltpu.make_async_copy(src, dst, l_sem.at[i])
             for i, (src, dst) in enumerate(((wr_ref.at[layer], wr), (mine0_ref, y_own.at[0]), (far0_ref, y_far.at[0]),
                                             (mine1_ref, y_own.at[1])))]
    for cp in loads:
        cp.start()
    entry_barrier((dev_y, dev_x, dev_d, dev_z, dev_yx))
    spans = [(t * NR, NR) for t in range(3)] + [(3 * NR, NR // 2)]
    y_copies = [remote(theirs1_ref.at[pl.ds(b, n)], y_far.at[1, pl.ds(b, n)], ys_sem.at[t], yr_sem.at[t], dev_y)
                for t, (b, n) in enumerate(spans)]
    for cp in y_copies:
        cp.start()
    beside()

    loads[0].wait()
    u = rms(a_ref[...]).astype(BF16)
    logits = jnp.zeros((ALL, 256), F32)
    rest = wr[...]
    for _ in range(3):
        part = rest.astype(BF16)
        rest = rest - part.astype(F32)
        logits = logits + mm(u, part)
    col = iota((ALL, 256), 1)
    g = [jnp.sum(jnp.where(id_ref[layer, :, k:k + 1] == col, logits, 0.0), axis=1, keepdims=True) for k in range(8)]
    top = functools.reduce(jnp.maximum, g)
    g = [jnp.exp(v - top) for v in g]
    total = functools.reduce(jnp.add, g)
    g = [v / total for v in g]
    pos = [pos_ref[layer, :, 8 + k:9 + k] for k in range(8)]
    lane = iota((ALL, 128), 1)
    for c in range(PAIRS // 128):
        w = jnp.zeros((ALL, 128), F32)
        for k in range(8):
            w = jnp.where(pos[k] == lane + c * 128, g[k], w)
        for i in range(3):
            part = w.astype(BF16)
            w = w - part.astype(F32)
            gate[i, :, c * 128:(c + 1) * 128] = part

    def mix(h, t):
        b, n = spans[t]
        y = (y_own[h, b:b + n, :] + y_far[h, b:b + n, :]).astype(BF16)
        first = h * NR
        if t < 3:
            return sum(mm(gate[i, :, first:first + NR], y) for i in range(3))
        lo, hi = [sum(mm(gate[i, :, first + q * n:first + (q + 1) * n], y) for i in range(3)) for q in range(2)]
        keep = jnp.broadcast_to(p == 0, lo.shape)
        return jnp.where(keep, lo, pltpu.roll(lo, 64, axis=1)) + jnp.where(keep, pltpu.roll(hi, 64, axis=1), hi)

    loads[1].wait()
    loads[2].wait()
    for t in range(4):
        base[t] = mix(0, t)
    loads[3].wait()

    def block_of(ee):
        return pl.ds(pl.multiple_of(ee * T, T), T)

    def give(t):
        cps = [remote(acc.at[t, block_of(ee)], back.at[t, i], bs_sem.at[t, i], br_sem.at[t, i], dev)
               for i, (ee, dev) in enumerate(((e_x, dev_x), (e_z, dev_z), (e_d, dev_d)))]
        for cp in cps:
            cp.start()
        return cps

    def cols(q, t):
        return pl.ds(pl.multiple_of(q * CM + t * 128, 128), 128) if t < 3 else slice(2 * CM, D)

    def finish(t, cps):
        for cp in cps:
            cp.wait_recv()
        total = acc[t, block_of(e), :] + back[t, 0] + back[t, 1] + back[t, 2]
        xsend[t] = (a_ref[block_of(e), cols(p, t)].astype(F32) + total).astype(BF16)
        cp = remote(xsend.at[t], xfar.at[t], fs_sem.at[t], fr_sem.at[t], dev_y)
        cp.start()
        return cp

    given, sent = [], []
    for t in range(4):
        y_copies[t].wait_recv()
        acc[t] = base[t] + mix(1, t)
        given.append(give(t))
        if t >= 1:
            sent.append(finish(t - 1, given[t - 1]))
    sent.append(finish(3, given[3]))
    for t in range(3):
        x_ref[:, cols(p, t)] = xsend[t]
        sent[t].wait()
        x_ref[:, cols(1 - p, t)] = xfar[t]
    sent[3].wait()
    keep_own = (iota((T, 128), 1) // 64) == p
    x_ref[:, 2 * CM:] = jnp.where(keep_own, xsend[3].astype(F32), xfar[3].astype(F32)).astype(BF16)
    for cp in y_copies + [c for cps in given for c in cps]:
        cp.wait_send()


MERGE_IN, MERGE_SCR = 8, 16


def merge_last_kernel(layer, *refs):
    merge_steps(layer, peers(), refs[:MERGE_IN], refs[MERGE_IN], refs[MERGE_IN + 1:], lambda: None)


def merge_next_kernel(layer, *refs):
    ins, len_ref, hbm, a_ref = refs[:MERGE_IN], refs[MERGE_IN], refs[MERGE_IN + 1:MERGE_IN + 7], refs[MERGE_IN + 7]
    x_ref, scr = refs[MERGE_IN + 8], refs[MERGE_IN + 9:]
    devs = peers()
    start, run = attn_steps(layer + 1, NCH, devs, len_ref, hbm, scr[MERGE_SCR:])
    merge_steps(layer, devs, ins, x_ref, scr[:MERGE_SCR], lambda: start(NCH))
    run(x_ref, a_ref, NCH, lambda: None)


def merge_scratch():
    dma = pltpu.SemaphoreType.DMA
    return [
        pltpu.VMEM((2, PR, 128), F32), pltpu.VMEM((2, PR, 128), F32),
        pltpu.VMEM((D, 256), F32), pltpu.VMEM((3, ALL, PAIRS), BF16),
        pltpu.VMEM((4, ALL, 128), F32), pltpu.VMEM((4, ALL, 128), F32), pltpu.VMEM((4, 3, T, 128), F32),
        pltpu.VMEM((4, T, 128), BF16), pltpu.VMEM((4, T, 128), BF16),
        dma((4,)), dma((4,)), dma((4,)), dma((4, 3)), dma((4, 3)), dma((4,)), dma((4,)),
    ]


def merge(layer, last, ins, cache_len, hbm):
    vm, sm, hb, anywhere = (pl.BlockSpec(memory_space=m) for m in (pltpu.VMEM, pltpu.SMEM, pltpu.HBM, pl.ANY))
    in_specs = [vm, vm, vm, anywhere, anywhere, anywhere, anywhere, hb]
    params = functools.partial(pltpu.CompilerParams, collective_id=1 + layer, has_side_effects=True)
    if last:
        return pl.pallas_call(
            functools.partial(merge_last_kernel, layer),
            name=f"merge_{layer}",
            out_shape=jax.ShapeDtypeStruct((T, D), BF16),
            in_specs=in_specs,
            out_specs=vm,
            scratch_shapes=merge_scratch(),
            compiler_params=params(vmem_limit_bytes=24 * MIB),
        )(*ins)
    return pl.pallas_call(
        functools.partial(merge_next_kernel, layer),
        name=f"merge_attn_{layer}",
        out_shape=jax.ShapeDtypeStruct((ALL, D), BF16),
        in_specs=in_specs + [sm] + [hb] * 6,
        out_specs=vm,
        scratch_shapes=[pltpu.VMEM((T, D), BF16)] + merge_scratch() + attn_scratch(NCH),
        compiler_params=params(vmem_limit_bytes=67043328),
    )(*ins, cache_len, *hbm)


def solution(mesh):
    tok_spec = P(('dp', 'ep'), None)
    cache_spec = P(None, ('dp', 'ep'), 'pool', None, None)
    up_spec = P(None, 'ep', None, 'pool')
    down_spec = P(None, 'ep', 'pool', None)
    in_specs = (tok_spec, cache_spec, cache_spec, P(('dp', 'ep')), P(), P(), P(), P(), P(), P(None, ('dp', 'ep'), None),
                up_spec, up_spec, down_spec)

    def body(hidden, k_cache, v_cache, cache_len, w_q, w_k, w_v, w_o, w_router, expert_ids, w_one, w_three, w_two):
        layers = w_q.shape[0]
        k = k_cache.reshape(layers, T, ROWS, HD)
        v = v_cache.reshape(layers, T, ROWS, HD)
        id_t = jnp.swapaxes(expert_ids, 1, 2)
        hbm = (k, v, w_q, w_k, w_v, w_o)
        a_all, ids_t, meta, pos_t = attention(hidden, cache_len, id_t, hbm)
        ids, pos = jnp.swapaxes(ids_t, 1, 2), jnp.swapaxes(pos_t, 1, 2)
        for layer in range(layers):
            mine0, theirs0 = experts(layer, 0, a_all, meta, pos_t, w_one, w_three, w_two)
            far0 = lax.ppermute(theirs0, 'pool', [(0, 1), (1, 0)])
            mine1, theirs1 = experts(layer, 1, a_all, meta, pos_t, w_one, w_three, w_two)
            ins = (a_all, ids, pos, mine0, far0, mine1, theirs1, w_router)
            last = layer == layers - 1
            a_all = merge(layer, last, ins, cache_len, hbm)
        return a_all

    return jax.shard_map(body, mesh=mesh, in_specs=in_specs, out_specs=tok_spec, check_vma=False)
```

```python
import functools

import jax
import jax.numpy as jnp
from jax import lax
from jax.experimental import pallas as pl
from jax.experimental.pallas import tpu as pltpu
from jax.sharding import PartitionSpec as P

MESH = pl.DeviceIdType.MESH
F32, BF16, I32 = jnp.float32, jnp.bfloat16, jnp.int32
NORM_EPS = 1e-6
T, D, HD, H = 128, 896, 128, 16
HALF = T // 2
KV = 2
POS = 256
ROWS = POS * KV
CH = 8
NCH = T // CH
NB = 8
ALL = 4 * T
NE = 64
PAIRS = 1024
FF = 128
NW = 32
CM = 384
PARTS = 2
NR = PAIRS // PARTS
PR = 3 * NR + NR // 2
PAD = 64
STEP_LOG = (6, 5)
MIB = 1024 * 1024


def rms(v):
    v = v.astype(F32)
    return v * lax.rsqrt(jnp.mean(v * v, axis=-1, keepdims=True) + NORM_EPS)


def mm(a, b):
    return jnp.dot(a, b, preferred_element_type=F32)


def iota(shape, dim):
    return lax.broadcasted_iota(I32, shape, dim)


def peers():
    g, p, e = lax.axis_index("dp"), lax.axis_index("pool"), lax.axis_index("ep")
    core = lax.rem(e, 2)
    e_x = lax.rem(e + 2, 4)
    e_d = e + 1 - 2 * core
    e_z = lax.rem(e_d + 2, 4)
    return p, e, e_x, e_d, e_z, (g, 1 - p, e), (g, p, e_x), (g, p, e_d), (g, p, e_z), (g, 1 - p, e_x)


def entry_barrier(targets):
    bar = pltpu.get_barrier_semaphore()
    for dev in targets:
        pl.semaphore_signal(bar, inc=1, device_id=dev, device_id_type=MESH)
    pl.semaphore_wait(bar, len(targets))


def remote(src, dst, send_sem, recv_sem, dev):
    return pltpu.make_async_remote_copy(src_ref=src, dst_ref=dst, send_sem=send_sem, recv_sem=recv_sem,
                                        device_id=dev, device_id_type=MESH)


def route(ids, e, meta, pos):
    sub = iota((128, ALL), 0)
    local = [ids[k:k + 1, :] - e * NE for k in range(8)]
    local = [jnp.where((v >= 0) & (v < NE), v, -1) for v in local]
    mask = jnp.zeros((128, ALL), F32)
    for v in local:
        mask = jnp.where(v == sub, 1.0, mask)
    mask_b = mask.astype(BF16)
    before = (iota((ALL, ALL), 0) < iota((ALL, ALL), 1)).astype(BF16)
    rank = mm(mask_b, before)
    n_col = jnp.broadcast_to(jnp.sum(mask, axis=1, keepdims=True), (128, 128)).astype(I32)
    n_row = lax.dot_general(jnp.ones((8, ALL), BF16), mask_b, (((1,), (1,)), ((), ())),
                            preferred_element_type=F32).astype(I32)
    lower = (iota((128, 128), 1) < iota((128, 128), 0)).astype(BF16)
    upper = (iota((128, 128), 0) < iota((128, 128), 1)).astype(BF16)
    as_b = lambda v: v.astype(F32).astype(BF16)
    off_col = mm(lower, as_b((n_col + 15) >> 4)) * 16.0
    offc_col = mm(lower, as_b(n_col >> 4)) * 16.0 + mm(lower, as_b(n_col & 15))
    off_row = mm(as_b((n_row + 15) >> 4), upper).astype(I32)
    offc_row = (mm(as_b(n_row >> 4), upper) * 16.0 + mm(as_b(n_row & 15), upper)).astype(I32)
    real = iota((8, 128), 1) < NE
    table = [n_row, off_row, offc_row]
    for r in range(PARTS):
        lo = jnp.sum(jnp.where(real & (offc_row + n_row <= r * NR), 1.0, 0.0), axis=1, keepdims=True)
        hi = jnp.sum(jnp.where(real & (offc_row < (r + 1) * NR), 1.0, 0.0), axis=1, keepdims=True)
        table.append(jnp.where(iota((8, 128), 1) == 0, lo, hi).astype(I32))
    row = iota((8, 128), 0)
    packed = jnp.zeros((8, 128), I32)
    for i, v in enumerate(table):
        packed = jnp.where(row == i, v, packed)
    meta[...] = packed
    for base, off in ((0, off_col), (8, offc_col)):
        where_to = off[:, 0:1] + rank + 1.0
        for k in range(8):
            found = jnp.sum(jnp.where(local[k] == sub, where_to, 0.0), axis=0, keepdims=True)
            pos[base + k:base + k + 1, :] = (found - 1.0).astype(I32)


def attn_steps(layer, nb, devs, len_ref, hbm, scr):
    k_ref, v_ref, wq_ref, wk_ref, wv_ref, wo_ref = hbm
    (kbuf, vbuf, wq_v, wk_v, wv_v, wo_v, q2d, kn2d, vn2d, num, nrec, stat, ssend, srec,
     kv_sem, w_sem, ns_sem, nr_sem, ss_sem, sr_sem, gs_sem, gr_sem) = scr
    p, e, e_x, e_d, e_z, dev_y, dev_x, dev_d, dev_z, dev_yx = devs

    def tok_of(c):
        first_half = (1 - p) * HALF + c * CH
        second_half = p * HALF + (c - NCH // 2) * CH
        return pl.multiple_of(jnp.where(c < NCH // 2, first_half, second_half), CH)

    def kv_copies(c):
        slot = c & (nb - 1)
        src = pl.ds(tok_of(c), CH)
        return (pltpu.make_async_copy(k_ref.at[layer, src], kbuf.at[slot], kv_sem.at[0, slot]),
                pltpu.make_async_copy(v_ref.at[layer, src], vbuf.at[slot], kv_sem.at[1, slot]))

    weights = [pltpu.make_async_copy(r.at[layer], b, w_sem.at[i])
               for i, (r, b) in enumerate(((wq_ref, wq_v), (wk_ref, wk_v), (wv_ref, wv_v), (wo_ref, wo_v)))]
    def start_kv(first, last):
        for c in range(first, last):
            for cp in kv_copies(jnp.int32(c)):
                cp.start()

    def start(chunks):
        for cp in weights[:3]:
            cp.start()
        start_kv(0, chunks)

    def run(x_ref, a_ref, started, between):
        normed = rms(x_ref[...]).astype(BF16)
        for cp in weights[:3]:
            cp.wait()
        start_kv(started, nb)
        weights[3].start()
        for hp in range(H // 2):
            pair = mm(normed, wq_v[:, hp * 256:(hp + 1) * 256]).astype(BF16).astype(F32)
            for i in range(2):
                q2d[pl.ds(hp * 2 + i, T, stride=H), :] = pair[:, i * HD:(i + 1) * HD]
        for w, dst in ((wk_v, kn2d), (wv_v, vn2d)):
            pair = mm(normed, w[...]).astype(BF16).astype(F32)
            for i in range(KV):
                dst[pl.ds(i, T, stride=KV), :] = pair[:, i * HD:(i + 1) * HD]

        scale = HD ** -0.5
        col = iota((H, ROWS), 1)
        group_ok = (col & 1) == (iota((H, ROWS), 0) // (H // KV))
        col_pos = jnp.where(group_ok, col >> 1, 1 << 30)
        lane = iota((H, T), 1)

        def heads_of(ref, tok):
            two = ref[pl.ds(tok * KV, KV), :]
            return jnp.concatenate([jnp.broadcast_to(two[i:i + 1], (H // KV, HD)) for i in range(KV)], axis=0)

        def num_copy(c):
            rows = pl.ds(pl.multiple_of(c * (CH * H), CH * H), CH * H)
            return remote(num.at[rows], nrec.at[rows], ns_sem.at[c], nr_sem.at[c], dev_y)

        stat_copy = remote(ssend, srec, ss_sem, sr_sem, dev_y)

        def chunk(c, carry):
            slot = c & (nb - 1)
            for cp in kv_copies(c):
                cp.wait()
            tok0 = tok_of(c)
            m_all, l_all, n_all = stat[0], stat[1], stat[2]
            for j0 in range(0, CH, 4):
                group = range(j0, j0 + 4)
                qs, ss = {}, {}
                for j in group:
                    qs[j] = q2d[pl.ds(pl.multiple_of((tok0 + j) * H, H), H), :]
                    ss[j] = lax.dot_general(qs[j].astype(BF16), kbuf[slot, j], (((1,), (1,)), ((), ())),
                                            preferred_element_type=F32) * scale
                ps = {}
                for j in group:
                    limit = len_ref[tok0 + j] - p * POS
                    s = jnp.where(col_pos < limit, ss[j], -1e30)
                    s_new = jnp.sum(qs[j] * heads_of(kn2d, tok0 + j), axis=1, keepdims=True) * scale
                    m = jnp.maximum(jnp.max(s, axis=1, keepdims=True), s_new)
                    pr = jnp.exp(s - m)
                    ps[j] = pr.astype(BF16)
                    here = lane == c * CH + j
                    m_all = jnp.where(here, m, m_all)
                    l_all = jnp.where(here, jnp.sum(pr, axis=1, keepdims=True), l_all)
                    n_all = jnp.where(here, s_new, n_all)
                for j in group:
                    num[pl.ds(pl.multiple_of((c * CH + j) * H, H), H), :] = mm(ps[j], vbuf[slot, j])
            stat[0], stat[1], stat[2] = m_all, l_all, n_all

            @pl.when(c + nb < NCH)
            def _():
                for cp in kv_copies(c + nb):
                    cp.start()

            @pl.when(c == NCH // 2 - 1)
            def _():
                ssend[0], ssend[1] = m_all, l_all

            @pl.when((c >= 1) & (c <= NCH // 2))
            def _():
                num_copy(c - 1).start()

            @pl.when(c == NCH // 2)
            def _():
                stat_copy.start()

            return carry

        stat[...] = jnp.zeros_like(stat)
        lax.fori_loop(0, NCH, chunk, 0)

        weights[3].wait()
        stat_copy.wait()
        m_own, l_own, s_new = stat[0], stat[1], stat[2]
        m_far = pltpu.roll(srec[0], HALF, axis=1)
        l_far = pltpu.roll(srec[1], HALF, axis=1)
        m = jnp.maximum(m_own, m_far)
        w_own, w_far, w_new = jnp.exp(m_own - m), jnp.exp(m_far - m), jnp.exp(s_new - m)
        denom = l_own * w_own + l_far * w_far + w_new
        c_own, c_far, c_new = w_own / denom, w_far / denom, w_new / denom

        def combine(c, carry):
            num_copy(c).wait()
            for j in range(CH):
                i = c * CH + j
                pick = lane == HALF + i
                own, far, new = [jnp.sum(jnp.where(pick, v, 0.0), axis=1, keepdims=True) for v in (c_own, c_far, c_new)]
                there = pl.ds(pl.multiple_of(i * H, H), H)
                here = pl.ds(pl.multiple_of((HALF + i) * H, H), H)
                num[here, :] = num[here, :] * own + nrec[there, :] * far + heads_of(vn2d, p * HALF + i) * new
            return carry

        lax.fori_loop(0, NCH // 2, combine, 0)

        proj = jnp.zeros((HALF, D), F32)
        for hp in range(H // 2):
            pair = jnp.concatenate([num[pl.ds(HALF * H + hp * 2 + i, HALF, stride=H), :].astype(BF16) for i in range(2)], axis=1)
            proj = proj + mm(pair, wo_v[hp * 256:(hp + 1) * 256, :])
        mine = pl.ds(pl.multiple_of(p * HALF, HALF), HALF)

        def rows(pp, ee):
            return pl.ds(pl.multiple_of(ee * T + pp * HALF, HALF), HALF)

        a_ref[rows(p, e), :] = (x_ref[mine, :].astype(F32) + proj).astype(BF16)

        def gather(i, pp, ee, dev):
            block = a_ref.at[rows(pp, ee)]
            cp = remote(block, block, gs_sem.at[i], gr_sem.at[i], dev)
            cp.start()
            return cp

        copies = [gather(0, p, e, dev_yx), gather(1, p, e, dev_x), gather(2, p, e, dev_y), gather(3, p, e, dev_d)]
        between()
        for i, pp, ee in ((2, 1 - p, e), (1, p, e_x), (0, 1 - p, e_x)):
            copies[i].wait_recv()
            copies.append(gather(len(copies), pp, ee, dev_d))
        for i in range(3, 7):
            copies[i].wait_recv()
        for cp in copies:
            cp.wait_send()

    return start, run


def attn_kernel(x_ref, len_ref, idt_ref, *refs):
    hbm, (a_ref, ida_ref, meta_ref, pos_ref), scr = refs[:6], refs[6:10], refs[10:]
    is_sem, ir_sem = scr[-2:]
    devs = peers()
    p, e, e_x, e_d, e_z, dev_y, dev_x, dev_d, dev_z, dev_yx = devs
    start, run = attn_steps(0, NB, devs, len_ref, hbm, scr[:-2])
    start(2)
    entry_barrier((dev_y, dev_x, dev_d, dev_z, dev_yx))
    mine = (slice(None), slice(None), pl.ds(pl.multiple_of(e * T, T), T))
    ida_ref[mine] = idt_ref[...]
    id_copies = []
    for i, dev in enumerate((dev_x, dev_d, dev_z)):
        id_copies.append(remote(idt_ref, ida_ref.at[mine], is_sem.at[i], ir_sem.at[i], dev))
        id_copies[-1].start()

    def make_tables():
        for cp in id_copies:
            cp.wait()
        for n in range(ida_ref.shape[0]):
            route(ida_ref.at[n], e, meta_ref.at[n], pos_ref.at[n])

    run(x_ref, a_ref, 2, make_tables)


def attn_scratch(nb):
    dma = pltpu.SemaphoreType.DMA
    return [
        pltpu.VMEM((nb, CH, ROWS, HD), BF16), pltpu.VMEM((nb, CH, ROWS, HD), BF16),
        pltpu.VMEM((D, H * HD), BF16), pltpu.VMEM((D, KV * HD), BF16), pltpu.VMEM((D, KV * HD), BF16),
        pltpu.VMEM((H * HD, D), BF16),
        pltpu.VMEM((T * H, HD), F32), pltpu.VMEM((T * KV, HD), F32), pltpu.VMEM((T * KV, HD), F32),
        pltpu.VMEM((T * H, HD), F32), pltpu.VMEM((HALF * H, HD), F32),
        pltpu.VMEM((3, H, T), F32), pltpu.VMEM((2, H, T), F32), pltpu.VMEM((2, H, T), F32),
        dma((2, nb)), dma((4,)), dma((NCH // 2,)), dma((NCH // 2,)), dma(()), dma(()), dma((7,)), dma((7,)),
    ]


def attention(x, cache_len, id_t, hbm):
    vm, sm, hb = (pl.BlockSpec(memory_space=m) for m in (pltpu.VMEM, pltpu.SMEM, pltpu.HBM))
    dma = pltpu.SemaphoreType.DMA
    layers = id_t.shape[0]
    return pl.pallas_call(
        attn_kernel,
        name="attn_0",
        out_shape=[jax.ShapeDtypeStruct((ALL, D), BF16), jax.ShapeDtypeStruct((layers, 8, ALL), I32),
                   jax.ShapeDtypeStruct((layers, 8, 128), I32), jax.ShapeDtypeStruct((layers, 16, ALL), I32)],
        in_specs=[vm, sm, vm] + [hb] * 6,
        out_specs=[vm] * 4,
        scratch_shapes=attn_scratch(NB) + [dma((3,)), dma((3,))],
        compiler_params=pltpu.CompilerParams(collective_id=0, has_side_effects=True, vmem_limit_bytes=61 * MIB),
    )(x, cache_len, id_t, *hbm)


def expert_kernel(layer, part, meta, a_hbm, pos_hbm, w1_ref, w3_ref, w2_ref, mine_ref, theirs_ref,
                  w1b, w3b, w2b, a_ref, pos_ref, u, xs, ym, yt, tail, w_sem, o_sem, i_sem):
    p = lax.axis_index("pool")
    stage = [pltpu.make_async_copy(a_hbm, a_ref, i_sem.at[0]), pltpu.make_async_copy(pos_hbm.at[layer], pos_ref, i_sem.at[1])]
    for cp in stage:
        cp.start()
    r0 = part * NR
    log_mc = STEP_LOG[part]
    MC = 1 << log_mc
    lo, hi = meta[layer, 3 + part, 0], meta[layer, 3 + part, 1]
    odd = (hi - lo) & 1
    lo, hi = jnp.where((odd == 1) & (hi == NE), lo - 1, lo), jnp.where((odd == 1) & (hi < NE), hi + 1, hi)

    def w_copies(i):
        slot = i & (NW - 1)
        return [pltpu.make_async_copy(r.at[layer, i], b.at[slot], w_sem.at[n, slot])
                for n, (r, b) in enumerate(((w1_ref, w1b), (w3_ref, w3b), (w2_ref, w2b)))]

    def start(i, carry):
        for cp in w_copies(i):
            cp.start()
        return carry

    lax.fori_loop(lo, jnp.minimum(lo + NW, hi), start, 0)

    for cp in stage:
        cp.wait()
    u[...] = rms(a_ref[...]).astype(BF16)

    def dispatch(i, carry):
        row = iota((256, ALL), 0) + i * 256
        hit = jnp.zeros((256, ALL), F32)
        for k in range(8):
            hit = jnp.where(pos_ref[k:k + 1, :] == row, 1.0, hit)
        xs[pl.ds(pl.multiple_of(i * 256, 256), 256), :] = mm(hit.astype(BF16), u[...]).astype(BF16)
        return carry

    lax.fori_loop(meta[layer, 1, lo] >> 4, (meta[layer, 1, hi] + 15) >> 4, dispatch, 0)

    def rows_at(i, j):
        slot = i & (NW - 1)
        rows = xs[pl.ds(pl.multiple_of(meta[layer, 1, i] * 16 + j * MC, 16), MC), :]
        both = mm(rows, jnp.concatenate([w1b[slot], w3b[slot]], axis=1))
        act = (jax.nn.silu(both[:, :FF]) * both[:, FF:]).astype(BF16)
        return mm(act, w2b[slot]), pl.ds(jnp.minimum(meta[layer, 2, i] + j * MC - r0, NR) + PAD, MC)

    def targets(to):
        return [ym.at[t // 3, t % 3, to] for t in range(6)] + [yt.at[to]]

    def first_step(i):
        return jnp.maximum(r0 - meta[layer, 2, i], 0) >> log_mc

    def more_steps(i):
        n, offc, first = meta[layer, 0, i], meta[layer, 2, i], first_step(i)

        def step(j, carry):
            y, to = rows_at(i, j)
            keep = iota((MC, 128), 0) < n - j * MC
            for t, ref in enumerate(targets(to)):
                ref[...] = jnp.where(keep, y[:, t * 128:(t + 1) * 128], ref[...])
            return carry

        lax.fori_loop(first + 1, (jnp.minimum(n, r0 + NR - offc) + MC - 1) >> log_mc, step, 0)

    def expert_pair(h, carry):
        pair = [lo + 2 * h, lo + 2 * h + 1]
        for i in pair:
            for cp in w_copies(i):
                cp.wait()
        done = [rows_at(i, first_step(i)) for i in pair]
        for y, to in done:
            for t, ref in enumerate(targets(to)):
                ref[...] = y[:, t * 128:(t + 1) * 128]
        for i in pair:
            more_steps(i)
        for i in pair:
            @pl.when(i + NW < hi)
            def _():
                start(i + NW, 0)
        return carry

    lax.fori_loop(0, (hi - lo) >> 1, expert_pair, 0)
    copies = []
    for n, (q, ref) in enumerate(((1 - p, theirs_ref), (p, mine_ref))):
        for t in range(3):
            copies.append(pltpu.make_async_copy(ym.at[q, t, pl.ds(PAD, NR)], ref.at[pl.ds(t * NR, NR)], o_sem.at[n, t]))
            copies[-1].start()
    top, bot = yt[PAD:PAD + NR // 2, :], yt[PAD + NR // 2:PAD + NR, :]
    left = iota((NR // 2, 128), 1) < 64
    tail[0] = jnp.where(left, top, pltpu.roll(bot, 64, axis=1))
    tail[1] = jnp.where(left, pltpu.roll(top, 64, axis=1), bot)
    for n, (q, ref) in enumerate(((1 - p, theirs_ref), (p, mine_ref))):
        copies.append(pltpu.make_async_copy(tail.at[q], ref.at[pl.ds(3 * NR, NR // 2)], o_sem.at[n, 3]))
        copies[-1].start()
    for cp in copies:
        cp.wait()


def experts(layer, part, a_all, meta, pos, w1, w3, w2):
    vm, sm, hb, anywhere = (pl.BlockSpec(memory_space=m) for m in (pltpu.VMEM, pltpu.SMEM, pltpu.HBM, pl.ANY))
    dma = pltpu.SemaphoreType.DMA
    return pl.pallas_call(
        functools.partial(expert_kernel, layer, part),
        name=f"experts_{layer}_{part}",
        out_shape=[jax.ShapeDtypeStruct((PR, 128), F32)] * 2,
        in_specs=[sm, anywhere, anywhere, hb, hb, hb],
        out_specs=[anywhere, anywhere],
        scratch_shapes=[
            pltpu.VMEM((NW, D, FF), BF16), pltpu.VMEM((NW, D, FF), BF16), pltpu.VMEM((NW, FF, D), BF16),
            pltpu.VMEM((ALL, D), BF16), pltpu.VMEM((16, ALL), I32),
            pltpu.VMEM((ALL, D), BF16), pltpu.VMEM((2304, D), BF16),
            pltpu.VMEM((2, 3, NR + 2 * PAD, 128), F32), pltpu.VMEM((NR + 2 * PAD, 128), F32),
            pltpu.VMEM((2, NR // 2, 128), F32),
            dma((3, NW)), dma((2, 4)), dma((2,)),
        ],
        compiler_params=pltpu.CompilerParams(vmem_limit_bytes=61 * MIB),
        cost_estimate=pl.CostEstimate(flops=4_000_000_000, bytes_accessed=44_000_000 // PARTS, transcendentals=PAIRS * FF // PARTS),
    )(meta, a_all, pos, w1, w3, w2)


def merge_steps(layer, devs, ins, x_ref, scr, beside):
    a_hbm, id_hbm, pos_hbm, mine0_ref, far0_ref, mine1_ref, theirs1_ref, wr_ref = ins
    (a_ref, id_ref, pos_ref, y_own, y_far, wr, gate, base, acc, back, xsend, xfar,
     l_sem, ys_sem, yr_sem, bs_sem, br_sem, fs_sem, fr_sem) = scr
    p, e, e_x, e_d, e_z, dev_y, dev_x, dev_d, dev_z, dev_yx = devs
    loads = [pltpu.make_async_copy(src, dst, l_sem.at[i])
             for i, (src, dst) in enumerate(((wr_ref.at[layer], wr), (mine0_ref, y_own.at[0]), (far0_ref, y_far.at[0]),
                                             (mine1_ref, y_own.at[1]), (a_hbm, a_ref), (id_hbm.at[layer], id_ref),
                                             (pos_hbm.at[layer], pos_ref)))]
    for cp in loads:
        cp.start()
    entry_barrier((dev_y, dev_x, dev_d, dev_z, dev_yx))
    spans = [(t * NR, NR) for t in range(3)] + [(3 * NR, NR // 2)]
    y_copies = [remote(theirs1_ref.at[pl.ds(b, n)], y_far.at[1, pl.ds(b, n)], ys_sem.at[t], yr_sem.at[t], dev_y)
                for t, (b, n) in enumerate(spans)]
    for cp in y_copies:
        cp.start()
    beside()

    for i in (0, 4, 5, 6):
        loads[i].wait()
    u = rms(a_ref[...]).astype(BF16)
    logits = jnp.zeros((ALL, 256), F32)
    rest = wr[...]
    for _ in range(3):
        part = rest.astype(BF16)
        rest = rest - part.astype(F32)
        logits = logits + mm(u, part)
    col = iota((ALL, 256), 1)
    g = [jnp.sum(jnp.where(id_ref[:, k:k + 1] == col, logits, 0.0), axis=1, keepdims=True) for k in range(8)]
    top = functools.reduce(jnp.maximum, g)
    g = [jnp.exp(v - top) for v in g]
    total = functools.reduce(jnp.add, g)
    g = [v / total for v in g]
    pos = [pos_ref[:, 8 + k:9 + k] for k in range(8)]
    lane = iota((ALL, 128), 1)
    for c in range(PAIRS // 128):
        w = jnp.zeros((ALL, 128), F32)
        for k in range(8):
            w = jnp.where(pos[k] == lane + c * 128, g[k], w)
        for i in range(3):
            part = w.astype(BF16)
            w = w - part.astype(F32)
            gate[i, :, c * 128:(c + 1) * 128] = part

    def mix(h, t):
        b, n = spans[t]
        y = (y_own[h, b:b + n, :] + y_far[h, b:b + n, :]).astype(BF16)
        first = h * NR
        if t < 3:
            return sum(mm(gate[i, :, first:first + NR], y) for i in range(3))
        lo, hi = [sum(mm(gate[i, :, first + q * n:first + (q + 1) * n], y) for i in range(3)) for q in range(2)]
        keep = jnp.broadcast_to(p == 0, lo.shape)
        return jnp.where(keep, lo, pltpu.roll(lo, 64, axis=1)) + jnp.where(keep, pltpu.roll(hi, 64, axis=1), hi)

    loads[1].wait()
    loads[2].wait()
    for t in range(4):
        base[t] = mix(0, t)
    loads[3].wait()

    def block_of(ee):
        return pl.ds(pl.multiple_of(ee * T, T), T)

    def give(t):
        cps = [remote(acc.at[t, block_of(ee)], back.at[t, i], bs_sem.at[t, i], br_sem.at[t, i], dev)
               for i, (ee, dev) in enumerate(((e_x, dev_x), (e_z, dev_z), (e_d, dev_d)))]
        for cp in cps:
            cp.start()
        return cps

    def cols(q, t):
        return pl.ds(pl.multiple_of(q * CM + t * 128, 128), 128) if t < 3 else slice(2 * CM, D)

    def finish(t, cps):
        for cp in cps:
            cp.wait_recv()
        total = acc[t, block_of(e), :] + back[t, 0] + back[t, 1] + back[t, 2]
        xsend[t] = (a_ref[block_of(e), cols(p, t)].astype(F32) + total).astype(BF16)
        cp = remote(xsend.at[t], xfar.at[t], fs_sem.at[t], fr_sem.at[t], dev_y)
        cp.start()
        return cp

    given, sent = [], []
    for t in range(4):
        y_copies[t].wait_recv()
        acc[t] = base[t] + mix(1, t)
        given.append(give(t))
        if t >= 1:
            sent.append(finish(t - 1, given[t - 1]))
    sent.append(finish(3, given[3]))
    for t in range(3):
        x_ref[:, cols(p, t)] = xsend[t]
        sent[t].wait()
        x_ref[:, cols(1 - p, t)] = xfar[t]
    sent[3].wait()
    keep_own = (iota((T, 128), 1) // 64) == p
    x_ref[:, 2 * CM:] = jnp.where(keep_own, xsend[3].astype(F32), xfar[3].astype(F32)).astype(BF16)
    for cp in y_copies + [c for cps in given for c in cps]:
        cp.wait_send()


MERGE_IN, MERGE_SCR = 8, 19


def merge_last_kernel(layer, *refs):
    merge_steps(layer, peers(), refs[:MERGE_IN], refs[MERGE_IN], refs[MERGE_IN + 1:], lambda: None)


def merge_next_kernel(layer, *refs):
    ins, len_ref, hbm, a_ref = refs[:MERGE_IN], refs[MERGE_IN], refs[MERGE_IN + 1:MERGE_IN + 7], refs[MERGE_IN + 7]
    x_ref, scr = refs[MERGE_IN + 8], refs[MERGE_IN + 9:]
    devs = peers()
    start, run = attn_steps(layer + 1, NCH, devs, len_ref, hbm, scr[MERGE_SCR:])
    merge_steps(layer, devs, ins, x_ref, scr[:MERGE_SCR], lambda: start(NCH))
    run(x_ref, a_ref, NCH, lambda: None)


def merge_scratch():
    dma = pltpu.SemaphoreType.DMA
    return [
        pltpu.VMEM((ALL, D), BF16), pltpu.VMEM((ALL, 8), I32), pltpu.VMEM((ALL, 16), I32),
        pltpu.VMEM((2, PR, 128), F32), pltpu.VMEM((2, PR, 128), F32),
        pltpu.VMEM((D, 256), F32), pltpu.VMEM((3, ALL, PAIRS), BF16),
        pltpu.VMEM((4, ALL, 128), F32), pltpu.VMEM((4, ALL, 128), F32), pltpu.VMEM((4, 3, T, 128), F32),
        pltpu.VMEM((4, T, 128), BF16), pltpu.VMEM((4, T, 128), BF16),
        dma((7,)), dma((4,)), dma((4,)), dma((4, 3)), dma((4, 3)), dma((4,)), dma((4,)),
    ]


def merge(layer, last, ins, cache_len, hbm):
    vm, sm, hb, anywhere = (pl.BlockSpec(memory_space=m) for m in (pltpu.VMEM, pltpu.SMEM, pltpu.HBM, pl.ANY))
    in_specs = [anywhere] * 7 + [hb]
    params = functools.partial(pltpu.CompilerParams, collective_id=1 + layer, has_side_effects=True)
    if last:
        return pl.pallas_call(
            functools.partial(merge_last_kernel, layer),
            name=f"merge_{layer}",
            out_shape=jax.ShapeDtypeStruct((T, D), BF16),
            in_specs=in_specs,
            out_specs=vm,
            scratch_shapes=merge_scratch(),
            compiler_params=params(vmem_limit_bytes=61 * MIB),
        )(*ins)
    return pl.pallas_call(
        functools.partial(merge_next_kernel, layer),
        name=f"merge_attn_{layer}",
        out_shape=jax.ShapeDtypeStruct((ALL, D), BF16),
        in_specs=in_specs + [sm] + [hb] * 6,
        out_specs=vm,
        scratch_shapes=[pltpu.VMEM((T, D), BF16)] + merge_scratch() + attn_scratch(NCH),
        compiler_params=params(vmem_limit_bytes=67043328),
    )(*ins, cache_len, *hbm)


def solution(mesh):
    tok_spec = P(('dp', 'ep'), None)
    cache_spec = P(None, ('dp', 'ep'), 'pool', None, None)
    up_spec = P(None, 'ep', None, 'pool')
    down_spec = P(None, 'ep', 'pool', None)
    in_specs = (tok_spec, cache_spec, cache_spec, P(('dp', 'ep')), P(), P(), P(), P(), P(), P(None, ('dp', 'ep'), None),
                up_spec, up_spec, down_spec)

    def body(hidden, k_cache, v_cache, cache_len, w_q, w_k, w_v, w_o, w_router, expert_ids, w_one, w_three, w_two):
        layers = w_q.shape[0]
        k = k_cache.reshape(layers, T, ROWS, HD)
        v = v_cache.reshape(layers, T, ROWS, HD)
        id_t = jnp.swapaxes(expert_ids, 1, 2)
        hbm = (k, v, w_q, w_k, w_v, w_o)
        a_all, ids_t, meta, pos_t = attention(hidden, cache_len, id_t, hbm)
        ids, pos = jnp.swapaxes(ids_t, 1, 2), jnp.swapaxes(pos_t, 1, 2)
        for layer in range(layers):
            mine0, theirs0 = experts(layer, 0, a_all, meta, pos_t, w_one, w_three, w_two)
            far0 = lax.ppermute(theirs0, 'pool', [(0, 1), (1, 0)])
            mine1, theirs1 = experts(layer, 1, a_all, meta, pos_t, w_one, w_three, w_two)
            ins = (a_all, ids, pos, mine0, far0, mine1, theirs1, w_router)
            last = layer == layers - 1
            a_all = merge(layer, last, ins, cache_len, hbm)
        return a_all

    return jax.shard_map(body, mesh=mesh, in_specs=in_specs, out_specs=tok_spec, check_vma=False)
```

```python
import functools

import jax
import jax.numpy as jnp
from jax import lax
from jax.experimental import pallas as pl
from jax.experimental.pallas import tpu as pltpu
from jax.sharding import PartitionSpec as P

MESH = pl.DeviceIdType.MESH
F32, BF16, I32 = jnp.float32, jnp.bfloat16, jnp.int32
NORM_EPS = 1e-6
T, D, HD, H = 128, 896, 128, 16
HALF = T // 2
KV = 2
POS = 256
ROWS = POS * KV
CH = 8
NCH = T // CH
HC = NCH // 4
ST = HC * CH
NB = 8
ALL = 4 * T
NE = 64
PAIRS = 1024
FF = 128
NW = 32
CM = 384
PARTS = 2
NR = PAIRS // PARTS
PR = 3 * NR + NR // 2
PAD = 64
STEP_LOG = (6, 5)
MIB = 1024 * 1024


def rms(v):
    v = v.astype(F32)
    return v * lax.rsqrt(jnp.mean(v * v, axis=-1, keepdims=True) + NORM_EPS)


def mm(a, b):
    return jnp.dot(a, b, preferred_element_type=F32)


def iota(shape, dim):
    return lax.broadcasted_iota(I32, shape, dim)


def peers():
    g, p, e = lax.axis_index("dp"), lax.axis_index("pool"), lax.axis_index("ep")
    core = lax.rem(e, 2)
    e_x = lax.rem(e + 2, 4)
    e_d = e + 1 - 2 * core
    e_z = lax.rem(e_d + 2, 4)
    return p, e, e_x, e_d, e_z, (g, 1 - p, e), (g, p, e_x), (g, p, e_d), (g, p, e_z), (g, 1 - p, e_x)


def entry_barrier(targets):
    bar = pltpu.get_barrier_semaphore()
    for dev in targets:
        pl.semaphore_signal(bar, inc=1, device_id=dev, device_id_type=MESH)
    pl.semaphore_wait(bar, len(targets))


def remote(src, dst, send_sem, recv_sem, dev):
    return pltpu.make_async_remote_copy(src_ref=src, dst_ref=dst, send_sem=send_sem, recv_sem=recv_sem,
                                        device_id=dev, device_id_type=MESH)


def route(ids, e, meta, pos):
    sub = iota((128, ALL), 0)
    local = [ids[k:k + 1, :] - e * NE for k in range(8)]
    local = [jnp.where((v >= 0) & (v < NE), v, -1) for v in local]
    mask = jnp.zeros((128, ALL), F32)
    for v in local:
        mask = jnp.where(v == sub, 1.0, mask)
    mask_b = mask.astype(BF16)
    before = (iota((ALL, ALL), 0) < iota((ALL, ALL), 1)).astype(BF16)
    rank = mm(mask_b, before)
    n_col = jnp.broadcast_to(jnp.sum(mask, axis=1, keepdims=True), (128, 128)).astype(I32)
    n_row = lax.dot_general(jnp.ones((8, ALL), BF16), mask_b, (((1,), (1,)), ((), ())),
                            preferred_element_type=F32).astype(I32)
    lower = (iota((128, 128), 1) < iota((128, 128), 0)).astype(BF16)
    upper = (iota((128, 128), 0) < iota((128, 128), 1)).astype(BF16)
    as_b = lambda v: v.astype(F32).astype(BF16)
    off_col = mm(lower, as_b((n_col + 15) >> 4)) * 16.0
    offc_col = mm(lower, as_b(n_col >> 4)) * 16.0 + mm(lower, as_b(n_col & 15))
    off_row = mm(as_b((n_row + 15) >> 4), upper).astype(I32)
    offc_row = (mm(as_b(n_row >> 4), upper) * 16.0 + mm(as_b(n_row & 15), upper)).astype(I32)
    real = iota((8, 128), 1) < NE
    table = [n_row, off_row, offc_row]
    for r in range(PARTS):
        lo = jnp.sum(jnp.where(real & (offc_row + n_row <= r * NR), 1.0, 0.0), axis=1, keepdims=True)
        hi = jnp.sum(jnp.where(real & (offc_row < (r + 1) * NR), 1.0, 0.0), axis=1, keepdims=True)
        table.append(jnp.where(iota((8, 128), 1) == 0, lo, hi).astype(I32))
    row = iota((8, 128), 0)
    packed = jnp.zeros((8, 128), I32)
    for i, v in enumerate(table):
        packed = jnp.where(row == i, v, packed)
    meta[...] = packed
    for base, off in ((0, off_col), (8, offc_col)):
        where_to = off[:, 0:1] + rank + 1.0
        for k in range(8):
            found = jnp.sum(jnp.where(local[k] == sub, where_to, 0.0), axis=0, keepdims=True)
            pos[base + k:base + k + 1, :] = (found - 1.0).astype(I32)


def attn_steps(layer, nb, devs, len_ref, hbm, scr):
    k_ref, v_ref, wq_ref, wk_ref, wv_ref, wo_ref = hbm
    (kbuf, vbuf, wq_v, wk_v, wv_v, wo_v, q2d, kn2d, vn2d, num, nrec, stat, ssend, srec,
     kv_sem, w_sem, ns_sem, nr_sem, ss_sem, sr_sem, gs_sem, gr_sem) = scr
    p, e, e_x, e_d, e_z, dev_y, dev_x, dev_d, dev_z, dev_yx = devs

    def tok_of(c):
        first_half = (1 - p) * HALF + c * CH
        second_half = p * HALF + (c - NCH // 2) * CH
        return pl.multiple_of(jnp.where(c < NCH // 2, first_half, second_half), CH)

    def kv_copies(c):
        slot = c & (nb - 1)
        src = pl.ds(tok_of(c), CH)
        return (pltpu.make_async_copy(k_ref.at[layer, src], kbuf.at[slot], kv_sem.at[0, slot]),
                pltpu.make_async_copy(v_ref.at[layer, src], vbuf.at[slot], kv_sem.at[1, slot]))

    weights = [pltpu.make_async_copy(r.at[layer], b, w_sem.at[i])
               for i, (r, b) in enumerate(((wq_ref, wq_v), (wk_ref, wk_v), (wv_ref, wv_v), (wo_ref, wo_v)))]
    def start_kv(first, last):
        for c in range(first, last):
            for cp in kv_copies(jnp.int32(c)):
                cp.start()

    def start(chunks):
        for cp in weights[:3]:
            cp.start()
        start_kv(0, chunks)

    def run(x_ref, a_ref, started, between):
        normed = rms(x_ref[...]).astype(BF16)
        for cp in weights[:3]:
            cp.wait()
        start_kv(started, nb)
        weights[3].start()
        for hp in range(H // 2):
            pair = mm(normed, wq_v[:, hp * 256:(hp + 1) * 256]).astype(BF16).astype(F32)
            for i in range(2):
                q2d[pl.ds(hp * 2 + i, T, stride=H), :] = pair[:, i * HD:(i + 1) * HD]
        for w, dst in ((wk_v, kn2d), (wv_v, vn2d)):
            pair = mm(normed, w[...]).astype(BF16).astype(F32)
            for i in range(KV):
                dst[pl.ds(i, T, stride=KV), :] = pair[:, i * HD:(i + 1) * HD]

        scale = HD ** -0.5
        col = iota((H, ROWS), 1)
        group_ok = (col & 1) == (iota((H, ROWS), 0) // (H // KV))
        col_pos = jnp.where(group_ok, col >> 1, 1 << 30)
        lane = iota((H, T), 1)

        def heads_of(ref, tok):
            two = ref[pl.ds(tok * KV, KV), :]
            return jnp.concatenate([jnp.broadcast_to(two[i:i + 1], (H // KV, HD)) for i in range(KV)], axis=0)

        def num_copy(c):
            rows = pl.ds(pl.multiple_of(c * (CH * H), CH * H), CH * H)
            return remote(num.at[rows], nrec.at[rows], ns_sem.at[c], nr_sem.at[c], dev_y)

        def stat_copy(h):
            return remote(ssend.at[h], srec.at[h], ss_sem.at[h], sr_sem.at[h], dev_y)

        def chunk(c, carry):
            slot = c & (nb - 1)
            for cp in kv_copies(c):
                cp.wait()
            tok0 = tok_of(c)
            m_all, l_all, n_all = stat[0], stat[1], stat[2]
            for j0 in range(0, CH, 4):
                group = range(j0, j0 + 4)
                qs, ss = {}, {}
                for j in group:
                    qs[j] = q2d[pl.ds(pl.multiple_of((tok0 + j) * H, H), H), :]
                    ss[j] = lax.dot_general(qs[j].astype(BF16), kbuf[slot, j], (((1,), (1,)), ((), ())),
                                            preferred_element_type=F32) * scale
                ps = {}
                for j in group:
                    limit = len_ref[tok0 + j] - p * POS
                    s = jnp.where(col_pos < limit, ss[j], -1e30)
                    s_new = jnp.sum(qs[j] * heads_of(kn2d, tok0 + j), axis=1, keepdims=True) * scale
                    m = jnp.maximum(jnp.max(s, axis=1, keepdims=True), s_new)
                    pr = jnp.exp(s - m)
                    ps[j] = pr.astype(BF16)
                    here = lane == c * CH + j
                    m_all = jnp.where(here, m, m_all)
                    l_all = jnp.where(here, jnp.sum(pr, axis=1, keepdims=True), l_all)
                    n_all = jnp.where(here, s_new, n_all)
                for j in group:
                    num[pl.ds(pl.multiple_of((c * CH + j) * H, H), H), :] = mm(ps[j], vbuf[slot, j])
            stat[0], stat[1], stat[2] = m_all, l_all, n_all

            @pl.when(c + nb < NCH)
            def _():
                for cp in kv_copies(c + nb):
                    cp.start()

            for h in range(2):
                @pl.when(c == (h + 1) * HC - 1)
                def _():
                    ssend[h, 0], ssend[h, 1] = m_all, l_all

            @pl.when((c >= 1) & (c <= NCH // 2))
            def _():
                num_copy(c - 1).start()

            for h in range(2):
                @pl.when(c == (h + 1) * HC)
                def _():
                    stat_copy(h).start()

            return carry

        def rows(pp, ee, h):
            return pl.ds(pl.multiple_of(ee * T + pp * HALF + h * ST, ST), ST)

        def gather(h, i, pp, ee, dev):
            block = a_ref.at[rows(pp, ee, h)]
            cp = remote(block, block, gs_sem.at[h, i], gr_sem.at[h, i], dev)
            cp.start()
            return cp

        def finish(h):
            stat_copy(h).wait()
            m_own, l_own, s_new = stat[0], stat[1], stat[2]
            m_far = pltpu.roll(srec[h, 0], HALF, axis=1)
            l_far = pltpu.roll(srec[h, 1], HALF, axis=1)
            m = jnp.maximum(m_own, m_far)
            w_own, w_far, w_new = jnp.exp(m_own - m), jnp.exp(m_far - m), jnp.exp(s_new - m)
            denom = l_own * w_own + l_far * w_far + w_new
            c_own, c_far, c_new = w_own / denom, w_far / denom, w_new / denom

            def combine(c, carry):
                num_copy(c).wait()
                for j in range(CH):
                    i = c * CH + j
                    pick = lane == HALF + i
                    own, far, new = [jnp.sum(jnp.where(pick, v, 0.0), axis=1, keepdims=True) for v in (c_own, c_far, c_new)]
                    there = pl.ds(pl.multiple_of(i * H, H), H)
                    here = pl.ds(pl.multiple_of((HALF + i) * H, H), H)
                    num[here, :] = num[here, :] * own + nrec[there, :] * far + heads_of(vn2d, p * HALF + i) * new
                return carry

            lax.fori_loop(h * HC, (h + 1) * HC, combine, 0)
            proj = jnp.zeros((ST, D), F32)
            first = (HALF + h * ST) * H
            for hp in range(H // 2):
                pair = jnp.concatenate([num[pl.ds(first + hp * 2 + i, ST, stride=H), :].astype(BF16) for i in range(2)], axis=1)
                proj = proj + mm(pair, wo_v[hp * 256:(hp + 1) * 256, :])
            mine = pl.ds(pl.multiple_of(p * HALF + h * ST, ST), ST)
            a_ref[rows(p, e, h), :] = (x_ref[mine, :].astype(F32) + proj).astype(BF16)
            return [gather(h, i, p, e, dev) for i, dev in enumerate((dev_yx, dev_x, dev_y, dev_d))]

        def forward(h, copies):
            for i, pp, ee in ((2, 1 - p, e), (1, p, e_x), (0, 1 - p, e_x)):
                copies[i].wait_recv()
                copies.append(gather(h, len(copies), pp, ee, dev_d))

        stat[...] = jnp.zeros_like(stat)
        split = NCH - HC
        lax.fori_loop(0, split, chunk, 0)
        weights[3].wait()
        early = finish(0)
        lax.fori_loop(split, NCH, chunk, 0)
        late = finish(1)
        between()
        forward(0, early)
        forward(1, late)
        for copies in (early, late):
            for cp in copies[3:]:
                cp.wait_recv()
            for cp in copies:
                cp.wait_send()

    return start, run


def attn_kernel(x_ref, len_ref, idt_ref, *refs):
    hbm, (a_ref, ida_ref, meta_ref, pos_ref), scr = refs[:6], refs[6:10], refs[10:]
    is_sem, ir_sem = scr[-2:]
    devs = peers()
    p, e, e_x, e_d, e_z, dev_y, dev_x, dev_d, dev_z, dev_yx = devs
    start, run = attn_steps(0, NB, devs, len_ref, hbm, scr[:-2])
    start(2)
    entry_barrier((dev_y, dev_x, dev_d, dev_z, dev_yx))
    mine = (slice(None), slice(None), pl.ds(pl.multiple_of(e * T, T), T))
    ida_ref[mine] = idt_ref[...]
    id_copies = []
    for i, dev in enumerate((dev_x, dev_d, dev_z)):
        id_copies.append(remote(idt_ref, ida_ref.at[mine], is_sem.at[i], ir_sem.at[i], dev))
        id_copies[-1].start()

    def make_tables():
        for cp in id_copies:
            cp.wait()
        for n in range(ida_ref.shape[0]):
            route(ida_ref.at[n], e, meta_ref.at[n], pos_ref.at[n])

    run(x_ref, a_ref, 2, make_tables)


def attn_scratch(nb):
    dma = pltpu.SemaphoreType.DMA
    return [
        pltpu.VMEM((nb, CH, ROWS, HD), BF16), pltpu.VMEM((nb, CH, ROWS, HD), BF16),
        pltpu.VMEM((D, H * HD), BF16), pltpu.VMEM((D, KV * HD), BF16), pltpu.VMEM((D, KV * HD), BF16),
        pltpu.VMEM((H * HD, D), BF16),
        pltpu.VMEM((T * H, HD), F32), pltpu.VMEM((T * KV, HD), F32), pltpu.VMEM((T * KV, HD), F32),
        pltpu.VMEM((T * H, HD), F32), pltpu.VMEM((HALF * H, HD), F32),
        pltpu.VMEM((3, H, T), F32), pltpu.VMEM((2, 2, H, T), F32), pltpu.VMEM((2, 2, H, T), F32),
        dma((2, nb)), dma((4,)), dma((NCH // 2,)), dma((NCH // 2,)), dma((2,)), dma((2,)), dma((2, 7)), dma((2, 7)),
    ]


def attention(x, cache_len, id_t, hbm):
    vm, sm, hb = (pl.BlockSpec(memory_space=m) for m in (pltpu.VMEM, pltpu.SMEM, pltpu.HBM))
    dma = pltpu.SemaphoreType.DMA
    layers = id_t.shape[0]
    return pl.pallas_call(
        attn_kernel,
        name="attn_0",
        out_shape=[jax.ShapeDtypeStruct((ALL, D), BF16), jax.ShapeDtypeStruct((layers, 8, ALL), I32),
                   jax.ShapeDtypeStruct((layers, 8, 128), I32), jax.ShapeDtypeStruct((layers, 16, ALL), I32)],
        in_specs=[vm, sm, vm] + [hb] * 6,
        out_specs=[vm] * 4,
        scratch_shapes=attn_scratch(NB) + [dma((3,)), dma((3,))],
        compiler_params=pltpu.CompilerParams(collective_id=0, has_side_effects=True, vmem_limit_bytes=61 * MIB),
    )(x, cache_len, id_t, *hbm)


def expert_kernel(layer, part, meta, a_hbm, pos_hbm, w1_ref, w3_ref, w2_ref, mine_ref, theirs_ref,
                  w1b, w3b, w2b, a_ref, pos_ref, u, xs, ym, yt, tail, w_sem, o_sem, i_sem):
    p = lax.axis_index("pool")
    stage = [pltpu.make_async_copy(a_hbm, a_ref, i_sem.at[0]), pltpu.make_async_copy(pos_hbm.at[layer], pos_ref, i_sem.at[1])]
    for cp in stage:
        cp.start()
    r0 = part * NR
    log_mc = STEP_LOG[part]
    MC = 1 << log_mc
    lo, hi = meta[layer, 3 + part, 0], meta[layer, 3 + part, 1]
    odd = (hi - lo) & 1
    lo, hi = jnp.where((odd == 1) & (hi == NE), lo - 1, lo), jnp.where((odd == 1) & (hi < NE), hi + 1, hi)

    def w_copies(i):
        slot = i & (NW - 1)
        return [pltpu.make_async_copy(r.at[layer, i], b.at[slot], w_sem.at[n, slot])
                for n, (r, b) in enumerate(((w1_ref, w1b), (w3_ref, w3b), (w2_ref, w2b)))]

    def start(i, carry):
        for cp in w_copies(i):
            cp.start()
        return carry

    lax.fori_loop(lo, jnp.minimum(lo + NW, hi), start, 0)

    for cp in stage:
        cp.wait()
    u[...] = rms(a_ref[...]).astype(BF16)

    def dispatch(i, carry):
        row = iota((256, ALL), 0) + i * 256
        hit = jnp.zeros((256, ALL), F32)
        for k in range(8):
            hit = jnp.where(pos_ref[k:k + 1, :] == row, 1.0, hit)
        xs[pl.ds(pl.multiple_of(i * 256, 256), 256), :] = mm(hit.astype(BF16), u[...]).astype(BF16)
        return carry

    lax.fori_loop(meta[layer, 1, lo] >> 4, (meta[layer, 1, hi] + 15) >> 4, dispatch, 0)

    def rows_at(i, j):
        slot = i & (NW - 1)
        rows = xs[pl.ds(pl.multiple_of(meta[layer, 1, i] * 16 + j * MC, 16), MC), :]
        act = (jax.nn.silu(mm(rows, w1b[slot])) * mm(rows, w3b[slot])).astype(BF16)
        return mm(act, w2b[slot]), pl.ds(jnp.minimum(meta[layer, 2, i] + j * MC - r0, NR) + PAD, MC)

    def targets(to):
        return [ym.at[t // 3, t % 3, to] for t in range(6)] + [yt.at[to]]

    def first_step(i):
        return jnp.maximum(r0 - meta[layer, 2, i], 0) >> log_mc

    def more_steps(i):
        n, offc, first = meta[layer, 0, i], meta[layer, 2, i], first_step(i)

        def step(j, carry):
            y, to = rows_at(i, j)
            keep = iota((MC, 128), 0) < n - j * MC
            for t, ref in enumerate(targets(to)):
                ref[...] = jnp.where(keep, y[:, t * 128:(t + 1) * 128], ref[...])
            return carry

        lax.fori_loop(first + 1, (jnp.minimum(n, r0 + NR - offc) + MC - 1) >> log_mc, step, 0)

    def expert_pair(h, carry):
        pair = [lo + 2 * h, lo + 2 * h + 1]
        for i in pair:
            for cp in w_copies(i):
                cp.wait()
        done = [rows_at(i, first_step(i)) for i in pair]
        for y, to in done:
            for t, ref in enumerate(targets(to)):
                ref[...] = y[:, t * 128:(t + 1) * 128]
        for i in pair:
            more_steps(i)
        for i in pair:
            @pl.when(i + NW < hi)
            def _():
                start(i + NW, 0)
        return carry

    lax.fori_loop(0, (hi - lo) >> 1, expert_pair, 0)
    copies = []
    for n, (q, ref) in enumerate(((1 - p, theirs_ref), (p, mine_ref))):
        for t in range(3):
            copies.append(pltpu.make_async_copy(ym.at[q, t, pl.ds(PAD, NR)], ref.at[pl.ds(t * NR, NR)], o_sem.at[n, t]))
            copies[-1].start()
    top, bot = yt[PAD:PAD + NR // 2, :], yt[PAD + NR // 2:PAD + NR, :]
    left = iota((NR // 2, 128), 1) < 64
    tail[0] = jnp.where(left, top, pltpu.roll(bot, 64, axis=1))
    tail[1] = jnp.where(left, pltpu.roll(top, 64, axis=1), bot)
    for n, (q, ref) in enumerate(((1 - p, theirs_ref), (p, mine_ref))):
        copies.append(pltpu.make_async_copy(tail.at[q], ref.at[pl.ds(3 * NR, NR // 2)], o_sem.at[n, 3]))
        copies[-1].start()
    for cp in copies:
        cp.wait()


def experts(layer, part, a_all, meta, pos, w1, w3, w2):
    vm, sm, hb, anywhere = (pl.BlockSpec(memory_space=m) for m in (pltpu.VMEM, pltpu.SMEM, pltpu.HBM, pl.ANY))
    dma = pltpu.SemaphoreType.DMA
    return pl.pallas_call(
        functools.partial(expert_kernel, layer, part),
        name=f"experts_{layer}_{part}",
        out_shape=[jax.ShapeDtypeStruct((PR, 128), F32)] * 2,
        in_specs=[sm, anywhere, anywhere, hb, hb, hb],
        out_specs=[anywhere, anywhere],
        scratch_shapes=[
            pltpu.VMEM((NW, D, FF), BF16), pltpu.VMEM((NW, D, FF), BF16), pltpu.VMEM((NW, FF, D), BF16),
            pltpu.VMEM((ALL, D), BF16), pltpu.VMEM((16, ALL), I32),
            pltpu.VMEM((ALL, D), BF16), pltpu.VMEM((2304, D), BF16),
            pltpu.VMEM((2, 3, NR + 2 * PAD, 128), F32), pltpu.VMEM((NR + 2 * PAD, 128), F32),
            pltpu.VMEM((2, NR // 2, 128), F32),
            dma((3, NW)), dma((2, 4)), dma((2,)),
        ],
        compiler_params=pltpu.CompilerParams(vmem_limit_bytes=61 * MIB),
        cost_estimate=pl.CostEstimate(flops=4_000_000_000, bytes_accessed=44_000_000 // PARTS, transcendentals=PAIRS * FF // PARTS),
    )(meta, a_all, pos, w1, w3, w2)


def merge_steps(layer, devs, ins, x_ref, scr, beside):
    a_hbm, id_hbm, pos_hbm, mine0_ref, far0_ref, mine1_ref, theirs1_ref, wr_ref = ins
    (a_ref, id_ref, pos_ref, y_own, y_far, wr, gate, base, acc, back, xsend, xfar,
     l_sem, ys_sem, yr_sem, bs_sem, br_sem, fs_sem, fr_sem) = scr
    p, e, e_x, e_d, e_z, dev_y, dev_x, dev_d, dev_z, dev_yx = devs
    loads = [pltpu.make_async_copy(src, dst, l_sem.at[i])
             for i, (src, dst) in enumerate(((wr_ref.at[layer], wr), (mine0_ref, y_own.at[0]), (far0_ref, y_far.at[0]),
                                             (mine1_ref, y_own.at[1]), (a_hbm, a_ref), (id_hbm.at[layer], id_ref),
                                             (pos_hbm.at[layer], pos_ref)))]
    for cp in loads:
        cp.start()
    entry_barrier((dev_y, dev_x, dev_d, dev_z, dev_yx))
    spans = [(t * NR, NR) for t in range(3)] + [(3 * NR, NR // 2)]
    y_copies = [remote(theirs1_ref.at[pl.ds(b, n)], y_far.at[1, pl.ds(b, n)], ys_sem.at[t], yr_sem.at[t], dev_y)
                for t, (b, n) in enumerate(spans)]
    for cp in y_copies:
        cp.start()
    beside()

    for i in (0, 4, 5, 6):
        loads[i].wait()
    u = rms(a_ref[...]).astype(BF16)
    logits = jnp.zeros((ALL, 256), F32)
    rest = wr[...]
    for _ in range(3):
        part = rest.astype(BF16)
        rest = rest - part.astype(F32)
        logits = logits + mm(u, part)
    col = iota((ALL, 256), 1)
    g = [jnp.sum(jnp.where(id_ref[:, k:k + 1] == col, logits, 0.0), axis=1, keepdims=True) for k in range(8)]
    top = functools.reduce(jnp.maximum, g)
    g = [jnp.exp(v - top) for v in g]
    total = functools.reduce(jnp.add, g)
    g = [v / total for v in g]
    pos = [pos_ref[:, 8 + k:9 + k] for k in range(8)]
    lane = iota((ALL, 128), 1)
    def build(c, carry):
        w = jnp.zeros((ALL, 128), F32)
        for k in range(8):
            w = jnp.where(pos[k] == lane + c * 128, g[k], w)
        for i in range(3):
            part = w.astype(BF16)
            w = w - part.astype(F32)
            gate[i, :, pl.ds(pl.multiple_of(c * 128, 128), 128)] = part
        return carry

    lax.fori_loop(0, PAIRS // 128, build, 0)

    def mix(h, t):
        b, n = spans[t]
        y = (y_own[h, b:b + n, :] + y_far[h, b:b + n, :]).astype(BF16)
        first = h * NR
        if t < 3:
            return sum(mm(gate[i, :, first:first + NR], y) for i in range(3))
        lo, hi = [sum(mm(gate[i, :, first + q * n:first + (q + 1) * n], y) for i in range(3)) for q in range(2)]
        keep = jnp.broadcast_to(p == 0, lo.shape)
        return jnp.where(keep, lo, pltpu.roll(lo, 64, axis=1)) + jnp.where(keep, pltpu.roll(hi, 64, axis=1), hi)

    loads[1].wait()
    loads[2].wait()
    for t in range(4):
        base[t] = mix(0, t)
    loads[3].wait()

    def block_of(ee):
        return pl.ds(pl.multiple_of(ee * T, T), T)

    left = iota((T // 2, 128), 1) < 64
    keep0 = jnp.broadcast_to(p == 0, left.shape)

    def swap(v):
        return pltpu.roll(v, 64, axis=1)

    def pack(v):
        top, bot = v[:T // 2], v[T // 2:]
        return jnp.where(left, jnp.where(keep0, top, swap(top)), jnp.where(keep0, swap(bot), bot))

    def span_of(ee, t):
        n = T if t < 3 else T // 2
        return pl.ds(pl.multiple_of(ee * n, n), n), pl.ds(0, n)

    def give(t):
        cps = []
        for i, (ee, dev) in enumerate(((e_x, dev_x), (e_z, dev_z), (e_d, dev_d))):
            src, dst = span_of(ee, t)
            cps.append(remote(acc.at[t, src], back.at[t, i, dst], bs_sem.at[t, i], br_sem.at[t, i], dev))
        for cp in cps:
            cp.start()
        return cps

    def cols(q, t):
        return pl.ds(pl.multiple_of(q * CM + t * 128, 128), 128) if t < 3 else slice(2 * CM, D)

    def finish(t, cps):
        for cp in cps:
            cp.wait_recv()
        src, dst = span_of(e, t)
        total = acc[t, src, :] + back[t, 0, dst, :] + back[t, 1, dst, :] + back[t, 2, dst, :]
        a_own = a_ref[block_of(e), cols(p, t)].astype(F32)
        xsend[t, dst, :] = ((a_own if t < 3 else pack(a_own)) + total).astype(BF16)
        cp = remote(xsend.at[t, dst], xfar.at[t, dst], fs_sem.at[t], fr_sem.at[t], dev_y)
        cp.start()
        return cp

    given, sent = [], []
    for t in range(4):
        y_copies[t].wait_recv()
        full = base[t] + mix(1, t)
        if t < 3:
            acc[t] = full
        else:
            for b in range(ALL // T):
                acc[t, b * T // 2:(b + 1) * T // 2, :] = pack(full[b * T:(b + 1) * T])
        given.append(give(t))
        if t >= 1:
            sent.append(finish(t - 1, given[t - 1]))
    sent.append(finish(3, given[3]))
    for t in range(3):
        x_ref[:, cols(p, t)] = xsend[t]
        sent[t].wait()
        x_ref[:, cols(1 - p, t)] = xfar[t]
    sent[3].wait()
    own, far = xsend[3, :T // 2, :].astype(F32), xfar[3, :T // 2, :].astype(F32)
    q0, q1 = jnp.where(keep0, own, far), jnp.where(keep0, far, own)
    x_ref[:T // 2, 2 * CM:] = jnp.where(left, q0, swap(q1)).astype(BF16)
    x_ref[T // 2:, 2 * CM:] = jnp.where(left, swap(q0), q1).astype(BF16)
    for cp in y_copies + [c for cps in given for c in cps]:
        cp.wait_send()


MERGE_IN, MERGE_SCR = 8, 19


def merge_last_kernel(layer, *refs):
    merge_steps(layer, peers(), refs[:MERGE_IN], refs[MERGE_IN], refs[MERGE_IN + 1:], lambda: None)


def merge_next_kernel(layer, *refs):
    ins, len_ref, hbm, a_ref = refs[:MERGE_IN], refs[MERGE_IN], refs[MERGE_IN + 1:MERGE_IN + 7], refs[MERGE_IN + 7]
    x_ref, scr = refs[MERGE_IN + 8], refs[MERGE_IN + 9:]
    devs = peers()
    start, run = attn_steps(layer + 1, NCH, devs, len_ref, hbm, scr[MERGE_SCR:])
    merge_steps(layer, devs, ins, x_ref, scr[:MERGE_SCR], lambda: start(NCH))
    run(x_ref, a_ref, NCH, lambda: None)


def merge_scratch():
    dma = pltpu.SemaphoreType.DMA
    return [
        pltpu.VMEM((ALL, D), BF16), pltpu.VMEM((ALL, 8), I32), pltpu.VMEM((ALL, 16), I32),
        pltpu.VMEM((2, PR, 128), F32), pltpu.VMEM((2, PR, 128), F32),
        pltpu.VMEM((D, 256), F32), pltpu.VMEM((3, ALL, PAIRS), BF16),
        pltpu.VMEM((4, ALL, 128), F32), pltpu.VMEM((4, ALL, 128), F32), pltpu.VMEM((4, 3, T, 128), F32),
        pltpu.VMEM((4, T, 128), BF16), pltpu.VMEM((4, T, 128), BF16),
        dma((7,)), dma((4,)), dma((4,)), dma((4, 3)), dma((4, 3)), dma((4,)), dma((4,)),
    ]


def merge(layer, last, ins, cache_len, hbm):
    vm, sm, hb, anywhere = (pl.BlockSpec(memory_space=m) for m in (pltpu.VMEM, pltpu.SMEM, pltpu.HBM, pl.ANY))
    in_specs = [anywhere] * 7 + [hb]
    params = functools.partial(pltpu.CompilerParams, collective_id=1 + layer, has_side_effects=True)
    if last:
        return pl.pallas_call(
            functools.partial(merge_last_kernel, layer),
            name=f"merge_{layer}",
            out_shape=jax.ShapeDtypeStruct((T, D), BF16),
            in_specs=in_specs,
            out_specs=vm,
            scratch_shapes=merge_scratch(),
            compiler_params=params(vmem_limit_bytes=61 * MIB),
        )(*ins)
    return pl.pallas_call(
        functools.partial(merge_next_kernel, layer),
        name=f"merge_attn_{layer}",
        out_shape=jax.ShapeDtypeStruct((ALL, D), BF16),
        in_specs=in_specs + [sm] + [hb] * 6,
        out_specs=vm,
        scratch_shapes=[pltpu.VMEM((T, D), BF16)] + merge_scratch() + attn_scratch(NCH),
        compiler_params=params(vmem_limit_bytes=67043328),
    )(*ins, cache_len, *hbm)


def solution(mesh):
    tok_spec = P(('dp', 'ep'), None)
    cache_spec = P(None, ('dp', 'ep'), 'pool', None, None)
    up_spec = P(None, 'ep', None, 'pool')
    down_spec = P(None, 'ep', 'pool', None)
    in_specs = (tok_spec, cache_spec, cache_spec, P(('dp', 'ep')), P(), P(), P(), P(), P(), P(None, ('dp', 'ep'), None),
                up_spec, up_spec, down_spec)

    def body(hidden, k_cache, v_cache, cache_len, w_q, w_k, w_v, w_o, w_router, expert_ids, w_one, w_three, w_two):
        layers = w_q.shape[0]
        k = k_cache.reshape(layers, T, ROWS, HD)
        v = v_cache.reshape(layers, T, ROWS, HD)
        id_t = jnp.swapaxes(expert_ids, 1, 2)
        hbm = (k, v, w_q, w_k, w_v, w_o)
        a_all, ids_t, meta, pos_t = attention(hidden, cache_len, id_t, hbm)
        ids, pos = jnp.swapaxes(ids_t, 1, 2), jnp.swapaxes(pos_t, 1, 2)
        for layer in range(layers):
            mine0, theirs0 = experts(layer, 0, a_all, meta, pos_t, w_one, w_three, w_two)
            far0 = lax.ppermute(theirs0, 'pool', [(0, 1), (1, 0)])
            mine1, theirs1 = experts(layer, 1, a_all, meta, pos_t, w_one, w_three, w_two)
            ins = (a_all, ids, pos, mine0, far0, mine1, theirs1, w_router)
            last = layer == layers - 1
            a_all = merge(layer, last, ins, cache_len, hbm)
        return a_all

    return jax.shard_map(body, mesh=mesh, in_specs=in_specs, out_specs=tok_spec, check_vma=False)
```

```python
import functools

import jax
import jax.numpy as jnp
from jax import lax
from jax.experimental import pallas as pl
from jax.experimental.pallas import tpu as pltpu
from jax.sharding import PartitionSpec as P

MESH = pl.DeviceIdType.MESH
F32, BF16, I32 = jnp.float32, jnp.bfloat16, jnp.int32
NORM_EPS = 1e-6
T, D, HD, H = 128, 896, 128, 16
HALF = T // 2
KV = 2
POS = 256
ROWS = POS * KV
CH = 8
NCH = T // CH
HC = NCH // 4
ST = HC * CH
NB = 8
ALL = 4 * T
NE = 64
PAIRS = 1024
FF = 128
NW = 32
CM = 384
PARTS = 2
NR = PAIRS // PARTS
PR = 3 * NR + NR // 2
PAD = 64
STEP_LOG = (6, 5)
LN = 128
MIB = 1024 * 1024


def rms(v):
    v = v.astype(F32)
    return v * lax.rsqrt(jnp.mean(v * v, axis=-1, keepdims=True) + NORM_EPS)


def mm(a, b):
    return jnp.dot(a, b, preferred_element_type=F32)


def iota(shape, dim):
    return lax.broadcasted_iota(I32, shape, dim)


def peers():
    g, p, e = lax.axis_index("dp"), lax.axis_index("pool"), lax.axis_index("ep")
    core = lax.rem(e, 2)
    e_x = lax.rem(e + 2, 4)
    e_d = e + 1 - 2 * core
    e_z = lax.rem(e_d + 2, 4)
    return p, e, e_x, e_d, e_z, (g, 1 - p, e), (g, p, e_x), (g, p, e_d), (g, p, e_z), (g, 1 - p, e_x)


def entry_barrier(targets):
    bar = pltpu.get_barrier_semaphore()
    for dev in targets:
        pl.semaphore_signal(bar, inc=1, device_id=dev, device_id_type=MESH)
    pl.semaphore_wait(bar, len(targets))


def remote(src, dst, send_sem, recv_sem, dev):
    return pltpu.make_async_remote_copy(src_ref=src, dst_ref=dst, send_sem=send_sem, recv_sem=recv_sem,
                                        device_id=dev, device_id_type=MESH)


def route(ids, e, meta, pos, cols):
    sub = iota((LN, ALL), 0)
    local = [ids[k:k + 1, :] - e * NE for k in range(8)]
    local = [jnp.where((v >= 0) & (v < NE), v, -1) for v in local]
    mask = jnp.zeros((LN, ALL), F32)
    for v in local:
        mask = jnp.where(v == sub, 1.0, mask)
    mask_b = mask.astype(BF16)
    before = (iota((ALL, ALL), 0) < iota((ALL, ALL), 1)).astype(BF16)
    rank = mm(mask_b, before)
    n_col = jnp.broadcast_to(jnp.sum(mask, axis=1, keepdims=True), (LN, LN)).astype(I32)
    n_row = lax.dot_general(jnp.ones((8, ALL), BF16), mask_b, (((1,), (1,)), ((), ())),
                            preferred_element_type=F32).astype(I32)
    lower = (iota((LN, LN), 1) < iota((LN, LN), 0)).astype(BF16)
    upper = (iota((LN, LN), 0) < iota((LN, LN), 1)).astype(BF16)
    as_b = lambda v: v.astype(F32).astype(BF16)
    off_col = mm(lower, as_b((n_col + 15) >> 4)) * 16.0
    offc_col = mm(lower, as_b(n_col >> 4)) * 16.0 + mm(lower, as_b(n_col & 15))
    off_row = mm(as_b((n_row + 15) >> 4), upper).astype(I32)
    offc_row = (mm(as_b(n_row >> 4), upper) * 16.0 + mm(as_b(n_row & 15), upper)).astype(I32)
    real = iota((8, LN), 1) < NE
    table = [n_row, off_row, offc_row]
    for r in range(PARTS):
        lo = jnp.sum(jnp.where(real & (offc_row + n_row <= r * NR), 1.0, 0.0), axis=1, keepdims=True)
        hi = jnp.sum(jnp.where(real & (offc_row < (r + 1) * NR), 1.0, 0.0), axis=1, keepdims=True)
        table.append(jnp.where(iota((8, LN), 1) == 0, lo, hi).astype(I32))
    row = iota((8, LN), 0)
    packed = jnp.zeros((8, LN), I32)
    for i, v in enumerate(table):
        packed = jnp.where(row == i, v, packed)
    meta[...] = packed
    found = []
    for off in (off_col, offc_col):
        where_to = off[:, 0:1] + rank + 1.0
        found += [jnp.sum(jnp.where(v == sub, where_to, 0.0), axis=0, keepdims=True) - 1.0 for v in local]
    for k in range(8):
        pos[k:k + 1, :] = found[k].astype(I32)
    row = iota((LN, ALL), 0)
    table = jnp.zeros((LN, ALL), F32)
    for k in range(8):
        table = jnp.where(row == k, found[8 + k], table)
        table = jnp.where(row == 8 + k, ids[k:k + 1, :].astype(F32), table)
    cols[...] = table.T.astype(I32)


def attn_steps(layer, nb, devs, len_ref, hbm, scr):
    k_ref, v_ref, wq_ref, wk_ref, wv_ref, wo_ref = hbm
    (kbuf, vbuf, wq_v, wk_v, wv_v, wo_v, q2d, kn2d, vn2d, num, nrec, stat, ssend, srec,
     kv_sem, w_sem, ns_sem, nr_sem, ss_sem, sr_sem, gs_sem, gr_sem) = scr
    p, e, e_x, e_d, e_z, dev_y, dev_x, dev_d, dev_z, dev_yx = devs

    def tok_of(c):
        first_half = (1 - p) * HALF + c * CH
        second_half = p * HALF + (c - NCH // 2) * CH
        return pl.multiple_of(jnp.where(c < NCH // 2, first_half, second_half), CH)

    def kv_copies(c):
        slot = c & (nb - 1)
        src = pl.ds(tok_of(c), CH)
        return (pltpu.make_async_copy(k_ref.at[layer, src], kbuf.at[slot], kv_sem.at[0, slot]),
                pltpu.make_async_copy(v_ref.at[layer, src], vbuf.at[slot], kv_sem.at[1, slot]))

    weights = [pltpu.make_async_copy(r.at[layer], b, w_sem.at[i])
               for i, (r, b) in enumerate(((wq_ref, wq_v), (wk_ref, wk_v), (wv_ref, wv_v), (wo_ref, wo_v)))]
    def start_kv(first, last):
        for c in range(first, last):
            for cp in kv_copies(jnp.int32(c)):
                cp.start()

    def start(chunks):
        for cp in weights[:3]:
            cp.start()
        start_kv(0, chunks)

    def run(x_ref, a_ref, started, between):
        normed = rms(x_ref[...]).astype(BF16)
        for cp in weights[:3]:
            cp.wait()
        start_kv(started, nb)
        weights[3].start()
        for hp in range(H // 2):
            pair = mm(normed, wq_v[:, hp * 256:(hp + 1) * 256]).astype(BF16).astype(F32)
            for i in range(2):
                q2d[pl.ds(hp * 2 + i, T, stride=H), :] = pair[:, i * HD:(i + 1) * HD]
        for w, dst in ((wk_v, kn2d), (wv_v, vn2d)):
            pair = mm(normed, w[...]).astype(BF16).astype(F32)
            for i in range(KV):
                dst[pl.ds(i, T, stride=KV), :] = pair[:, i * HD:(i + 1) * HD]

        scale = HD ** -0.5
        col = iota((H, ROWS), 1)
        group_ok = (col & 1) == (iota((H, ROWS), 0) // (H // KV))
        col_pos = jnp.where(group_ok, col >> 1, 1 << 30)
        lane = iota((H, T), 1)

        def heads_of(ref, tok):
            two = ref[pl.ds(tok * KV, KV), :]
            return jnp.concatenate([jnp.broadcast_to(two[i:i + 1], (H // KV, HD)) for i in range(KV)], axis=0)

        def num_copy(c):
            rows = pl.ds(pl.multiple_of(c * (CH * H), CH * H), CH * H)
            return remote(num.at[rows], nrec.at[rows], ns_sem.at[c], nr_sem.at[c], dev_y)

        def stat_copy(h):
            return remote(ssend.at[h], srec.at[h], ss_sem.at[h], sr_sem.at[h], dev_y)

        def chunk(c, carry):
            slot = c & (nb - 1)
            for cp in kv_copies(c):
                cp.wait()
            tok0 = tok_of(c)
            m_all, l_all, n_all = stat[0], stat[1], stat[2]
            for j0 in range(0, CH, 4):
                group = range(j0, j0 + 4)
                qs, ss = {}, {}
                for j in group:
                    qs[j] = q2d[pl.ds(pl.multiple_of((tok0 + j) * H, H), H), :]
                    ss[j] = lax.dot_general(qs[j].astype(BF16), kbuf[slot, j], (((1,), (1,)), ((), ())),
                                            preferred_element_type=F32) * scale
                ps = {}
                for j in group:
                    limit = len_ref[tok0 + j] - p * POS
                    s = jnp.where(col_pos < limit, ss[j], -1e30)
                    s_new = jnp.sum(qs[j] * heads_of(kn2d, tok0 + j), axis=1, keepdims=True) * scale
                    m = jnp.maximum(jnp.max(s, axis=1, keepdims=True), s_new)
                    pr = jnp.exp(s - m)
                    ps[j] = pr.astype(BF16)
                    here = lane == c * CH + j
                    m_all = jnp.where(here, m, m_all)
                    l_all = jnp.where(here, jnp.sum(pr, axis=1, keepdims=True), l_all)
                    n_all = jnp.where(here, s_new, n_all)
                for j in group:
                    num[pl.ds(pl.multiple_of((c * CH + j) * H, H), H), :] = mm(ps[j], vbuf[slot, j])
            stat[0], stat[1], stat[2] = m_all, l_all, n_all

            @pl.when(c + nb < NCH)
            def _():
                for cp in kv_copies(c + nb):
                    cp.start()

            for h in range(2):
                @pl.when(c == (h + 1) * HC - 1)
                def _():
                    ssend[h, 0], ssend[h, 1] = m_all, l_all

            @pl.when((c >= 1) & (c <= NCH // 2))
            def _():
                num_copy(c - 1).start()

            for h in range(2):
                @pl.when(c == (h + 1) * HC)
                def _():
                    stat_copy(h).start()

            return carry

        def rows(pp, ee, h):
            return pl.ds(pl.multiple_of(ee * T + pp * HALF + h * ST, ST), ST)

        def gather(h, i, pp, ee, dev):
            block = a_ref.at[rows(pp, ee, h)]
            cp = remote(block, block, gs_sem.at[h, i], gr_sem.at[h, i], dev)
            cp.start()
            return cp

        def finish(h):
            stat_copy(h).wait()
            m_own, l_own, s_new = stat[0], stat[1], stat[2]
            m_far = pltpu.roll(srec[h, 0], HALF, axis=1)
            l_far = pltpu.roll(srec[h, 1], HALF, axis=1)
            m = jnp.maximum(m_own, m_far)
            w_own, w_far, w_new = jnp.exp(m_own - m), jnp.exp(m_far - m), jnp.exp(s_new - m)
            denom = l_own * w_own + l_far * w_far + w_new
            c_own, c_far, c_new = w_own / denom, w_far / denom, w_new / denom

            def combine(c, carry):
                num_copy(c).wait()
                for j in range(CH):
                    i = c * CH + j
                    pick = lane == HALF + i
                    own, far, new = [jnp.sum(jnp.where(pick, v, 0.0), axis=1, keepdims=True) for v in (c_own, c_far, c_new)]
                    there = pl.ds(pl.multiple_of(i * H, H), H)
                    here = pl.ds(pl.multiple_of((HALF + i) * H, H), H)
                    num[here, :] = num[here, :] * own + nrec[there, :] * far + heads_of(vn2d, p * HALF + i) * new
                return carry

            lax.fori_loop(h * HC, (h + 1) * HC, combine, 0)
            proj = jnp.zeros((ST, D), F32)
            first = (HALF + h * ST) * H
            for hp in range(H // 2):
                pair = jnp.concatenate([num[pl.ds(first + hp * 2 + i, ST, stride=H), :].astype(BF16) for i in range(2)], axis=1)
                proj = proj + mm(pair, wo_v[hp * 256:(hp + 1) * 256, :])
            mine = pl.ds(pl.multiple_of(p * HALF + h * ST, ST), ST)
            a_ref[rows(p, e, h), :] = (x_ref[mine, :].astype(F32) + proj).astype(BF16)
            return [gather(h, i, p, e, dev) for i, dev in enumerate((dev_yx, dev_x, dev_y, dev_d))]

        def forward(h, copies):
            for i, pp, ee in ((2, 1 - p, e), (1, p, e_x), (0, 1 - p, e_x)):
                copies[i].wait_recv()
                copies.append(gather(h, len(copies), pp, ee, dev_d))

        stat[...] = jnp.zeros_like(stat)
        split = NCH - HC
        lax.fori_loop(0, split, chunk, 0)
        weights[3].wait()
        early = finish(0)
        lax.fori_loop(split, NCH, chunk, 0)
        late = finish(1)
        between()
        forward(0, early)
        forward(1, late)
        for copies in (early, late):
            for cp in copies[3:]:
                cp.wait_recv()
            for cp in copies:
                cp.wait_send()

    return start, run


def attn_kernel(x_ref, len_ref, idt_ref, *refs):
    hbm, (a_ref, meta_ref, pos_ref, cols_ref), (ida_ref, *scr) = refs[:6], refs[6:10], refs[10:]
    is_sem, ir_sem = scr[-2:]
    devs = peers()
    p, e, e_x, e_d, e_z, dev_y, dev_x, dev_d, dev_z, dev_yx = devs
    start, run = attn_steps(0, NB, devs, len_ref, hbm, scr[:-2])
    start(2)
    entry_barrier((dev_y, dev_x, dev_d, dev_z, dev_yx))
    mine = (slice(None), slice(None), pl.ds(pl.multiple_of(e * T, T), T))
    ida_ref[mine] = idt_ref[...]
    id_copies = []
    for i, dev in enumerate((dev_x, dev_d, dev_z)):
        id_copies.append(remote(idt_ref, ida_ref.at[mine], is_sem.at[i], ir_sem.at[i], dev))
        id_copies[-1].start()

    def make_tables():
        for cp in id_copies:
            cp.wait()
        for n in range(ida_ref.shape[0]):
            route(ida_ref.at[n], e, meta_ref.at[n], pos_ref.at[n], cols_ref.at[n])

    run(x_ref, a_ref, 2, make_tables)


def attn_scratch(nb):
    dma = pltpu.SemaphoreType.DMA
    return [
        pltpu.VMEM((nb, CH, ROWS, HD), BF16), pltpu.VMEM((nb, CH, ROWS, HD), BF16),
        pltpu.VMEM((D, H * HD), BF16), pltpu.VMEM((D, KV * HD), BF16), pltpu.VMEM((D, KV * HD), BF16),
        pltpu.VMEM((H * HD, D), BF16),
        pltpu.VMEM((T * H, HD), F32), pltpu.VMEM((T * KV, HD), F32), pltpu.VMEM((T * KV, HD), F32),
        pltpu.VMEM((T * H, HD), F32), pltpu.VMEM((HALF * H, HD), F32),
        pltpu.VMEM((3, H, T), F32), pltpu.VMEM((2, 2, H, T), F32), pltpu.VMEM((2, 2, H, T), F32),
        dma((2, nb)), dma((4,)), dma((NCH // 2,)), dma((NCH // 2,)), dma((2,)), dma((2,)), dma((2, 7)), dma((2, 7)),
    ]


def attention(x, cache_len, id_t, hbm):
    vm, sm, hb = (pl.BlockSpec(memory_space=m) for m in (pltpu.VMEM, pltpu.SMEM, pltpu.HBM))
    dma = pltpu.SemaphoreType.DMA
    layers = id_t.shape[0]
    return pl.pallas_call(
        attn_kernel,
        name="attn_0",
        out_shape=[jax.ShapeDtypeStruct((ALL, D), BF16), jax.ShapeDtypeStruct((layers, 8, LN), I32),
                   jax.ShapeDtypeStruct((layers, 8, ALL), I32), jax.ShapeDtypeStruct((layers, ALL, LN), I32)],
        in_specs=[vm, sm, vm] + [hb] * 6,
        out_specs=[vm] * 4,
        scratch_shapes=[pltpu.VMEM((layers, 8, ALL), I32)] + attn_scratch(NB) + [dma((3,)), dma((3,))],
        compiler_params=pltpu.CompilerParams(collective_id=0, has_side_effects=True, vmem_limit_bytes=61 * MIB),
    )(x, cache_len, id_t, *hbm)


def expert_kernel(layer, part, meta, a_hbm, pos_hbm, w1_ref, w3_ref, w2_ref, mine_ref, theirs_ref,
                  w1b, w3b, w2b, a_ref, pos_ref, u, xs, ym, yt, tail, w_sem, o_sem, i_sem):
    p = lax.axis_index("pool")
    stage = [pltpu.make_async_copy(a_hbm, a_ref, i_sem.at[0]), pltpu.make_async_copy(pos_hbm.at[layer], pos_ref, i_sem.at[1])]
    for cp in stage:
        cp.start()
    r0 = part * NR
    log_mc = STEP_LOG[part]
    MC = 1 << log_mc
    lo, hi = meta[layer, 3 + part, 0], meta[layer, 3 + part, 1]
    odd = (hi - lo) & 1
    lo, hi = jnp.where((odd == 1) & (hi == NE), lo - 1, lo), jnp.where((odd == 1) & (hi < NE), hi + 1, hi)

    def w_copies(i):
        slot = i & (NW - 1)
        return [pltpu.make_async_copy(r.at[layer, i], b.at[slot], w_sem.at[n, slot])
                for n, (r, b) in enumerate(((w1_ref, w1b), (w3_ref, w3b), (w2_ref, w2b)))]

    def start(i, carry):
        for cp in w_copies(i):
            cp.start()
        return carry

    lax.fori_loop(lo, jnp.minimum(lo + NW, hi), start, 0)

    for cp in stage:
        cp.wait()
    u[...] = rms(a_ref[...]).astype(BF16)

    def dispatch(i, carry):
        row = iota((256, ALL), 0) + i * 256
        hit = jnp.zeros((256, ALL), F32)
        for k in range(8):
            hit = jnp.where(pos_ref[k:k + 1, :] == row, 1.0, hit)
        xs[pl.ds(pl.multiple_of(i * 256, 256), 256), :] = mm(hit.astype(BF16), u[...]).astype(BF16)
        return carry

    lax.fori_loop(meta[layer, 1, lo] >> 4, (meta[layer, 1, hi] + 15) >> 4, dispatch, 0)

    def rows_at(i, j):
        slot = i & (NW - 1)
        rows = xs[pl.ds(pl.multiple_of(meta[layer, 1, i] * 16 + j * MC, 16), MC), :]
        act = (jax.nn.silu(mm(rows, w1b[slot])) * mm(rows, w3b[slot])).astype(BF16)
        return mm(act, w2b[slot]), pl.ds(jnp.minimum(meta[layer, 2, i] + j * MC - r0, NR) + PAD, MC)

    def targets(to):
        return [ym.at[t // 3, t % 3, to] for t in range(6)] + [yt.at[to]]

    def first_step(i):
        return jnp.maximum(r0 - meta[layer, 2, i], 0) >> log_mc

    def more_steps(i):
        n, offc, first = meta[layer, 0, i], meta[layer, 2, i], first_step(i)

        def step(j, carry):
            y, to = rows_at(i, j)
            keep = iota((MC, LN), 0) < n - j * MC
            for t, ref in enumerate(targets(to)):
                ref[...] = jnp.where(keep, y[:, t * LN:(t + 1) * LN], ref[...])
            return carry

        lax.fori_loop(first + 1, (jnp.minimum(n, r0 + NR - offc) + MC - 1) >> log_mc, step, 0)

    def expert_pair(h, carry):
        pair = [lo + 2 * h, lo + 2 * h + 1]
        for i in pair:
            for cp in w_copies(i):
                cp.wait()
        done = [rows_at(i, first_step(i)) for i in pair]
        for y, to in done:
            for t, ref in enumerate(targets(to)):
                ref[...] = y[:, t * LN:(t + 1) * LN]
        for i in pair:
            more_steps(i)
        for i in pair:
            @pl.when(i + NW < hi)
            def _():
                start(i + NW, 0)
        return carry

    lax.fori_loop(0, (hi - lo) >> 1, expert_pair, 0)
    copies = []
    for n, (q, ref) in enumerate(((1 - p, theirs_ref), (p, mine_ref))):
        for t in range(3):
            copies.append(pltpu.make_async_copy(ym.at[q, t, pl.ds(PAD, NR)], ref.at[pl.ds(t * NR, NR)], o_sem.at[n, t]))
            copies[-1].start()
    top, bot = yt[PAD:PAD + NR // 2, :], yt[PAD + NR // 2:PAD + NR, :]
    left = iota((NR // 2, LN), 1) < 64
    tail[0] = jnp.where(left, top, pltpu.roll(bot, 64, axis=1))
    tail[1] = jnp.where(left, pltpu.roll(top, 64, axis=1), bot)
    for n, (q, ref) in enumerate(((1 - p, theirs_ref), (p, mine_ref))):
        copies.append(pltpu.make_async_copy(tail.at[q], ref.at[pl.ds(3 * NR, NR // 2)], o_sem.at[n, 3]))
        copies[-1].start()
    for cp in copies:
        cp.wait()


def experts(layer, part, a_all, meta, pos, w1, w3, w2):
    vm, sm, hb, anywhere = (pl.BlockSpec(memory_space=m) for m in (pltpu.VMEM, pltpu.SMEM, pltpu.HBM, pl.ANY))
    dma = pltpu.SemaphoreType.DMA
    return pl.pallas_call(
        functools.partial(expert_kernel, layer, part),
        name=f"experts_{layer}_{part}",
        out_shape=[jax.ShapeDtypeStruct((PR, LN), F32)] * 2,
        in_specs=[sm, anywhere, anywhere, hb, hb, hb],
        out_specs=[anywhere, anywhere],
        scratch_shapes=[
            pltpu.VMEM((NW, D, FF), BF16), pltpu.VMEM((NW, D, FF), BF16), pltpu.VMEM((NW, FF, D), BF16),
            pltpu.VMEM((ALL, D), BF16), pltpu.VMEM((8, ALL), I32),
            pltpu.VMEM((ALL, D), BF16), pltpu.VMEM((2304, D), BF16),
            pltpu.VMEM((2, 3, NR + 2 * PAD, LN), F32), pltpu.VMEM((NR + 2 * PAD, LN), F32),
            pltpu.VMEM((2, NR // 2, LN), F32),
            dma((3, NW)), dma((2, 4)), dma((2,)),
        ],
        compiler_params=pltpu.CompilerParams(vmem_limit_bytes=67043328),
        cost_estimate=pl.CostEstimate(flops=4_000_000_000, bytes_accessed=44_000_000 // PARTS, transcendentals=PAIRS * FF // PARTS),
    )(meta, a_all, pos, w1, w3, w2)


def merge_steps(layer, devs, ins, x_ref, scr, beside):
    a_hbm, cols_hbm, mine0_ref, far0_ref, mine1_ref, theirs1_ref, wr_ref = ins
    (a_ref, cols_ref, y_own, y_far, wr, gate, base, acc, back, xsend, xfar,
     l_sem, ys_sem, yr_sem, bs_sem, br_sem, fs_sem, fr_sem) = scr
    p, e, e_x, e_d, e_z, dev_y, dev_x, dev_d, dev_z, dev_yx = devs
    loads = [pltpu.make_async_copy(src, dst, l_sem.at[i])
             for i, (src, dst) in enumerate(((wr_ref.at[layer], wr), (mine0_ref, y_own.at[0]), (far0_ref, y_far.at[0]),
                                             (mine1_ref, y_own.at[1]), (a_hbm, a_ref), (cols_hbm.at[layer], cols_ref)))]
    for cp in loads:
        cp.start()
    entry_barrier((dev_y, dev_x, dev_d, dev_z, dev_yx))
    spans = [(t * NR, NR) for t in range(3)] + [(3 * NR, NR // 2)]
    y_copies = [remote(theirs1_ref.at[pl.ds(b, n)], y_far.at[1, pl.ds(b, n)], ys_sem.at[t], yr_sem.at[t], dev_y)
                for t, (b, n) in enumerate(spans)]
    for cp in y_copies:
        cp.start()
    beside()

    for i in (0, 4, 5):
        loads[i].wait()
    u = rms(a_ref[...]).astype(BF16)
    logits = jnp.zeros((ALL, 256), F32)
    rest = wr[...]
    for _ in range(3):
        part = rest.astype(BF16)
        rest = rest - part.astype(F32)
        logits = logits + mm(u, part)
    col = iota((ALL, 256), 1)
    g = [jnp.sum(jnp.where(cols_ref[:, 8 + k:9 + k] == col, logits, 0.0), axis=1, keepdims=True) for k in range(8)]
    top = functools.reduce(jnp.maximum, g)
    g = [jnp.exp(v - top) for v in g]
    total = functools.reduce(jnp.add, g)
    g = [v / total for v in g]
    pos = [cols_ref[:, k:k + 1] for k in range(8)]
    lane = iota((ALL, LN), 1)
    def build(c, carry):
        w = jnp.zeros((ALL, LN), F32)
        for k in range(8):
            w = jnp.where(pos[k] == lane + c * LN, g[k], w)
        for i in range(3):
            part = w.astype(BF16)
            w = w - part.astype(F32)
            gate[i, :, pl.ds(pl.multiple_of(c * LN, LN), LN)] = part
        return carry

    lax.fori_loop(0, PAIRS // LN, build, 0)

    def mix(h, t):
        b, n = spans[t]
        y = (y_own[h, b:b + n, :] + y_far[h, b:b + n, :]).astype(BF16)
        first = h * NR
        if t < 3:
            return sum(mm(gate[i, :, first:first + NR], y) for i in range(3))
        lo, hi = [sum(mm(gate[i, :, first + q * n:first + (q + 1) * n], y) for i in range(3)) for q in range(2)]
        keep = jnp.broadcast_to(p == 0, lo.shape)
        return jnp.where(keep, lo, pltpu.roll(lo, 64, axis=1)) + jnp.where(keep, pltpu.roll(hi, 64, axis=1), hi)

    loads[1].wait()
    loads[2].wait()
    for t in range(4):
        base[t] = mix(0, t)
    loads[3].wait()

    def block_of(ee):
        return pl.ds(pl.multiple_of(ee * T, T), T)

    left = iota((T // 2, LN), 1) < 64
    keep0 = jnp.broadcast_to(p == 0, left.shape)

    def swap(v):
        return pltpu.roll(v, 64, axis=1)

    def pack(v):
        top, bot = v[:T // 2], v[T // 2:]
        return jnp.where(left, jnp.where(keep0, top, swap(top)), jnp.where(keep0, swap(bot), bot))

    def span_of(ee, t):
        n = T if t < 3 else T // 2
        return pl.ds(pl.multiple_of(ee * n, n), n), pl.ds(0, n)

    def give(t):
        cps = []
        for i, (ee, dev) in enumerate(((e_x, dev_x), (e_z, dev_z), (e_d, dev_d))):
            src, dst = span_of(ee, t)
            cps.append(remote(acc.at[t, src], back.at[t, i, dst], bs_sem.at[t, i], br_sem.at[t, i], dev))
        for cp in cps:
            cp.start()
        return cps

    def cols(q, t):
        return pl.ds(pl.multiple_of(q * CM + t * LN, LN), LN) if t < 3 else slice(2 * CM, D)

    def finish(t, cps):
        for cp in cps:
            cp.wait_recv()
        src, dst = span_of(e, t)
        total = acc[t, src, :] + back[t, 0, dst, :] + back[t, 1, dst, :] + back[t, 2, dst, :]
        a_own = a_ref[block_of(e), cols(p, t)].astype(F32)
        xsend[t, dst, :] = ((a_own if t < 3 else pack(a_own)) + total).astype(BF16)
        cp = remote(xsend.at[t, dst], xfar.at[t, dst], fs_sem.at[t], fr_sem.at[t], dev_y)
        cp.start()
        return cp

    given, sent = [], []
    for t in range(4):
        y_copies[t].wait_recv()
        full = base[t] + mix(1, t)
        if t < 3:
            acc[t] = full
        else:
            for b in range(ALL // T):
                acc[t, b * T // 2:(b + 1) * T // 2, :] = pack(full[b * T:(b + 1) * T])
        given.append(give(t))
        if t >= 1:
            sent.append(finish(t - 1, given[t - 1]))
    sent.append(finish(3, given[3]))
    for t in range(3):
        x_ref[:, cols(p, t)] = xsend[t]
        sent[t].wait()
        x_ref[:, cols(1 - p, t)] = xfar[t]
    sent[3].wait()
    own, far = xsend[3, :T // 2, :].astype(F32), xfar[3, :T // 2, :].astype(F32)
    q0, q1 = jnp.where(keep0, own, far), jnp.where(keep0, far, own)
    x_ref[:T // 2, 2 * CM:] = jnp.where(left, q0, swap(q1)).astype(BF16)
    x_ref[T // 2:, 2 * CM:] = jnp.where(left, swap(q0), q1).astype(BF16)
    for cp in y_copies + [c for cps in given for c in cps]:
        cp.wait_send()


MERGE_IN, MERGE_SCR = 7, 18


def merge_last_kernel(layer, *refs):
    merge_steps(layer, peers(), refs[:MERGE_IN], refs[MERGE_IN], refs[MERGE_IN + 1:], lambda: None)


def merge_next_kernel(layer, *refs):
    ins, len_ref, hbm, a_ref = refs[:MERGE_IN], refs[MERGE_IN], refs[MERGE_IN + 1:MERGE_IN + 7], refs[MERGE_IN + 7]
    x_ref, scr = refs[MERGE_IN + 8], refs[MERGE_IN + 9:]
    devs = peers()
    start, run = attn_steps(layer + 1, NCH, devs, len_ref, hbm, scr[MERGE_SCR:])
    merge_steps(layer, devs, ins, x_ref, scr[:MERGE_SCR], lambda: start(NCH))
    run(x_ref, a_ref, NCH, lambda: None)


def merge_scratch():
    dma = pltpu.SemaphoreType.DMA
    return [
        pltpu.VMEM((ALL, D), BF16), pltpu.VMEM((ALL, LN), I32),
        pltpu.VMEM((2, PR, LN), F32), pltpu.VMEM((2, PR, LN), F32),
        pltpu.VMEM((D, 256), F32), pltpu.VMEM((3, ALL, PAIRS), BF16),
        pltpu.VMEM((4, ALL, LN), F32), pltpu.VMEM((4, ALL, LN), F32), pltpu.VMEM((4, 3, T, LN), F32),
        pltpu.VMEM((4, T, LN), BF16), pltpu.VMEM((4, T, LN), BF16),
        dma((6,)), dma((4,)), dma((4,)), dma((4, 3)), dma((4, 3)), dma((4,)), dma((4,)),
    ]


def merge(layer, last, ins, cache_len, hbm):
    vm, sm, hb, anywhere = (pl.BlockSpec(memory_space=m) for m in (pltpu.VMEM, pltpu.SMEM, pltpu.HBM, pl.ANY))
    in_specs = [anywhere] * 6 + [hb]
    params = functools.partial(pltpu.CompilerParams, collective_id=1 + layer, has_side_effects=True)
    if last:
        return pl.pallas_call(
            functools.partial(merge_last_kernel, layer),
            name=f"merge_{layer}",
            out_shape=jax.ShapeDtypeStruct((T, D), BF16),
            in_specs=in_specs,
            out_specs=vm,
            scratch_shapes=merge_scratch(),
            compiler_params=params(vmem_limit_bytes=63963136),
        )(*ins)
    return pl.pallas_call(
        functools.partial(merge_next_kernel, layer),
        name=f"merge_attn_{layer}",
        out_shape=jax.ShapeDtypeStruct((ALL, D), BF16),
        in_specs=in_specs + [sm] + [hb] * 6,
        out_specs=vm,
        scratch_shapes=[pltpu.VMEM((T, D), BF16)] + merge_scratch() + attn_scratch(NCH),
        compiler_params=params(vmem_limit_bytes=67043328),
    )(*ins, cache_len, *hbm)


def solution(mesh):
    tok_spec = P(('dp', 'ep'), None)
    cache_spec = P(None, ('dp', 'ep'), 'pool', None, None)
    up_spec = P(None, 'ep', None, 'pool')
    down_spec = P(None, 'ep', 'pool', None)
    in_specs = (tok_spec, cache_spec, cache_spec, P(('dp', 'ep')), P(), P(), P(), P(), P(), P(None, ('dp', 'ep'), None),
                up_spec, up_spec, down_spec)

    def body(hidden, k_cache, v_cache, cache_len, w_q, w_k, w_v, w_o, w_router, expert_ids, w_one, w_three, w_two):
        layers = w_q.shape[0]
        k = k_cache.reshape(layers, T, ROWS, HD)
        v = v_cache.reshape(layers, T, ROWS, HD)
        id_t = jnp.swapaxes(expert_ids, 1, 2)
        hbm = (k, v, w_q, w_k, w_v, w_o)
        a_all, meta, pos, cols = attention(hidden, cache_len, id_t, hbm)
        for layer in range(layers):
            mine0, theirs0 = experts(layer, 0, a_all, meta, pos, w_one, w_three, w_two)
            far0 = lax.ppermute(theirs0, 'pool', [(0, 1), (1, 0)])
            mine1, theirs1 = experts(layer, 1, a_all, meta, pos, w_one, w_three, w_two)
            ins = (a_all, cols, mine0, far0, mine1, theirs1, w_router)
            last = layer == layers - 1
            a_all = merge(layer, last, ins, cache_len, hbm)
        return a_all

    return jax.shard_map(body, mesh=mesh, in_specs=in_specs, out_specs=tok_spec, check_vma=False)
```
